128 devices in a mesh: dom: 128 (over z, y, x, core).
Axes of the slice: x: 4, y: 4, z: 4, core: 2. Of those that a mesh axis runs over, the one named last changes fastest.
Arguments:
- right_side: float32 [18, 131072], P(None, 'dom'), may hold values from -20 to 20
- element_matrix: bfloat16 [72, 72, 65536], P(None, None, 'dom'), may hold values from -8 to 8, as said below
- face_map: int32 [4, 65536], P(None, 'dom'), may hold values from 0 to 1535
- share_index: int32 [128, 4, 128], P('dom'), may hold values from 0 to 1023
- share_count: int32 [128, 4], P('dom'), may hold values from 0 to 128, as said below
- face_mass: float32 [131072], P('dom'), may hold values from 0.5 to 2
- absorbing: int32 [131072], P('dom'), may hold values 0 or 1
- impedance: float32 [131072], P('dom'), may hold values from 0.5 to 4
Outputs:
- solution: float32 [18, 131072], P(None, 'dom')
- residual: float32 [18, 131072], P(None, 'dom')
The draws below stay inside these ranges and needn't reach their ends.
Inputs may be any that keep to these rules, and one draw needn't show every extreme that they name: `element_matrix`: each element's 72 x 72 matrix is symmetric positive definite. share_count[d, k] is 0 where device d + o_k lies outside the axis; it equals 128 for some device and offset in every draw.
All inputs are finite; a program needn't handle non-finite values. No bound on the sum of `absorbing` on one device may be relied on, other than what follows from the above.
Results may differ from the reference program's by a relative error of at most 0.0003.
Values sent between devices are 32-bit elements; how exact they have to be, the bound alone decides.
A program may use at most 64 MiB of HBM per device.

```python
import math
import jax
import jax.numpy as jnp
from jax import lax

TRACE = 18
SIDES = 4
DOFS = 72
REACH = 2
OFFSETS = 4
E_DEV = 512
F_DEV = 1024
GH = 128
ITERS = 2
E_TOTAL = 65536
F_TOTAL = 131072
N_DOM = 128


def draw_right_side(key, part):
    devices = F_TOTAL // F_DEV
    first_key, second_key, third_key = jax.random.split(key, 3)
    base_draw = jnp.clip(jax.random.normal(first_key, (TRACE, F_TOTAL), jnp.float32), -4.0, 4.0)
    component = jnp.exp(jax.random.uniform(second_key, (TRACE,), jnp.float32, jnp.log(0.5), jnp.log(5.0)))
    face_scale = jnp.exp(jax.random.uniform(third_key, (F_TOTAL,), jnp.float32, jnp.log(0.3), jnp.log(3.0)))
    device_of = jnp.arange(F_TOTAL, dtype=jnp.int32) // F_DEV
    ramp_scale = jnp.power(3.0, 0.5 * device_of.astype(jnp.float32) / (devices - 1))
    values_out = base_draw * component[:, None] * face_scale[None, :] * ramp_scale[None, :] * 0.25
    return jnp.clip(values_out, -20.0, 20.0).astype(jnp.float32)


def draw_element_matrix(key, part):
    devices = E_TOTAL // E_DEV

    def one_device(part_index):
        device_key = jax.random.fold_in(key, part_index)
        first_key, second_key = jax.random.split(device_key)
        raw_draw = jnp.clip(jax.random.normal(first_key, (DOFS, DOFS, E_DEV), jnp.float32), -5.0, 5.0)
        symmetric = 0.5 * (raw_draw + raw_draw.transpose(1, 0, 2)) * 0.025
        identity = jnp.eye(DOFS, dtype=jnp.float32)[:, :, None]
        off_diag = symmetric * (1.0 - identity)
        rowsum = jnp.sum(jnp.abs(off_diag), axis=1)
        stiffness = jnp.exp(jax.random.uniform(second_key, (E_DEV,), jnp.float32, jnp.log(0.5), jnp.log(2.0)))
        matrix = (off_diag + identity * (rowsum + 0.3)[:, None, :]) * stiffness[None, None, :]
        return matrix.astype(jnp.bfloat16)
    stacked = lax.map(one_device, jnp.arange(devices, dtype=jnp.int32))
    return jnp.moveaxis(stacked, 0, 2).reshape(DOFS, DOFS, E_TOTAL)


def draw_share_count(key, part):
    devices = F_TOTAL // F_DEV
    first_key, second_key, third_key, fourth_key = jax.random.split(key, 4)
    full_draw = jax.random.randint(first_key, (devices, OFFSETS), 0, 4)
    small_draw = jax.random.randint(second_key, (devices, OFFSETS), 0, GH // 4 + 1)
    counts = jnp.where(full_draw == 0, GH, small_draw)
    row_index = lax.broadcasted_iota(jnp.int32, (devices, OFFSETS), 0)
    blocks = lax.broadcasted_iota(jnp.int32, (devices, OFFSETS), 1)
    shift_by = jnp.where(blocks < REACH, blocks - REACH, blocks - REACH + 1)
    inside = (row_index + shift_by >= 0) & (row_index + shift_by < devices)
    pick_row = jax.random.randint(third_key, (), REACH, devices - REACH)
    pick_block = jax.random.randint(fourth_key, (), 0, OFFSETS)
    counts = jnp.where((row_index == pick_row) & (blocks == pick_block), GH, counts)
    return jnp.where(inside, counts, 0).astype(jnp.int32)


def touch_ends(entries, rng, smallest, top_value):
    shape = entries.shape
    index_at = [jax.random.randint(jax.random.fold_in(rng, axis), (), 0, shape[axis]) for axis in range(len(shape))]
    entries = entries.at[tuple(index_at)].set(smallest)
    longest = shape.index(max(shape))
    index_at[longest] = (index_at[longest] + 1) % shape[longest]
    return entries.at[tuple(index_at)].set(top_value)


def level_of(rng, shape, cuts, low, top_value):
    factor_of, own = 1.0, jax.random.fold_in(rng, 6)
    for axis_at, shards_of in cuts:
        heights = jnp.exp(jax.random.uniform(jax.random.fold_in(own, axis_at), (shards_of,), jnp.float32, low / len(cuts), top_value / len(cuts)))
        factor_of = factor_of * jnp.repeat(heights, shape[axis_at] // shards_of).reshape([-1 if axis == axis_at else 1 for axis in range(len(shape))])
    return factor_of


def setup_inputs(seed: int = 0) -> dict:
    streams_of = jax.random.split(jax.random.key(seed), 9)
    right_side = draw_right_side(jax.random.fold_in(streams_of[8], 71), 0)
    element_matrix = draw_element_matrix(jax.random.fold_in(streams_of[8], 71), 0)
    face_map = touch_ends(jax.random.randint(streams_of[2], (SIDES, E_TOTAL), 0, F_DEV + OFFSETS * GH), jax.random.fold_in(streams_of[2], 1), 0, (F_DEV + OFFSETS * GH) - 1).astype(jnp.int32)
    share_index = touch_ends(jax.random.randint(streams_of[3], (N_DOM, OFFSETS, GH), 0, F_DEV), jax.random.fold_in(streams_of[3], 1), 0, F_DEV - 1).astype(jnp.int32)
    share_count = draw_share_count(jax.random.fold_in(streams_of[8], 71), 0)
    face_mass = jnp.clip(jnp.exp(math.log(2.0) - 1.3862944 * jax.random.uniform(streams_of[5], (F_TOTAL,), jnp.float32) ** level_of(streams_of[5], (F_TOTAL,), ((0, 128),), -0.2, 0.2)), 0.5, 2.0)
    absorbing = touch_ends((jax.random.randint(streams_of[6], (F_TOTAL,), 0, 4) < 1).astype(jnp.int32), jax.random.fold_in(streams_of[6], 1), 0, 1)
    impedance = jnp.clip(jnp.exp(math.log(4.0) - 2.0794415 * jax.random.uniform(streams_of[7], (F_TOTAL,), jnp.float32) ** level_of(streams_of[7], (F_TOTAL,), ((0, 128),), -0.2, 0.2)), 0.5, 4.0)
    return {"right_side": right_side, "element_matrix": element_matrix, "face_map": face_map, "share_index": share_index, "share_count": share_count, "face_mass": face_mass, "absorbing": absorbing, "impedance": impedance}


def offset_of(block_index):
    return block_index - REACH if block_index < REACH else block_index - REACH + 1


def slot_map(face_map, share_index, share_count):
    element_count = face_map.shape[1]
    owner = jnp.arange(element_count, dtype=jnp.int32) // E_DEV
    owner = jnp.broadcast_to(owner[None, :], face_map.shape)
    local_face = face_map < F_DEV
    ghost_slot = jnp.maximum(face_map - F_DEV, 0)
    block_index = ghost_slot // GH
    within = ghost_slot % GH
    offsets = jnp.array([offset_of(b) for b in range(OFFSETS)], dtype=jnp.int32)
    sender = owner - offsets[block_index]
    sender_ok = (sender >= 0) & (sender < N_DOM)
    sender_safe = jnp.clip(sender, 0, N_DOM - 1).astype(jnp.int32)
    remote = share_index[sender_safe, block_index, within]
    live_count = share_count[sender_safe, block_index]
    alive_slot = sender_ok & (within < live_count)
    target = jnp.where(local_face, owner * F_DEV + face_map, sender_safe * F_DEV + remote).astype(jnp.int32)
    weight = jnp.where(local_face | alive_slot, 1.0, 0.0).astype(jnp.float32)
    return target, weight


def operate(field_now, element_matrix, target, weight, diagonal):
    picked = field_now[:, target] * weight[None, :, :]
    picked = picked.transpose(1, 0, 2).reshape(DOFS, E_TOTAL)

    def one_part(part_index):
        first_element = part_index * E_DEV
        matrices = lax.dynamic_slice_in_dim(element_matrix, first_element, E_DEV, 2).astype(jnp.float32)
        traces_in = lax.dynamic_slice_in_dim(picked, first_element, E_DEV, 1)
        return jnp.sum(matrices * traces_in[None, :, :], axis=1)

    products = lax.map(one_part, jnp.arange(N_DOM, dtype=jnp.int32))
    product = products.transpose(1, 0, 2).reshape(DOFS, E_TOTAL)
    spread = product.reshape(SIDES, TRACE, E_TOTAL) * weight[:, None, :]
    spread = spread.transpose(1, 0, 2)
    result = jnp.zeros_like(field_now).at[:, target].add(spread)
    return result + diagonal[None, :] * field_now


def reference(right_side, element_matrix, face_map, share_index, share_count, face_mass, absorbing, impedance):
    diagonal = face_mass + absorbing.astype(jnp.float32) * impedance
    target, weight = slot_map(face_map, share_index, share_count)
    solution = jnp.zeros_like(right_side)
    residual = right_side
    direction = right_side
    norm_now = jnp.sum(residual * residual)
    for rounds in range(ITERS):
        image_vec = operate(direction, element_matrix, target, weight, diagonal)
        step_size = norm_now / jnp.sum(direction * image_vec)
        solution = solution + step_size * direction
        residual = residual - step_size * image_vec
        norm_next = jnp.sum(residual * residual)
        direction = residual + (norm_next / norm_now) * direction
        norm_now = norm_next
    return solution, residual
```

```python
import functools

import jax
import jax.numpy as jnp
from jax import lax
from jax.experimental import pallas as pl
from jax.experimental.pallas import tpu as pltpu
from jax.sharding import PartitionSpec as P

TRACE = 18
ROWS = 24
SIDES = 4
DOFS = 72
E_DEV = 512
F_DEV = 1024
GH = 128
OFFSETS = (-2, -1, 1, 2)
N_DOM = 128
LANES = 128
WIDE = 256
MESH = pl.DeviceIdType.MESH


def lane_pick(blocks, index_row):
    low = jnp.broadcast_to(index_row & (LANES - 1), (ROWS, LANES))
    high = jnp.broadcast_to(index_row >> 7, (ROWS, LANES))
    picked = jnp.zeros((ROWS, LANES), jnp.float32)
    for at, block in enumerate(blocks):
        moved = jnp.take_along_axis(block, low, axis=1, mode="promise_in_bounds")
        picked = jnp.where(high == at, moved, picked)
    return picked


def split_two(value):
    head = value.astype(jnp.bfloat16)
    tail = (value - head.astype(jnp.float32)).astype(jnp.bfloat16)
    return head.astype(jnp.float32), tail.astype(jnp.float32)


def spread_rows(value, index_row, groups):
    head, tail = split_two(value)
    high = jnp.broadcast_to(index_row >> 8, value.shape)
    pieces = []
    for group in range(groups):
        mask = high == group
        pieces.append(jnp.where(mask, head, 0.0))
        pieces.append(jnp.where(mask, tail, 0.0))
    return jnp.concatenate(pieces, axis=0).astype(jnp.bfloat16)


def one_hot_low(index_row):
    count = index_row.shape[1]
    low = jnp.broadcast_to(index_row & (WIDE - 1), (WIDE, count))
    rows = lax.broadcasted_iota(jnp.int32, (WIDE, count), 0)
    return jnp.where(rows == low, 1.0, 0.0).astype(jnp.bfloat16)


def nt_dot(left, right):
    return lax.dot_general(left, right, (((1,), (1,)), ((), ())), preferred_element_type=jnp.float32)


def kernel(
    right_hbm, matrix_hbm, map_hbm, share_hbm, count_hbm, mass_hbm, absorb_hbm, imped_hbm,
    x_hbm, r_hbm,
    right_ref, map_ref, share_ref, count_ref, mass_ref, absorb_ref, imped_ref, x_ref, r_ref, load_sem, store_sem,
    matrix, field0, field1, image, diag, picked0, picked1, product, hot, hot_share,
    out_buf, ghost_buf, part_buf, back_buf, sum_buf, sum_in,
    matrix_sem, out_send, out_recv, part_send, part_recv, sum_send, sum_recv,
):
    me = lax.axis_index("dom")
    loads = [
        pltpu.make_async_copy(source, target, load_sem.at[at])
        for at, (source, target) in enumerate((
            (share_hbm, share_ref), (count_hbm, count_ref), (right_hbm, right_ref), (map_hbm, map_ref),
            (mass_hbm, mass_ref), (absorb_hbm, absorb_ref), (imped_hbm, imped_ref),
        ))
    ]
    for load in loads:
        load.start()
    matrix_copy = pltpu.make_async_copy(matrix_hbm, matrix, matrix_sem)
    matrix_copy.start()

    core = lax.rem(me, 2)
    at_x = lax.rem(me // 2, 4)
    at_y = lax.rem(me // 8, 4)
    at_z = me // 32

    def line_partner(axis, step):
        if axis == 0:
            return me + 1 - 2 * core
        place, stride = ((at_x, 2), (at_y, 8), (at_z, 32))[axis - 1]
        return me + (lax.rem(place + step, 4) - place) * stride

    inside_to = [(me + o >= 0) & (me + o < N_DOM) for o in OFFSETS]
    inside_from = [(me - o >= 0) & (me - o < N_DOM) for o in OFFSETS]

    barrier = pltpu.get_barrier_semaphore()
    arrivals = jnp.int32(10)
    for k, o in enumerate(OFFSETS):
        @pl.when(inside_to[k])
        def _():
            pl.semaphore_signal(barrier, inc=1, device_id=(me + o,), device_id_type=MESH)
        arrivals = arrivals + inside_from[k].astype(jnp.int32)
    for axis in range(4):
        for step in range(1, 2 if axis == 0 else 4):
            pl.semaphore_signal(
                barrier, inc=1, device_id=(line_partner(axis, step),), device_id_type=MESH
            )

    for load in loads:
        load.wait()
    field0[0:TRACE, :] = right_ref[...]
    field0[TRACE:ROWS, :] = jnp.zeros((ROWS - TRACE, F_DEV), jnp.float32)
    diag[...] = mass_ref[...] + absorb_ref[...].astype(jnp.float32) * imped_ref[...]
    for k in range(4):
        @pl.when(jnp.logical_not(inside_from[k]))
        def _():
            for turn in range(2):
                ghost_buf[turn, k] = jnp.zeros((ROWS, GH), jnp.float32)
        @pl.when(jnp.logical_not(inside_to[k]))
        def _():
            for turn in range(2):
                back_buf[turn, k] = jnp.zeros((ROWS, GH), jnp.float32)

    lane = lax.broadcasted_iota(jnp.int32, (ROWS, GH), 1)
    alive = [lane < count_ref[0, k] for k in range(4)]

    def own_blocks(ref):
        return [ref[:, b * LANES:(b + 1) * LANES] for b in range(F_DEV // LANES)]

    def out_copy(turn, k):
        return pltpu.make_async_remote_copy(
            src_ref=out_buf.at[turn, k], dst_ref=ghost_buf.at[turn, k],
            send_sem=out_send.at[turn, k], recv_sem=out_recv.at[turn, k],
            device_id=(me + OFFSETS[k],), device_id_type=MESH,
        )

    def part_copy(turn, k):
        return pltpu.make_async_remote_copy(
            src_ref=part_buf.at[turn, k], dst_ref=back_buf.at[turn, k],
            send_sem=part_send.at[turn, k], recv_sem=part_recv.at[turn, k],
            device_id=(me - OFFSETS[k],), device_id_type=MESH,
        )

    def send_out(turn, ref):
        blocks = own_blocks(ref)
        for k in range(4):
            gone = lane_pick(blocks, share_ref[k:k + 1, :])
            out_buf[turn, k] = jnp.where(alive[k], gone, 0.0)
        if turn == 0:
            pl.semaphore_wait(barrier, arrivals)
        for k in range(4):
            @pl.when(inside_to[k])
            def _():
                out_copy(turn, k).start()

    def await_out(turn):
        for k in range(4):
            @pl.when(inside_from[k])
            def _():
                out_copy(turn, k).wait_recv()

    def send_part(turn):
        for k in range(4):
            @pl.when(inside_from[k])
            def _():
                part_copy(turn, k).start()

    def await_part(turn):
        for k in range(4):
            @pl.when(inside_to[k])
            def _():
                part_copy(turn, k).wait_recv()

    def pick_all(turn, ref, store):
        blocks = own_blocks(ref) + [ghost_buf[turn, k] for k in range(4)]
        for side in range(SIDES):
            for b in range(E_DEV // LANES):
                cols = slice(b * LANES, (b + 1) * LANES)
                store(side, b, lane_pick(blocks, map_ref[side:side + 1, cols]))

    def multiply(picked):
        for b in range(E_DEV // LANES):
            cols = slice(b * LANES, (b + 1) * LANES)
            total = jnp.zeros((DOFS, LANES), jnp.float32)
            for side in range(SIDES):
                def one(c, total):
                    row = picked[side, b, pl.ds(c, 8, stride=0), :]
                    part = matrix[side * TRACE + c, :, cols].astype(jnp.float32)
                    return total + (part.reshape(DOFS // 8, 8, LANES) * row[None]).reshape(DOFS, LANES)
                total = lax.fori_loop(0, TRACE, one, total, unroll=6)
            for side in range(SIDES):
                product[side, 0:TRACE, cols] = total[side * TRACE:(side + 1) * TRACE]

    def energy(picked):
        total = jnp.zeros((8, LANES), jnp.float32)
        for side in range(SIDES):
            for b in range(E_DEV // LANES):
                cols = slice(b * LANES, (b + 1) * LANES)
                both = picked[side, b] * product[side, :, cols]
                total = total + both[0:8] + both[8:16] + both[16:24]
        return total

    def face_sums(ref):
        square = jnp.zeros((8, LANES), jnp.float32)
        weighted = jnp.zeros((8, LANES), jnp.float32)
        for b in range(F_DEV // LANES):
            value = ref[:, b * LANES:(b + 1) * LANES]
            both = value * value
            both = both[0:8] + both[8:16] + both[16:24]
            square = square + both
            weighted = weighted + both * diag[b:b + 1, :]
        return square, weighted

    def scatter(turn, ref):
        total = jnp.zeros((6 * 2 * ROWS, WIDE), jnp.float32)
        for side in range(SIDES):
            left = spread_rows(product[side], map_ref[side:side + 1, :], 6)
            total = total + nt_dot(left, hot[:, side * E_DEV:(side + 1) * E_DEV])
        for group in range(6):
            base = group * 2 * ROWS
            both = total[base:base + ROWS] + total[base + ROWS:base + 2 * ROWS]
            if group >= 4:
                part_buf[turn, 2 * (group - 4)] = both[:, 0:GH]
                part_buf[turn, 2 * (group - 4) + 1] = both[:, GH:]
            else:
                for half in range(2):
                    b = 2 * group + half
                    cols = slice(b * LANES, (b + 1) * LANES)
                    image[turn, :, cols] = (
                        both[:, half * LANES:(half + 1) * LANES] + diag[b:b + 1, :] * ref[:, cols]
                    )

    def add_back(turn):
        total = jnp.zeros((4 * 2 * ROWS, WIDE), jnp.float32)
        for k in range(4):
            value = jnp.where(alive[k], back_buf[turn, k], 0.0)
            left = spread_rows(value, share_ref[k:k + 1, :], 4)
            total = total + nt_dot(left, hot_share[:, k * GH:(k + 1) * GH])
        for group in range(4):
            base = group * 2 * ROWS
            both = total[base:base + ROWS] + total[base + ROWS:base + 2 * ROWS]
            cols = slice(group * WIDE, (group + 1) * WIDE)
            image[turn, :, cols] = image[turn, :, cols] + both

    def sum_copy(turn, axis, step):
        return pltpu.make_async_remote_copy(
            src_ref=sum_buf.at[turn, axis], dst_ref=sum_in.at[turn, axis, step - 1],
            send_sem=sum_send.at[turn, axis, step - 1], recv_sem=sum_recv.at[turn, axis, step - 1],
            device_id=(line_partner(axis, step),), device_id_type=MESH,
        )

    def axis_steps(axis):
        return range(1, 2 if axis == 0 else 4)

    def sum_start(turn, axis, tile):
        sum_buf[turn, axis] = tile
        for step in axis_steps(axis):
            sum_copy(turn, axis, step).start()

    def sum_finish(turn, axis):
        tile = sum_buf[turn, axis]
        for step in axis_steps(axis):
            sum_copy(turn, axis, step).wait_recv()
        for step in axis_steps(axis):
            tile = tile + sum_in[turn, axis, step - 1]
        return tile

    def pack(first, second):
        row = lax.broadcasted_iota(jnp.int32, (8, LANES), 0)
        return jnp.where(
            row == 0,
            jnp.sum(first, axis=0, keepdims=True),
            jnp.where(row == 1, jnp.sum(second, axis=0, keepdims=True), 0.0),
        )

    def unpack(tile):
        total = jnp.sum(tile, axis=1, keepdims=True)
        return total[0:1], total[1:2]

    def clear_tail(ref):
        for side in range(SIDES):
            ref[side, TRACE:ROWS, :] = jnp.zeros((ROWS - TRACE, E_DEV), jnp.float32)

    send_out(0, field0)
    clear_tail(product)
    for side in range(SIDES):
        hot[:, side * E_DEV:(side + 1) * E_DEV] = one_hot_low(map_ref[side:side + 1, :])
    for k in range(4):
        hot_share[:, k * GH:(k + 1) * GH] = one_hot_low(share_ref[k:k + 1, :])
    square, weighted = face_sums(field0)
    matrix_copy.wait()
    await_out(0)

    def keep0(side, b, value):
        picked0[side, b] = value

    pick_all(0, field0, keep0)
    multiply(picked0)
    tile = pack(square, weighted + energy(picked0))
    sum_start(0, 3, tile)
    scatter(0, field0)
    send_part(0)
    sum_start(0, 2, sum_finish(0, 3))
    await_part(0)
    add_back(0)
    send_out(1, image.at[0])
    sum_start(0, 1, sum_finish(0, 2))
    sum_start(0, 0, sum_finish(0, 1))
    norm0, curve0 = unpack(sum_finish(0, 0))
    step0 = norm0 / curve0
    for b in range(F_DEV // LANES):
        cols = slice(b * LANES, (b + 1) * LANES)
        field1[:, cols] = field0[:, cols] - step0 * image[0, :, cols]
    square, weighted = face_sums(field1)
    await_out(1)

    def keep1(side, b, value):
        picked1[side, b] = picked0[side, b] - step0 * value

    pick_all(1, image.at[0], keep1)
    multiply(picked1)
    tile = pack(square, weighted + energy(picked1))
    sum_start(1, 3, tile)
    scatter(1, field1)
    send_part(1)
    sum_start(1, 2, sum_finish(1, 3))
    await_part(1)
    add_back(1)
    sum_start(1, 1, sum_finish(1, 2))
    sum_start(1, 0, sum_finish(1, 1))
    norm1, curve1 = unpack(sum_finish(1, 0))
    ratio = norm1 / norm0
    step1 = norm1 / (curve1 - ratio * norm1 / step0)
    for b in range(F_DEV // LANES):
        cols = slice(b * LANES, (b + 1) * LANES)
        start = field0[0:TRACE, cols]
        later = field1[0:TRACE, cols]
        x_ref[:, cols] = step0 * start + step1 * (later + ratio * start)
        r_ref[:, cols] = later - step1 * (image[1, 0:TRACE, cols] + ratio * image[0, 0:TRACE, cols])

    stores = [
        pltpu.make_async_copy(source, target, store_sem.at[at])
        for at, (source, target) in enumerate(((x_ref, x_hbm), (r_ref, r_hbm)))
    ]
    for store in stores:
        store.start()
    for store in stores:
        store.wait()
    for turn in range(2):
        for k in range(4):
            @pl.when(inside_to[k])
            def _():
                out_copy(turn, k).wait_send()
            @pl.when(inside_from[k])
            def _():
                part_copy(turn, k).wait_send()
        for axis in range(4):
            for step in axis_steps(axis):
                sum_copy(turn, axis, step).wait_send()


def shards(right_side, element_matrix, face_map, share_index, share_count, face_mass, absorbing, impedance):
    hbm = pl.BlockSpec(memory_space=pltpu.HBM)
    f32, bf16, i32 = jnp.float32, jnp.bfloat16, jnp.int32
    out = jax.ShapeDtypeStruct((TRACE, F_DEV), f32)
    return pl.pallas_call(
        kernel,
        name="trace_cg",
        out_shape=(out, out),
        in_specs=[hbm] * 8,
        out_specs=(hbm, hbm),
        scratch_shapes=[
            pltpu.VMEM((TRACE, F_DEV), f32),
            pltpu.VMEM((SIDES, E_DEV), i32),
            pltpu.VMEM((4, GH), i32),
            pltpu.SMEM((1, 4), i32),
            pltpu.VMEM((8, LANES), f32),
            pltpu.VMEM((8, LANES), i32),
            pltpu.VMEM((8, LANES), f32),
            pltpu.VMEM((TRACE, F_DEV), f32),
            pltpu.VMEM((TRACE, F_DEV), f32),
            pltpu.SemaphoreType.DMA((7,)),
            pltpu.SemaphoreType.DMA((2,)),
            pltpu.VMEM((DOFS, DOFS, E_DEV), bf16),
            pltpu.VMEM((ROWS, F_DEV), f32),
            pltpu.VMEM((ROWS, F_DEV), f32),
            pltpu.VMEM((2, ROWS, F_DEV), f32),
            pltpu.VMEM((8, LANES), f32),
            pltpu.VMEM((SIDES, 4, ROWS, LANES), f32),
            pltpu.VMEM((SIDES, 4, ROWS, LANES), f32),
            pltpu.VMEM((SIDES, ROWS, E_DEV), f32),
            pltpu.VMEM((WIDE, SIDES * E_DEV), bf16),
            pltpu.VMEM((WIDE, 4 * GH), bf16),
            pltpu.VMEM((2, 4, ROWS, GH), f32),
            pltpu.VMEM((2, 4, ROWS, GH), f32),
            pltpu.VMEM((2, 4, ROWS, GH), f32),
            pltpu.VMEM((2, 4, ROWS, GH), f32),
            pltpu.VMEM((2, 4, 8, LANES), f32),
            pltpu.VMEM((2, 4, 3, 8, LANES), f32),
            pltpu.SemaphoreType.DMA,
            pltpu.SemaphoreType.DMA((2, 4)),
            pltpu.SemaphoreType.DMA((2, 4)),
            pltpu.SemaphoreType.DMA((2, 4)),
            pltpu.SemaphoreType.DMA((2, 4)),
            pltpu.SemaphoreType.DMA((2, 4, 3)),
            pltpu.SemaphoreType.DMA((2, 4, 3)),
        ],
        compiler_params=pltpu.CompilerParams(
            collective_id=0, has_side_effects=True, vmem_limit_bytes=67043328
        ),
    )(
        right_side, element_matrix, face_map, share_index.reshape(4, GH), share_count,
        face_mass.reshape(8, LANES), absorbing.reshape(8, LANES), impedance.reshape(8, LANES),
    )


def solution(mesh):
    in_specs = (
        P(None, "dom"), P(None, None, "dom"), P(None, "dom"), P("dom", None, None),
        P("dom", None), P("dom"), P("dom"), P("dom"),
    )
    return jax.shard_map(
        shards, mesh=mesh, in_specs=in_specs,
        out_specs=(P(None, "dom"), P(None, "dom")), check_vma=False,
    )
```

```python
import functools

import jax
import jax.numpy as jnp
from jax import lax
from jax.experimental import pallas as pl
from jax.experimental.pallas import tpu as pltpu
from jax.sharding import PartitionSpec as P

TRACE = 18
ROWS = 24
SIDES = 4
DOFS = 72
E_DEV = 512
F_DEV = 1024
GH = 128
OFFSETS = (-2, -1, 1, 2)
N_DOM = 128
LANES = 128
WIDE = 256
MESH = pl.DeviceIdType.MESH


def lane_pick(blocks, index_row):
    low = jnp.broadcast_to(index_row & (LANES - 1), (8, LANES))
    high = jnp.broadcast_to(index_row >> 7, (8, LANES))
    masks = [high == at for at in range(len(blocks))]
    pieces = []
    for i in range(ROWS // 8):
        picked = jnp.zeros((8, LANES), jnp.float32)
        for mask, block in zip(masks, blocks):
            moved = jnp.take_along_axis(block(i), low, axis=1, mode="promise_in_bounds")
            picked = jnp.where(mask, moved, picked)
        pieces.append(picked)
    return jnp.concatenate(pieces, axis=0)


def split_two(value):
    head = value.astype(jnp.bfloat16)
    tail = (value - head.astype(jnp.float32)).astype(jnp.bfloat16)
    return head.astype(jnp.float32), tail.astype(jnp.float32)


def spread_rows(value, index_row, groups):
    head, tail = split_two(value)
    high = jnp.broadcast_to(index_row >> 8, value.shape)
    pieces = []
    for group in range(groups):
        mask = high == group
        pieces.append(jnp.where(mask, head, 0.0))
        pieces.append(jnp.where(mask, tail, 0.0))
    return jnp.concatenate(pieces, axis=0).astype(jnp.bfloat16)


def one_hot_low(index_row):
    count = index_row.shape[1]
    low = jnp.broadcast_to(index_row & (WIDE - 1), (WIDE, count))
    rows = lax.broadcasted_iota(jnp.int32, (WIDE, count), 0)
    return jnp.where(rows == low, 1.0, 0.0).astype(jnp.bfloat16)


def nt_dot(left, right):
    return lax.dot_general(left, right, (((1,), (1,)), ((), ())), preferred_element_type=jnp.float32)


def kernel(
    right_hbm, matrix_hbm, map_hbm, share_hbm, count_hbm, mass_hbm, absorb_hbm, imped_hbm,
    lead_ref, later_ref, along_ref, step_ref,
    right_ref, map_ref, share_ref, count_ref, mass_ref, absorb_ref, imped_ref, load_sem, meet_sem,
    matrix, widened, field0, field1, image, diag, picked0, picked1, product, hot, hot_share,
    out_buf, ghost_buf, part_buf, back_buf, sum_buf, sum_in,
    matrix_sem, out_send, out_recv, part_send, part_recv, sum_send, sum_recv,
):
    me = lax.axis_index("dom")
    loads = [
        pltpu.make_async_copy(source, target, load_sem.at[at])
        for at, (source, target) in enumerate((
            (share_hbm, share_ref), (count_hbm, count_ref), (right_hbm, right_ref), (map_hbm, map_ref),
            (mass_hbm, mass_ref), (absorb_hbm, absorb_ref), (imped_hbm, imped_ref),
        ))
    ]
    for load in loads:
        load.start()
    matrix_copy = pltpu.make_async_copy(matrix_hbm, matrix, matrix_sem)
    matrix_copy.start()

    core = lax.rem(me, 2)
    at_x = lax.rem(me // 2, 4)
    at_y = lax.rem(me // 8, 4)
    at_z = me // 32

    along_x = [lax.rem(at_x + d, 4) * 2 for d in range(4)]
    along_y = [lax.rem(at_y + d, 4) * 8 for d in range(4)]
    along_z = [lax.rem(at_z + d, 4) * 32 for d in range(4)]
    cores = (core, 1 - core)

    def device_at(dz, dy, dx, dc):
        return along_z[dz] + along_y[dy] + along_x[dx] + cores[dc]

    inside_to = [(me + o >= 0) & (me + o < N_DOM) for o in OFFSETS]
    inside_from = [(me - o >= 0) & (me - o < N_DOM) for o in OFFSETS]

    barrier = pltpu.get_barrier_semaphore()
    arrivals = jnp.int32(13)
    for k, o in enumerate(OFFSETS):
        @pl.when(inside_to[k])
        def _():
            pl.semaphore_signal(barrier, inc=1, device_id=(me + o,), device_id_type=MESH)
        arrivals = arrivals + inside_from[k].astype(jnp.int32)
    line_y = [device_at(0, d, 0, 0) for d in range(1, 4)]
    line_z = [device_at(d, 0, 0, 0) for d in range(1, 4)]
    pairs_x = [device_at(0, 0, d, c) for d in range(4) for c in range(2) if d or c]
    for other in pairs_x + line_y + line_z:
        pl.semaphore_signal(barrier, inc=1, device_id=(other,), device_id_type=MESH)

    def meet(at, others):
        for other in others:
            pl.semaphore_signal(meet_sem.at[at], inc=1, device_id=(other,), device_id_type=MESH)

    for load in loads:
        load.wait()
    field0[0:TRACE, :] = right_ref[...]
    field0[TRACE:ROWS, :] = jnp.zeros((ROWS - TRACE, F_DEV), jnp.float32)
    diag[...] = mass_ref[...] + absorb_ref[...].astype(jnp.float32) * imped_ref[...]
    for k in range(4):
        @pl.when(jnp.logical_not(inside_from[k]))
        def _():
            for turn in range(2):
                ghost_buf[turn, k] = jnp.zeros((ROWS, GH), jnp.float32)
        @pl.when(jnp.logical_not(inside_to[k]))
        def _():
            for turn in range(2):
                back_buf[turn, k] = jnp.zeros((ROWS, GH), jnp.float32)

    lane = lax.broadcasted_iota(jnp.int32, (ROWS, GH), 1)
    alive = [lane < count_ref[0, k] for k in range(4)]

    def own_blocks(ref):
        return [
            lambda i, b=b: ref[8 * i:8 * i + 8, b * LANES:(b + 1) * LANES] for b in range(F_DEV // LANES)
        ]

    def out_copy(turn, k):
        return pltpu.make_async_remote_copy(
            src_ref=out_buf.at[turn, k], dst_ref=ghost_buf.at[turn, k],
            send_sem=out_send.at[turn, k], recv_sem=out_recv.at[turn, k],
            device_id=(me + OFFSETS[k],), device_id_type=MESH,
        )

    def part_copy(turn, k):
        return pltpu.make_async_remote_copy(
            src_ref=part_buf.at[turn, k], dst_ref=back_buf.at[turn, k],
            send_sem=part_send.at[turn, k], recv_sem=part_recv.at[turn, k],
            device_id=(me - OFFSETS[k],), device_id_type=MESH,
        )

    def send_out(turn, ref):
        blocks = own_blocks(ref)
        for k in range(4):
            gone = lane_pick(blocks, share_ref[k:k + 1, :])
            out_buf[turn, k] = jnp.where(alive[k], gone, 0.0)
        if turn == 0:
            pl.semaphore_wait(barrier, arrivals)
        for k in range(4):
            @pl.when(inside_to[k])
            def _():
                out_copy(turn, k).start()

    def await_out(turn):
        for k in range(4):
            @pl.when(inside_from[k])
            def _():
                out_copy(turn, k).wait_recv()

    def send_part(turn):
        for k in range(4):
            @pl.when(inside_from[k])
            def _():
                part_copy(turn, k).start()

    def await_part(turn):
        for k in range(4):
            @pl.when(inside_to[k])
            def _():
                part_copy(turn, k).wait_recv()

    def pick_all(turn, ref, store):
        blocks = own_blocks(ref) + [
            lambda i, k=k: ghost_buf[turn, k, 8 * i:8 * i + 8] for k in range(4)
        ]
        for side in range(SIDES):
            for b in range(E_DEV // LANES):
                cols = slice(b * LANES, (b + 1) * LANES)
                store(side, b, lane_pick(blocks, map_ref[side:side + 1, cols]))

    def multiply(picked):
        for b in range(E_DEV // LANES):
            cols = slice(b * LANES, (b + 1) * LANES)
            total = jnp.zeros((DOFS, LANES), jnp.float32)
            for side in range(SIDES):
                def one(c, total):
                    row = picked[side, b, pl.ds(c, 8, stride=0), :]
                    part = widened[side * TRACE + c, :, cols]
                    return total + (part.reshape(DOFS // 8, 8, LANES) * row[None]).reshape(DOFS, LANES)
                total = lax.fori_loop(0, TRACE, one, total, unroll=6)
            for side in range(SIDES):
                product[side, 0:TRACE, cols] = total[side * TRACE:(side + 1) * TRACE]

    def energy(picked):
        total = jnp.zeros((8, LANES), jnp.float32)
        for side in range(SIDES):
            for b in range(E_DEV // LANES):
                cols = slice(b * LANES, (b + 1) * LANES)
                both = picked[side, b] * product[side, :, cols]
                total = total + both[0:8] + both[8:16] + both[16:24]
        return total

    def face_sums(ref):
        square = jnp.zeros((8, LANES), jnp.float32)
        weighted = jnp.zeros((8, LANES), jnp.float32)
        for b in range(F_DEV // LANES):
            value = ref[:, b * LANES:(b + 1) * LANES]
            both = value * value
            both = both[0:8] + both[8:16] + both[16:24]
            square = square + both
            weighted = weighted + both * diag[b:b + 1, :]
        return square, weighted

    def scatter(turn, ref):
        total = jnp.zeros((6 * 2 * ROWS, WIDE), jnp.float32)
        for side in range(SIDES):
            left = spread_rows(product[side], map_ref[side:side + 1, :], 6)
            total = total + nt_dot(left, hot[:, side * E_DEV:(side + 1) * E_DEV])
        for group in range(6):
            base = group * 2 * ROWS
            both = total[base:base + ROWS] + total[base + ROWS:base + 2 * ROWS]
            if group >= 4:
                part_buf[turn, 2 * (group - 4)] = both[:, 0:GH]
                part_buf[turn, 2 * (group - 4) + 1] = both[:, GH:]
            else:
                for half in range(2):
                    b = 2 * group + half
                    cols = slice(b * LANES, (b + 1) * LANES)
                    image[turn, :, cols] = (
                        both[:, half * LANES:(half + 1) * LANES] + diag[b:b + 1, :] * ref[:, cols]
                    )

    def add_back(turn):
        total = jnp.zeros((4 * 2 * ROWS, WIDE), jnp.float32)
        for k in range(4):
            value = jnp.where(alive[k], back_buf[turn, k], 0.0)
            left = spread_rows(value, share_ref[k:k + 1, :], 4)
            total = total + nt_dot(left, hot_share[:, k * GH:(k + 1) * GH])
        for group in range(4):
            base = group * 2 * ROWS
            both = total[base:base + ROWS] + total[base + ROWS:base + 2 * ROWS]
            cols = slice(group * WIDE, (group + 1) * WIDE)
            image[turn, :, cols] = image[turn, :, cols] + both

    others = sorted(
        ((dz, dy, dx, dc) for dz in range(4) for dy in range(4) for dx in range(4) for dc in range(2) if dz or dy or dx or dc),
        key=lambda at: -sum(min(d, 4 - d) for d in at[:3]),
    )

    def sum_start(turn, square, weighted):
        lane_at = lax.broadcasted_iota(jnp.int32, (1, LANES), 1)
        first = jnp.sum(square, axis=0, keepdims=True)
        second = jnp.sum(weighted, axis=0, keepdims=True)
        first = first + pltpu.roll(first, LANES // 2, 1)
        second = second + pltpu.roll(second, LANES // 2, 1)
        row = jnp.where(lane_at < LANES // 2, first, second)
        sum_buf[turn] = row
        sum_in[turn, me] = row
        for at in others:
            pltpu.make_async_remote_copy(
                src_ref=sum_buf.at[turn], dst_ref=sum_in.at[turn, me],
                send_sem=sum_send.at[turn], recv_sem=sum_recv.at[turn],
                device_id=(device_at(*at),), device_id_type=MESH,
            ).start()

    def sum_whole(turn, sem):
        return pltpu.make_async_copy(
            sum_in.at[turn, pl.ds(0, N_DOM - 1)], sum_in.at[turn, pl.ds(1, N_DOM - 1)], sem.at[turn]
        )

    def sum_finish(turn):
        sum_whole(turn, sum_recv).wait()
        total = jnp.sum(sum_in[turn], axis=0)
        lane_at = lax.broadcasted_iota(jnp.int32, (1, LANES), 1)
        first = jnp.sum(jnp.where(lane_at < LANES // 2, total, 0.0), axis=1, keepdims=True)
        second = jnp.sum(jnp.where(lane_at < LANES // 2, 0.0, total), axis=1, keepdims=True)
        return first, second

    def clear_tail(ref):
        for side in range(SIDES):
            ref[side, TRACE:ROWS, :] = jnp.zeros((ROWS - TRACE, E_DEV), jnp.float32)

    send_out(0, field0)
    meet(0, line_y)
    clear_tail(product)
    for side in range(SIDES):
        hot[:, side * E_DEV:(side + 1) * E_DEV] = one_hot_low(map_ref[side:side + 1, :])
    for k in range(4):
        hot_share[:, k * GH:(k + 1) * GH] = one_hot_low(share_ref[k:k + 1, :])
    square, weighted = face_sums(field0)
    pl.semaphore_wait(meet_sem.at[0], 3)
    meet(1, line_z)
    matrix_copy.wait()

    def widen(row, carry):
        widened[row] = matrix[row].astype(jnp.float32)
        return carry

    lax.fori_loop(0, DOFS, widen, 0, unroll=4)
    pl.semaphore_wait(meet_sem.at[1], 3)
    await_out(0)

    def keep0(side, b, value):
        picked0[side, b] = value

    pick_all(0, field0, keep0)
    multiply(picked0)
    square0, weighted0 = square, weighted + energy(picked0)
    scatter(0, field0)
    send_part(0)
    sum_start(0, square0, weighted0)
    await_part(0)
    add_back(0)
    send_out(1, image.at[0])
    norm0, curve0 = sum_finish(0)
    step0 = norm0 / curve0
    for b in range(F_DEV // LANES):
        cols = slice(b * LANES, (b + 1) * LANES)
        field1[:, cols] = field0[:, cols] - step0 * image[0, :, cols]
    square, weighted = face_sums(field1)
    await_out(1)

    def keep1(side, b, value):
        picked1[side, b] = picked0[side, b] - step0 * value

    pick_all(1, image.at[0], keep1)
    multiply(picked1)
    sum_start(1, square, weighted + energy(picked1))
    scatter(1, field1)
    send_part(1)
    await_part(1)
    add_back(1)
    norm1, curve1 = sum_finish(1)
    ratio = norm1 / norm0
    step1 = norm1 / (curve1 - ratio * norm1 / step0)
    lead = step0 + step1 * ratio
    for b in range(F_DEV // LANES):
        cols = slice(b * LANES, (b + 1) * LANES)
        lead_ref[:, cols] = lead * field0[0:TRACE, cols]
        later_ref[:, cols] = field1[0:TRACE, cols]
        along_ref[:, cols] = image[1, 0:TRACE, cols] + ratio * image[0, 0:TRACE, cols]
    step_ref[...] = jnp.broadcast_to(step1, (TRACE, F_DEV))

    for turn in range(2):
        for k in range(4):
            @pl.when(inside_to[k])
            def _():
                out_copy(turn, k).wait_send()
            @pl.when(inside_from[k])
            def _():
                part_copy(turn, k).wait_send()
        sum_whole(turn, sum_send).wait()


def shards(right_side, element_matrix, face_map, share_index, share_count, face_mass, absorbing, impedance):
    hbm = pl.BlockSpec(memory_space=pltpu.HBM)
    f32, bf16, i32 = jnp.float32, jnp.bfloat16, jnp.int32
    out = pltpu.VMEM((TRACE, F_DEV), f32)
    vmem = pl.BlockSpec(memory_space=pltpu.VMEM)
    lead, later, along, step = pl.pallas_call(
        kernel,
        name="trace_cg",
        out_shape=(out, out, out, out),
        in_specs=[hbm] * 8,
        out_specs=(vmem, vmem, vmem, vmem),
        scratch_shapes=[
            pltpu.VMEM((TRACE, F_DEV), f32),
            pltpu.VMEM((SIDES, E_DEV), i32),
            pltpu.VMEM((4, GH), i32),
            pltpu.SMEM((1, 4), i32),
            pltpu.VMEM((8, LANES), f32),
            pltpu.VMEM((8, LANES), i32),
            pltpu.VMEM((8, LANES), f32),
            pltpu.SemaphoreType.DMA((7,)),
            pltpu.SemaphoreType.REGULAR((2,)),
            pltpu.VMEM((DOFS, DOFS, E_DEV), bf16),
            pltpu.VMEM((DOFS, DOFS, E_DEV), f32),
            pltpu.VMEM((ROWS, F_DEV), f32),
            pltpu.VMEM((ROWS, F_DEV), f32),
            pltpu.VMEM((2, ROWS, F_DEV), f32),
            pltpu.VMEM((8, LANES), f32),
            pltpu.VMEM((SIDES, 4, ROWS, LANES), f32),
            pltpu.VMEM((SIDES, 4, ROWS, LANES), f32),
            pltpu.VMEM((SIDES, ROWS, E_DEV), f32),
            pltpu.VMEM((WIDE, SIDES * E_DEV), bf16),
            pltpu.VMEM((WIDE, 4 * GH), bf16),
            pltpu.VMEM((2, 4, ROWS, GH), f32),
            pltpu.VMEM((2, 4, ROWS, GH), f32),
            pltpu.VMEM((2, 4, ROWS, GH), f32),
            pltpu.VMEM((2, 4, ROWS, GH), f32),
            pltpu.VMEM((2, 1, LANES), f32),
            pltpu.VMEM((2, N_DOM, 1, LANES), f32),
            pltpu.SemaphoreType.DMA,
            pltpu.SemaphoreType.DMA((2, 4)),
            pltpu.SemaphoreType.DMA((2, 4)),
            pltpu.SemaphoreType.DMA((2, 4)),
            pltpu.SemaphoreType.DMA((2, 4)),
            pltpu.SemaphoreType.DMA((2,)),
            pltpu.SemaphoreType.DMA((2,)),
        ],
        compiler_params=pltpu.CompilerParams(
            collective_id=0, has_side_effects=True, vmem_limit_bytes=65 * 1000 * 1000
        ),
    )(
        right_side, element_matrix, face_map, share_index.reshape(4, GH), share_count,
        face_mass.reshape(8, LANES), absorbing.reshape(8, LANES), impedance.reshape(8, LANES),
    )
    return lead + step * later, later - step * along


def solution(mesh):
    in_specs = (
        P(None, "dom"), P(None, None, "dom"), P(None, "dom"), P("dom", None, None),
        P("dom", None), P("dom"), P("dom"), P("dom"),
    )
    return jax.shard_map(
        shards, mesh=mesh, in_specs=in_specs,
        out_specs=(P(None, "dom"), P(None, "dom")), check_vma=False,
    )
```

```python
import functools

import jax
import jax.numpy as jnp
from jax import lax
from jax.experimental import pallas as pl
from jax.experimental.pallas import tpu as pltpu
from jax.sharding import PartitionSpec as P

TRACE = 18
ROWS = 24
SIDES = 4
DOFS = 72
E_DEV = 512
F_DEV = 1024
GH = 128
OFFSETS = (-2, -1, 1, 2)
N_DOM = 128
LANES = 128
WIDE = 256
MESH = pl.DeviceIdType.MESH


def lane_pick(blocks, index_row, first, base):
    low = jnp.broadcast_to(index_row & (LANES - 1), (8, LANES))
    high = jnp.broadcast_to(index_row >> 7, (8, LANES))
    masks = [high == first + at for at in range(len(blocks))]
    pieces = []
    for i in range(ROWS // 8):
        picked = jnp.zeros((8, LANES), jnp.float32) if base is None else base(i)
        for mask, block in zip(masks, blocks):
            moved = jnp.take_along_axis(block(i), low, axis=1, mode="promise_in_bounds")
            picked = jnp.where(mask, moved, picked)
        pieces.append(picked)
    return jnp.concatenate(pieces, axis=0)


def split_two(value):
    head = value.astype(jnp.bfloat16)
    tail = (value - head.astype(jnp.float32)).astype(jnp.bfloat16)
    return head.astype(jnp.float32), tail.astype(jnp.float32)


def spread_rows(value, index_row, groups):
    head, tail = split_two(value)
    high = jnp.broadcast_to(index_row >> 8, value.shape)
    pieces = []
    for group in groups:
        mask = high == group
        pieces.append(jnp.where(mask, head, 0.0))
        pieces.append(jnp.where(mask, tail, 0.0))
    return jnp.concatenate(pieces, axis=0).astype(jnp.bfloat16)


def one_hot_low(index_row):
    low = (index_row & (WIDE - 1)).astype(jnp.float32)
    column = jnp.broadcast_to(low, (LANES, LANES)).T
    lane = lax.broadcasted_iota(jnp.int32, (LANES, LANES), 1).astype(jnp.float32)
    halves = [jnp.where(column == lane + half * LANES, 1.0, 0.0) for half in range(2)]
    return jnp.concatenate(halves, axis=1).astype(jnp.bfloat16)


def wide_dot(left, right):
    return jnp.dot(left, right, preferred_element_type=jnp.float32)


def kernel(
    right_hbm, matrix_hbm, map_hbm, share_hbm, count_hbm, mass_hbm, absorb_hbm, imped_hbm,
    lead_ref, later_ref, along_ref, step_ref,
    right_ref, map_ref, share_ref, count_ref, mass_ref, absorb_ref, imped_ref, load_sem, meet_sem,
    matrix, widened, field0, field1, image, diag, picked0, picked1, product, hot, hot_share,
    out_buf, ghost_buf, part_buf, back_buf, sum_buf, sum_in,
    matrix_sem, out_send, out_recv, part_send, part_recv, sum_send, sum_recv,
):
    me = lax.axis_index("dom")
    loads = [
        pltpu.make_async_copy(source, target, load_sem.at[at])
        for at, (source, target) in enumerate((
            (share_hbm, share_ref), (count_hbm, count_ref), (right_hbm, right_ref), (map_hbm, map_ref),
            (mass_hbm, mass_ref), (absorb_hbm, absorb_ref), (imped_hbm, imped_ref),
        ))
    ]
    for load in loads:
        load.start()
    matrix_copy = pltpu.make_async_copy(matrix_hbm, matrix, matrix_sem)
    matrix_copy.start()

    core = lax.rem(me, 2)
    at_x = lax.rem(me // 2, 4)
    at_y = lax.rem(me // 8, 4)
    at_z = me // 32

    along_x = [lax.rem(at_x + d, 4) * 2 for d in range(4)]
    along_y = [lax.rem(at_y + d, 4) * 8 for d in range(4)]
    along_z = [lax.rem(at_z + d, 4) * 32 for d in range(4)]
    cores = (core, 1 - core)

    def device_at(dz, dy, dx, dc):
        return along_z[dz] + along_y[dy] + along_x[dx] + cores[dc]

    inside_to = [(me + o >= 0) & (me + o < N_DOM) for o in OFFSETS]
    inside_from = [(me - o >= 0) & (me - o < N_DOM) for o in OFFSETS]

    barrier = pltpu.get_barrier_semaphore()
    arrivals = jnp.int32(13)
    for k, o in enumerate(OFFSETS):
        @pl.when(inside_to[k])
        def _():
            pl.semaphore_signal(barrier, inc=1, device_id=(me + o,), device_id_type=MESH)
        arrivals = arrivals + inside_from[k].astype(jnp.int32)
    line_y = [device_at(0, d, 0, 0) for d in range(1, 4)]
    line_z = [device_at(d, 0, 0, 0) for d in range(1, 4)]
    pairs_x = [device_at(0, 0, d, c) for d in range(4) for c in range(2) if d or c]
    for other in pairs_x + line_y + line_z:
        pl.semaphore_signal(barrier, inc=1, device_id=(other,), device_id_type=MESH)

    def meet(at, others):
        for other in others:
            pl.semaphore_signal(meet_sem.at[at], inc=1, device_id=(other,), device_id_type=MESH)

    for load in loads:
        load.wait()
    field0[0:TRACE, :] = right_ref[...]
    field0[TRACE:ROWS, :] = jnp.zeros((ROWS - TRACE, F_DEV), jnp.float32)
    diag[...] = mass_ref[...] + absorb_ref[...].astype(jnp.float32) * imped_ref[...]
    for k in range(4):
        @pl.when(jnp.logical_not(inside_from[k]))
        def _():
            for turn in range(2):
                ghost_buf[turn, k] = jnp.zeros((ROWS, GH), jnp.float32)
        @pl.when(jnp.logical_not(inside_to[k]))
        def _():
            for turn in range(2):
                back_buf[turn, k] = jnp.zeros((ROWS, GH), jnp.float32)

    lane = lax.broadcasted_iota(jnp.int32, (ROWS, GH), 1)
    alive = [lane < count_ref[0, k] for k in range(4)]

    def own_blocks(ref):
        return [
            lambda i, b=b: ref[8 * i:8 * i + 8, b * LANES:(b + 1) * LANES] for b in range(F_DEV // LANES)
        ]

    def out_copy(turn, k):
        return pltpu.make_async_remote_copy(
            src_ref=out_buf.at[turn, k], dst_ref=ghost_buf.at[turn, k],
            send_sem=out_send.at[turn, k], recv_sem=out_recv.at[turn, k],
            device_id=(me + OFFSETS[k],), device_id_type=MESH,
        )

    def part_copy(turn, k):
        return pltpu.make_async_remote_copy(
            src_ref=part_buf.at[turn, k], dst_ref=back_buf.at[turn, k],
            send_sem=part_send.at[turn, k], recv_sem=part_recv.at[turn, k],
            device_id=(me - OFFSETS[k],), device_id_type=MESH,
        )

    def send_out(turn, ref):
        blocks = own_blocks(ref)
        for k in range(4):
            gone = lane_pick(blocks, share_ref[k:k + 1, :], 0, None)
            out_buf[turn, k] = jnp.where(alive[k], gone, 0.0)
        if turn == 0:
            pl.semaphore_wait(barrier, arrivals)
        for k in range(4):
            @pl.when(inside_to[k])
            def _():
                out_copy(turn, k).start()

    def await_out(turn):
        for k in range(4):
            @pl.when(inside_from[k])
            def _():
                out_copy(turn, k).wait_recv()

    def send_part(turn):
        for k in range(4):
            @pl.when(inside_from[k])
            def _():
                part_copy(turn, k).start()

    def await_part(turn):
        for k in range(4):
            @pl.when(inside_to[k])
            def _():
                part_copy(turn, k).wait_recv()

    def pick_own(ref, picked):
        blocks = own_blocks(ref)
        for side in range(SIDES):
            for b in range(E_DEV // LANES):
                cols = slice(b * LANES, (b + 1) * LANES)
                picked[side, b] = lane_pick(blocks, map_ref[side:side + 1, cols], 0, None)

    def pick_ghost(turn, picked, finish):
        blocks = [lambda i, k=k: ghost_buf[turn, k, 8 * i:8 * i + 8] for k in range(4)]
        for side in range(SIDES):
            for b in range(E_DEV // LANES):
                cols = slice(b * LANES, (b + 1) * LANES)
                base = lambda i, side=side, b=b: picked[side, b, 8 * i:8 * i + 8]
                value = lane_pick(blocks, map_ref[side:side + 1, cols], F_DEV // LANES, base)
                picked[side, b] = finish(side, b, value)

    def multiply(picked):
        energy = jnp.zeros((TRACE, LANES), jnp.float32)
        for b in range(E_DEV // LANES):
            cols = slice(b * LANES, (b + 1) * LANES)

            def one(side, total, b=b):
                for c in range(TRACE):
                    row = picked[side, b, c:c + 1, :]
                    total = total + widened[b, side * TRACE + c] * row
                return total

            total = lax.fori_loop(0, SIDES, one, jnp.zeros((DOFS, LANES), jnp.float32))
            for side in range(SIDES):
                piece = total[side * TRACE:(side + 1) * TRACE]
                product[side, 0:TRACE, cols] = piece
                energy = energy + piece * picked[side, b, 0:TRACE, :]
        return jnp.sum(energy, axis=0, keepdims=True)

    def face_sums(ref):
        square = jnp.zeros((8, LANES), jnp.float32)
        weighted = jnp.zeros((8, LANES), jnp.float32)
        for b in range(F_DEV // LANES):
            value = ref[:, b * LANES:(b + 1) * LANES]
            both = value * value
            both = both[0:8] + both[8:16] + both[16:24]
            square = square + both
            weighted = weighted + both * diag[b:b + 1, :]
        return jnp.sum(square, axis=0, keepdims=True), jnp.sum(weighted, axis=0, keepdims=True)

    def scatter(groups):
        total = jnp.zeros((len(groups) * 2 * ROWS, WIDE), jnp.float32)
        for side in range(SIDES):
            left = spread_rows(product[side], map_ref[side:side + 1, :], groups)
            total = total + wide_dot(left, hot[side * E_DEV:(side + 1) * E_DEV, :])
        for at in range(len(groups)):
            base = at * 2 * ROWS
            yield total[base:base + ROWS] + total[base + ROWS:base + 2 * ROWS]

    def scatter_ghost(turn):
        for at, both in enumerate(scatter((4, 5))):
            part_buf[turn, 2 * at] = both[:, 0:GH]
            part_buf[turn, 2 * at + 1] = both[:, GH:]

    def scatter_own(turn, ref):
        for at, both in enumerate(scatter((0, 1, 2, 3))):
            for half in range(2):
                b = 2 * at + half
                cols = slice(b * LANES, (b + 1) * LANES)
                image[turn, :, cols] = both[:, half * LANES:(half + 1) * LANES] + diag[b:b + 1, :] * ref[:, cols]

    def add_back(turn):
        total = jnp.zeros((4 * 2 * ROWS, WIDE), jnp.float32)
        for k in range(4):
            value = jnp.where(alive[k], back_buf[turn, k], 0.0)
            left = spread_rows(value, share_ref[k:k + 1, :], (0, 1, 2, 3))
            total = total + wide_dot(left, hot_share[k * GH:(k + 1) * GH, :])
        for group in range(4):
            base = group * 2 * ROWS
            both = total[base:base + ROWS] + total[base + ROWS:base + 2 * ROWS]
            cols = slice(group * WIDE, (group + 1) * WIDE)
            image[turn, :, cols] = image[turn, :, cols] + both

    others = sorted(
        ((dz, dy, dx, dc) for dz in range(4) for dy in range(4) for dx in range(4) for dc in range(2) if dz or dy or dx or dc),
        key=lambda at: -sum(min(d, 4 - d) for d in at[:3]),
    )

    def sum_start(turn, first, second):
        lane_at = lax.broadcasted_iota(jnp.int32, (1, LANES), 1)
        first = first + pltpu.roll(first, LANES // 2, 1)
        second = second + pltpu.roll(second, LANES // 2, 1)
        row = jnp.where(lane_at < LANES // 2, first, second)
        sum_buf[turn] = row
        sum_in[turn, me] = row
        for at in others:
            pltpu.make_async_remote_copy(
                src_ref=sum_buf.at[turn], dst_ref=sum_in.at[turn, me],
                send_sem=sum_send.at[turn], recv_sem=sum_recv.at[turn],
                device_id=(device_at(*at),), device_id_type=MESH,
            ).start()

    def sum_whole(turn, sem):
        return pltpu.make_async_copy(
            sum_in.at[turn, pl.ds(0, N_DOM - 1)], sum_in.at[turn, pl.ds(1, N_DOM - 1)], sem.at[turn]
        )

    def sum_finish(turn):
        sum_whole(turn, sum_recv).wait()
        total = jnp.sum(sum_in[turn], axis=0)
        lane_at = lax.broadcasted_iota(jnp.int32, (1, LANES), 1)
        first = jnp.sum(jnp.where(lane_at < LANES // 2, total, 0.0), axis=1, keepdims=True)
        second = jnp.sum(jnp.where(lane_at < LANES // 2, 0.0, total), axis=1, keepdims=True)
        return first, second

    def clear_tail(ref):
        for side in range(SIDES):
            ref[side, TRACE:ROWS, :] = jnp.zeros((ROWS - TRACE, E_DEV), jnp.float32)

    send_out(0, field0)
    meet(0, line_y)
    clear_tail(product)
    for side in range(SIDES):
        for b in range(E_DEV // LANES):
            first = side * E_DEV + b * LANES
            hot[first:first + LANES, :] = one_hot_low(map_ref[side:side + 1, b * LANES:(b + 1) * LANES])
    for k in range(4):
        hot_share[k * GH:(k + 1) * GH, :] = one_hot_low(share_ref[k:k + 1, :])
    square, weighted = face_sums(field0)
    pl.semaphore_wait(meet_sem.at[0], 3)
    meet(1, line_z)
    matrix_copy.wait()

    def widen(row, carry):
        whole = matrix[row].astype(jnp.float32)
        for b in range(E_DEV // LANES):
            widened[b, row] = whole[:, b * LANES:(b + 1) * LANES]
        return carry

    pick_own(field0, picked0)
    lax.fori_loop(0, DOFS, widen, 0, unroll=2)
    pl.semaphore_wait(meet_sem.at[1], 3)
    await_out(0)

    pick_ghost(0, picked0, lambda side, b, value: value)
    weighted = weighted + multiply(picked0)
    scatter_ghost(0)
    send_part(0)
    sum_start(0, square, weighted)
    scatter_own(0, field0)
    await_part(0)
    add_back(0)
    send_out(1, image.at[0])
    pick_own(image.at[0], picked1)
    norm0, curve0 = sum_finish(0)
    step0 = norm0 / curve0
    for b in range(F_DEV // LANES):
        cols = slice(b * LANES, (b + 1) * LANES)
        field1[:, cols] = field0[:, cols] - step0 * image[0, :, cols]
    square, weighted = face_sums(field1)
    await_out(1)
    pick_ghost(1, picked1, lambda side, b, value: picked0[side, b] - step0 * value)
    sum_start(1, square, weighted + multiply(picked1))
    scatter_ghost(1)
    send_part(1)
    scatter_own(1, field1)
    await_part(1)
    add_back(1)
    norm1, curve1 = sum_finish(1)
    ratio = norm1 / norm0
    step1 = norm1 / (curve1 - ratio * norm1 / step0)
    lead = step0 + step1 * ratio
    for b in range(F_DEV // LANES):
        cols = slice(b * LANES, (b + 1) * LANES)
        lead_ref[:, cols] = lead * field0[0:TRACE, cols]
        later_ref[:, cols] = field1[0:TRACE, cols]
        along_ref[:, cols] = image[1, 0:TRACE, cols] + ratio * image[0, 0:TRACE, cols]
    step_ref[...] = jnp.broadcast_to(step1, (TRACE, F_DEV))

    for turn in range(2):
        for k in range(4):
            @pl.when(inside_to[k])
            def _():
                out_copy(turn, k).wait_send()
            @pl.when(inside_from[k])
            def _():
                part_copy(turn, k).wait_send()
        sum_whole(turn, sum_send).wait()


def shards(right_side, element_matrix, face_map, share_index, share_count, face_mass, absorbing, impedance):
    hbm = pl.BlockSpec(memory_space=pltpu.HBM)
    f32, bf16, i32 = jnp.float32, jnp.bfloat16, jnp.int32
    out = pltpu.VMEM((TRACE, F_DEV), f32)
    vmem = pl.BlockSpec(memory_space=pltpu.VMEM)
    lead, later, along, step = pl.pallas_call(
        kernel,
        name="trace_cg",
        out_shape=(out, out, out, out),
        in_specs=[hbm] * 8,
        out_specs=(vmem, vmem, vmem, vmem),
        scratch_shapes=[
            pltpu.VMEM((TRACE, F_DEV), f32),
            pltpu.VMEM((SIDES, E_DEV), i32),
            pltpu.VMEM((4, GH), i32),
            pltpu.SMEM((1, 4), i32),
            pltpu.VMEM((8, LANES), f32),
            pltpu.VMEM((8, LANES), i32),
            pltpu.VMEM((8, LANES), f32),
            pltpu.SemaphoreType.DMA((7,)),
            pltpu.SemaphoreType.REGULAR((2,)),
            pltpu.VMEM((DOFS, DOFS, E_DEV), bf16),
            pltpu.VMEM((E_DEV // LANES, DOFS, DOFS, LANES), f32),
            pltpu.VMEM((ROWS, F_DEV), f32),
            pltpu.VMEM((ROWS, F_DEV), f32),
            pltpu.VMEM((2, ROWS, F_DEV), f32),
            pltpu.VMEM((8, LANES), f32),
            pltpu.VMEM((SIDES, 4, ROWS, LANES), f32),
            pltpu.VMEM((SIDES, 4, ROWS, LANES), f32),
            pltpu.VMEM((SIDES, ROWS, E_DEV), f32),
            pltpu.VMEM((SIDES * E_DEV, WIDE), bf16),
            pltpu.VMEM((4 * GH, WIDE), bf16),
            pltpu.VMEM((2, 4, ROWS, GH), f32),
            pltpu.VMEM((2, 4, ROWS, GH), f32),
            pltpu.VMEM((2, 4, ROWS, GH), f32),
            pltpu.VMEM((2, 4, ROWS, GH), f32),
            pltpu.VMEM((2, 1, LANES), f32),
            pltpu.VMEM((2, N_DOM, 1, LANES), f32),
            pltpu.SemaphoreType.DMA,
            pltpu.SemaphoreType.DMA((2, 4)),
            pltpu.SemaphoreType.DMA((2, 4)),
            pltpu.SemaphoreType.DMA((2, 4)),
            pltpu.SemaphoreType.DMA((2, 4)),
            pltpu.SemaphoreType.DMA((2,)),
            pltpu.SemaphoreType.DMA((2,)),
        ],
        compiler_params=pltpu.CompilerParams(
            collective_id=0, has_side_effects=True, vmem_limit_bytes=65 * 1000 * 1000
        ),
    )(
        right_side, element_matrix, face_map, share_index.reshape(4, GH), share_count,
        face_mass.reshape(8, LANES), absorbing.reshape(8, LANES), impedance.reshape(8, LANES),
    )
    return lead + step * later, later - step * along


def solution(mesh):
    in_specs = (
        P(None, "dom"), P(None, None, "dom"), P(None, "dom"), P("dom", None, None),
        P("dom", None), P("dom"), P("dom"), P("dom"),
    )
    return jax.shard_map(
        shards, mesh=mesh, in_specs=in_specs,
        out_specs=(P(None, "dom"), P(None, "dom")), check_vma=False,
    )
```

```python
import functools

import jax
import jax.numpy as jnp
from jax import lax
from jax.experimental import pallas as pl
from jax.experimental.pallas import tpu as pltpu
from jax.sharding import PartitionSpec as P

TRACE = 18
ROWS = 24
SIDES = 4
DOFS = 72
E_DEV = 512
F_DEV = 1024
GH = 128
OFFSETS = (-2, -1, 1, 2)
N_DOM = 128
LANES = 128
WIDE = 256
MESH = pl.DeviceIdType.MESH


def lane_pick(blocks, index_row, first, base):
    low = jnp.broadcast_to(index_row & (LANES - 1), (8, LANES))
    high = jnp.broadcast_to(index_row >> 7, (8, LANES))
    masks = [high == first + at for at in range(len(blocks))]
    pieces = []
    for i in range(ROWS // 8):
        picked = jnp.zeros((8, LANES), jnp.float32) if base is None else base(i)
        for mask, block in zip(masks, blocks):
            moved = jnp.take_along_axis(block(i), low, axis=1, mode="promise_in_bounds")
            picked = jnp.where(mask, moved, picked)
        pieces.append(picked)
    return jnp.concatenate(pieces, axis=0)


def split_two(value):
    head = value.astype(jnp.bfloat16)
    tail = (value - head.astype(jnp.float32)).astype(jnp.bfloat16)
    return head.astype(jnp.float32), tail.astype(jnp.float32)


def spread_rows(value, index_row, groups):
    head, tail = split_two(value)
    high = jnp.broadcast_to(index_row >> 8, value.shape)
    pieces = []
    for group in groups:
        mask = high == group
        pieces.append(jnp.where(mask, head, 0.0))
        pieces.append(jnp.where(mask, tail, 0.0))
    return jnp.concatenate(pieces, axis=0).astype(jnp.bfloat16)


def as_column(row):
    return jnp.broadcast_to(row, (LANES, LANES)).T


def one_hot_low(index_row):
    column = as_column((index_row & (WIDE - 1)).astype(jnp.float32))
    lane = lax.broadcasted_iota(jnp.int32, (LANES, LANES), 1).astype(jnp.float32)
    halves = [jnp.where(column == lane + half * LANES, 1.0, 0.0) for half in range(2)]
    return jnp.concatenate(halves, axis=1).astype(jnp.bfloat16)


def stacked(blocks):
    pairs = [split_two(block) for block in blocks]
    return jnp.concatenate([jnp.concatenate(pair, axis=0) for pair in pairs], axis=1).astype(jnp.bfloat16)


def wide_dot(left, right):
    return jnp.dot(left, right, preferred_element_type=jnp.float32)


def kernel(
    right_hbm, matrix_hbm, map_hbm, share_hbm, count_hbm, mass_hbm, absorb_hbm, imped_hbm,
    lead_ref, later_ref, along_ref, step_ref,
    right_ref, map_ref, share_ref, count_ref, mass_ref, absorb_ref, imped_ref, load_sem, meet_sem,
    matrix, widened, field0, field1, image, diag, picked0, picked1, product, hot, hot_share, hot_back, match,
    out_buf, ghost_buf, part_buf, back_buf, cross_buf, ghost_sum, list_out, list_in, sum_buf, sum_in,
    matrix_sem, out_send, out_recv, part_send, part_recv, cross_send, cross_recv, list_send, list_recv, sum_send, sum_recv,
):
    me = lax.axis_index("dom")
    loads = [
        pltpu.make_async_copy(source, target, load_sem.at[at])
        for at, (source, target) in enumerate((
            (share_hbm, share_ref), (count_hbm, count_ref), (right_hbm, right_ref), (map_hbm, map_ref),
            (mass_hbm, mass_ref), (absorb_hbm, absorb_ref), (imped_hbm, imped_ref),
        ))
    ]
    for load in loads:
        load.start()
    matrix_copy = pltpu.make_async_copy(matrix_hbm, matrix, matrix_sem)
    matrix_copy.start()

    core = lax.rem(me, 2)
    at_x = lax.rem(me // 2, 4)
    at_y = lax.rem(me // 8, 4)
    at_z = me // 32

    along_x = [lax.rem(at_x + d, 4) * 2 for d in range(4)]
    along_y = [lax.rem(at_y + d, 4) * 8 for d in range(4)]
    along_z = [lax.rem(at_z + d, 4) * 32 for d in range(4)]
    cores = (core, 1 - core)

    def device_at(dz, dy, dx, dc):
        return along_z[dz] + along_y[dy] + along_x[dx] + cores[dc]

    inside_to = [(me + o >= 0) & (me + o < N_DOM) for o in OFFSETS]
    inside_from = [(me - o >= 0) & (me - o < N_DOM) for o in OFFSETS]
    crosses = sorted(
        ((k, u) for k in range(4) for u in range(4) if k != u), key=lambda at: -abs(OFFSETS[at[1]] - OFFSETS[at[0]])
    )

    def cross_ok(k, u):
        user = me - OFFSETS[k] + OFFSETS[u]
        return inside_from[k] & (user >= 0) & (user < N_DOM)


    barrier = pltpu.get_barrier_semaphore()
    arrivals = jnp.int32(13)
    for k, o in enumerate(OFFSETS):
        @pl.when(inside_to[k])
        def _():
            pl.semaphore_signal(barrier, inc=1, device_id=(me + o,), device_id_type=MESH)
        arrivals = arrivals + inside_from[k].astype(jnp.int32)
    line_y = [device_at(0, d, 0, 0) for d in range(1, 4)]
    line_z = [device_at(d, 0, 0, 0) for d in range(1, 4)]
    pairs_x = [device_at(0, 0, d, c) for d in range(4) for c in range(2) if d or c]
    for other in pairs_x + line_y + line_z:
        pl.semaphore_signal(barrier, inc=1, device_id=(other,), device_id_type=MESH)

    def meet(at, others):
        for other in others:
            pl.semaphore_signal(meet_sem.at[at], inc=1, device_id=(other,), device_id_type=MESH)

    for load in loads:
        load.wait()
    field0[0:TRACE, :] = right_ref[...]
    field0[TRACE:ROWS, :] = jnp.zeros((ROWS - TRACE, F_DEV), jnp.float32)
    diag[...] = mass_ref[...] + absorb_ref[...].astype(jnp.float32) * imped_ref[...]
    for k in range(4):
        @pl.when(jnp.logical_not(inside_from[k]))
        def _():
            for turn in range(2):
                ghost_buf[turn, k] = jnp.zeros((ROWS, GH), jnp.float32)
        @pl.when(jnp.logical_not(inside_to[k]))
        def _():
            for turn in range(2):
                back_buf[turn, k] = jnp.zeros((ROWS, GH), jnp.float32)
    for k, u in crosses:
        @pl.when(jnp.logical_not(cross_ok(k, u)))
        def _():
            cross_buf[k, u, 0:TRACE] = jnp.zeros((TRACE, GH), jnp.float32)
    for k in range(4):
        @pl.when(jnp.logical_not(inside_from[k]))
        def _():
            list_in[k] = jnp.full((4, GH), -1.0, jnp.float32)
        for u in range(4):
            cross_buf[k, u, TRACE:ROWS] = jnp.zeros((ROWS - TRACE, GH), jnp.float32)

    lane = lax.broadcasted_iota(jnp.int32, (ROWS, GH), 1)
    alive = [lane < count_ref[0, k] for k in range(4)]

    def own_blocks(ref):
        return [
            lambda i, b=b: ref[8 * i:8 * i + 8, b * LANES:(b + 1) * LANES] for b in range(F_DEV // LANES)
        ]

    def out_copy(turn, k):
        return pltpu.make_async_remote_copy(
            src_ref=out_buf.at[turn, k], dst_ref=ghost_buf.at[turn, k],
            send_sem=out_send.at[turn, k], recv_sem=out_recv.at[turn, k],
            device_id=(me + OFFSETS[k],), device_id_type=MESH,
        )

    def list_copy(k):
        return pltpu.make_async_remote_copy(
            src_ref=list_out, dst_ref=list_in.at[k], send_sem=list_send.at[k], recv_sem=list_recv.at[k],
            device_id=(me + OFFSETS[k],), device_id_type=MESH,
        )

    def cross_copy(k, u):
        rows = pl.ds(0, TRACE)
        return pltpu.make_async_remote_copy(
            src_ref=part_buf.at[0, k, rows], dst_ref=cross_buf.at[u, k, rows],
            send_sem=cross_send.at[u, k], recv_sem=cross_recv.at[u, k],
            device_id=(me - OFFSETS[k] + OFFSETS[u],), device_id_type=MESH,
        )

    def part_copy(turn, k):
        return pltpu.make_async_remote_copy(
            src_ref=part_buf.at[turn, k], dst_ref=back_buf.at[turn, k],
            send_sem=part_send.at[turn, k], recv_sem=part_recv.at[turn, k],
            device_id=(me - OFFSETS[k],), device_id_type=MESH,
        )

    def send_out(turn, ref):
        blocks = own_blocks(ref)
        for k in range(4):
            gone = lane_pick(blocks, share_ref[k:k + 1, :], 0, None)
            out_buf[turn, k] = jnp.where(alive[k], gone, 0.0)
        if turn == 0:
            pl.semaphore_wait(barrier, arrivals)
        for k in (0, 3, 1, 2):
            @pl.when(inside_to[k])
            def _():
                out_copy(turn, k).start()
                if turn == 0:
                    list_copy(k).start()

    def await_out(turn):
        for k in range(4):
            @pl.when(inside_from[k])
            def _():
                out_copy(turn, k).wait_recv()
                if turn == 0:
                    list_copy(k).wait_recv()

    def send_part(turn):
        for k in range(4):
            @pl.when(inside_from[k])
            def _():
                part_copy(turn, k).start()

    def send_cross():
        for k, u in crosses:
            @pl.when(cross_ok(k, u))
            def _():
                cross_copy(k, u).start()

    def await_cross():
        for k, u in crosses:
            @pl.when(cross_ok(u, k))
            def _():
                cross_copy(k, u).wait_recv()

    def await_part(turn):
        for k in range(4):
            @pl.when(inside_to[k])
            def _():
                part_copy(turn, k).wait_recv()

    def pick_own(ref, picked):
        blocks = own_blocks(ref)
        for side in range(SIDES):
            for b in range(E_DEV // LANES):
                cols = slice(b * LANES, (b + 1) * LANES)
                picked[side, b] = lane_pick(blocks, map_ref[side:side + 1, cols], 0, None)

    def pick_ghost(ghosts, picked):
        blocks = [lambda i, k=k: ghosts[k, 8 * i:8 * i + 8] for k in range(4)]
        for side in range(SIDES):
            for b in range(E_DEV // LANES):
                cols = slice(b * LANES, (b + 1) * LANES)
                base = lambda i, side=side, b=b: picked[side, b, 8 * i:8 * i + 8]
                picked[side, b] = lane_pick(blocks, map_ref[side:side + 1, cols], F_DEV // LANES, base)

    def multiply(turn, picked):
        for b in range(E_DEV // LANES):
            cols = slice(b * LANES, (b + 1) * LANES)

            def one(side, total, b=b):
                for c in range(TRACE):
                    row = picked[side, b, c:c + 1, :]
                    total = total + widened[b, side * TRACE + c] * row
                return total

            total = lax.fori_loop(0, SIDES, one, jnp.zeros((DOFS, LANES), jnp.float32))
            for side in range(SIDES):
                product[turn, side, 0:TRACE, cols] = total[side * TRACE:(side + 1) * TRACE]

    def energy(step):
        total = jnp.zeros((ROWS, LANES), jnp.float32)
        for side in range(SIDES):
            for b in range(E_DEV // LANES):
                cols = slice(b * LANES, (b + 1) * LANES)
                image_part = product[0, side, :, cols]
                value = picked0[side, b]
                if step is not None:
                    image_part = image_part - step * product[1, side, :, cols]
                    product[1, side, :, cols] = image_part
                    value = value - step * picked1[side, b]
                total = total + value * image_part
        return jnp.sum(total, axis=0, keepdims=True)

    def face_sums(ref):
        square = jnp.zeros((8, LANES), jnp.float32)
        weighted = jnp.zeros((8, LANES), jnp.float32)
        for b in range(F_DEV // LANES):
            value = ref[:, b * LANES:(b + 1) * LANES]
            both = value * value
            both = both[0:8] + both[8:16] + both[16:24]
            square = square + both
            weighted = weighted + both * diag[b:b + 1, :]
        return jnp.sum(square, axis=0, keepdims=True), jnp.sum(weighted, axis=0, keepdims=True)

    def scatter(turn, groups):
        total = jnp.zeros((len(groups) * 2 * ROWS, WIDE), jnp.float32)
        for side in range(SIDES):
            left = spread_rows(product[turn, side], map_ref[side:side + 1, :], groups)
            total = total + wide_dot(left, hot[side * E_DEV:(side + 1) * E_DEV, :])
        for at in range(len(groups)):
            base = at * 2 * ROWS
            yield total[base:base + ROWS] + total[base + ROWS:base + 2 * ROWS]

    def scatter_ghost(turn):
        for at, both in enumerate(scatter(turn, (4, 5))):
            part_buf[turn, 2 * at] = both[:, 0:GH]
            part_buf[turn, 2 * at + 1] = both[:, GH:]

    def scatter_own(turn, ref):
        for at, both in enumerate(scatter(turn, (0, 1, 2, 3))):
            for half in range(2):
                b = 2 * at + half
                cols = slice(b * LANES, (b + 1) * LANES)
                image[turn, :, cols] = both[:, half * LANES:(half + 1) * LANES] + diag[b:b + 1, :] * ref[:, cols]

    def add_back(turn):
        total = jnp.zeros((4 * 2 * ROWS, WIDE), jnp.float32)
        for k in range(4):
            value = jnp.where(alive[k], back_buf[turn, k], 0.0)
            left = spread_rows(value, share_ref[k:k + 1, :], (0, 1, 2, 3))
            total = total + wide_dot(left, hot_share[k * GH:(k + 1) * GH, :])
        for group in range(4):
            base = group * 2 * ROWS
            both = total[base:base + ROWS] + total[base + ROWS:base + 2 * ROWS]
            cols = slice(group * WIDE, (group + 1) * WIDE)
            image[turn, :, cols] = image[turn, :, cols] + both

    others = sorted(
        ((dz, dy, dx, dc) for dz in range(4) for dy in range(4) for dx in range(4) for dc in range(2) if dz or dy or dx or dc),
        key=lambda at: -sum(min(d, 4 - d) for d in at[:3]),
    )

    def sum_start(turn, first, second):
        lane_at = lax.broadcasted_iota(jnp.int32, (1, LANES), 1)
        first = first + pltpu.roll(first, LANES // 2, 1)
        second = second + pltpu.roll(second, LANES // 2, 1)
        row = jnp.where(lane_at < LANES // 2, first, second)
        sum_buf[turn] = row
        sum_in[turn, me] = row
        for at in others:
            pltpu.make_async_remote_copy(
                src_ref=sum_buf.at[turn], dst_ref=sum_in.at[turn, me],
                send_sem=sum_send.at[turn], recv_sem=sum_recv.at[turn],
                device_id=(device_at(*at),), device_id_type=MESH,
            ).start()

    def sum_whole(turn, sem):
        return pltpu.make_async_copy(
            sum_in.at[turn, pl.ds(0, N_DOM - 1)], sum_in.at[turn, pl.ds(1, N_DOM - 1)], sem.at[turn]
        )

    def sum_finish(turn):
        sum_whole(turn, sum_recv).wait()
        total = jnp.sum(sum_in[turn], axis=0)
        lane_at = lax.broadcasted_iota(jnp.int32, (1, LANES), 1)
        first = jnp.sum(jnp.where(lane_at < LANES // 2, total, 0.0), axis=1, keepdims=True)
        second = jnp.sum(jnp.where(lane_at < LANES // 2, 0.0, total), axis=1, keepdims=True)
        return first, second

    def clear_tail(ref):
        for turn in range(2):
            for side in range(SIDES):
                ref[turn, side, TRACE:ROWS, :] = jnp.zeros((ROWS - TRACE, E_DEV), jnp.float32)

    def complete_ghosts():
        for k in range(4):
            left = stacked([part_buf[0, k] if u == k else cross_buf[k, u] for u in range(4)])
            both = wide_dot(left, match[k])
            ghost_sum[k] = ghost_buf[1, k] + both[0:ROWS] + both[ROWS:2 * ROWS]

    def pick_back():
        both = wide_dot(stacked([back_buf[0, k] for k in range(4)]), hot_back[...])
        for side in range(SIDES):
            for b in range(E_DEV // LANES):
                first = side * E_DEV + b * LANES
                part = both[0:ROWS, first:first + LANES] + both[ROWS:2 * ROWS, first:first + LANES]
                picked1[side, b] = picked1[side, b] + part

    lists = [jnp.where(alive[k][0:1], share_ref[k:k + 1, :].astype(jnp.float32), -1.0) for k in range(4)]
    for k in range(4):
        list_out[k:k + 1, :] = lists[k]
    send_out(0, field0)
    meet(0, line_y)
    clear_tail(product)
    for side in range(SIDES):
        for b in range(E_DEV // LANES):
            first = side * E_DEV + b * LANES
            hot[first:first + LANES, :] = one_hot_low(map_ref[side:side + 1, b * LANES:(b + 1) * LANES])
    for k in range(4):
        hot_share[k * GH:(k + 1) * GH, :] = one_hot_low(share_ref[k:k + 1, :])
    square, weighted = face_sums(field0)
    for u in range(4):
        column = as_column(lists[u])
        for side in range(SIDES):
            for b in range(E_DEV // LANES):
                cols = slice(b * LANES, (b + 1) * LANES)
                hit = column == map_ref[side:side + 1, cols].astype(jnp.float32)
                first = side * E_DEV + b * LANES
                hot_back[u * GH:(u + 1) * GH, first:first + LANES] = jnp.where(hit, 1.0, 0.0).astype(jnp.bfloat16)
    pl.semaphore_wait(meet_sem.at[0], 3)
    meet(1, line_z)
    matrix_copy.wait()

    def widen(row, carry):
        whole = matrix[row].astype(jnp.float32)
        for b in range(E_DEV // LANES):
            widened[b, row] = whole[:, b * LANES:(b + 1) * LANES]
        return carry

    pick_own(field0, picked0)
    lax.fori_loop(0, DOFS, widen, 0, unroll=2)
    pl.semaphore_wait(meet_sem.at[1], 3)
    await_out(0)

    pick_ghost(ghost_buf.at[0], picked0)
    multiply(0, picked0)
    scatter_ghost(0)
    send_cross()
    send_part(0)
    scatter_own(0, field0)
    send_out(1, image.at[0])
    sum_start(0, square, weighted + energy(None))
    pick_own(image.at[0], picked1)
    for k in range(4):
        target = jnp.where(list_in[k, k:k + 1, :] < 0.0, -2.0, list_in[k, k:k + 1, :])
        for u in range(4):
            hit = as_column(list_in[k, u:u + 1, :]) == target
            match[k, u * GH:(u + 1) * GH, :] = jnp.where(hit, 1.0, 0.0).astype(jnp.bfloat16)
    await_part(0)
    await_out(1)
    await_cross()
    complete_ghosts()
    pick_back()
    add_back(0)
    pick_ghost(ghost_sum, picked1)
    multiply(1, picked1)
    norm0, curve0 = sum_finish(0)
    step0 = norm0 / curve0
    for b in range(F_DEV // LANES):
        cols = slice(b * LANES, (b + 1) * LANES)
        field1[:, cols] = field0[:, cols] - step0 * image[0, :, cols]
    square, weighted = face_sums(field1)
    sum_start(1, square, weighted + energy(step0))
    scatter_ghost(1)
    send_part(1)
    scatter_own(1, field1)
    await_part(1)
    add_back(1)
    norm1, curve1 = sum_finish(1)
    ratio = norm1 / norm0
    step1 = norm1 / (curve1 - ratio * norm1 / step0)
    lead = step0 + step1 * ratio
    for b in range(F_DEV // LANES):
        cols = slice(b * LANES, (b + 1) * LANES)
        lead_ref[:, cols] = lead * field0[0:TRACE, cols]
        later_ref[:, cols] = field1[0:TRACE, cols]
        along_ref[:, cols] = image[1, 0:TRACE, cols] + ratio * image[0, 0:TRACE, cols]
    step_ref[...] = jnp.broadcast_to(step1, (TRACE, F_DEV))

    for turn in range(2):
        for k in range(4):
            @pl.when(inside_to[k])
            def _():
                out_copy(turn, k).wait_send()
                if turn == 0:
                    list_copy(k).wait_send()
            @pl.when(inside_from[k])
            def _():
                part_copy(turn, k).wait_send()
        sum_whole(turn, sum_send).wait()
    for k, u in crosses:
        @pl.when(cross_ok(k, u))
        def _():
            cross_copy(k, u).wait_send()


def shards(right_side, element_matrix, face_map, share_index, share_count, face_mass, absorbing, impedance):
    hbm = pl.BlockSpec(memory_space=pltpu.HBM)
    f32, bf16, i32 = jnp.float32, jnp.bfloat16, jnp.int32
    out = pltpu.VMEM((TRACE, F_DEV), f32)
    vmem = pl.BlockSpec(memory_space=pltpu.VMEM)
    lead, later, along, step = pl.pallas_call(
        kernel,
        name="trace_cg",
        out_shape=(out, out, out, out),
        in_specs=[hbm] * 8,
        out_specs=(vmem, vmem, vmem, vmem),
        scratch_shapes=[
            pltpu.VMEM((TRACE, F_DEV), f32),
            pltpu.VMEM((SIDES, E_DEV), i32),
            pltpu.VMEM((4, GH), i32),
            pltpu.SMEM((1, 4), i32),
            pltpu.VMEM((8, LANES), f32),
            pltpu.VMEM((8, LANES), i32),
            pltpu.VMEM((8, LANES), f32),
            pltpu.SemaphoreType.DMA((7,)),
            pltpu.SemaphoreType.REGULAR((2,)),
            pltpu.VMEM((DOFS, DOFS, E_DEV), bf16),
            pltpu.VMEM((E_DEV // LANES, DOFS, DOFS, LANES), f32),
            pltpu.VMEM((ROWS, F_DEV), f32),
            pltpu.VMEM((ROWS, F_DEV), f32),
            pltpu.VMEM((2, ROWS, F_DEV), f32),
            pltpu.VMEM((8, LANES), f32),
            pltpu.VMEM((SIDES, 4, ROWS, LANES), f32),
            pltpu.VMEM((SIDES, 4, ROWS, LANES), f32),
            pltpu.VMEM((2, SIDES, ROWS, E_DEV), f32),
            pltpu.VMEM((SIDES * E_DEV, WIDE), bf16),
            pltpu.VMEM((4 * GH, WIDE), bf16),
            pltpu.VMEM((4 * GH, SIDES * E_DEV), bf16),
            pltpu.VMEM((4, 4 * GH, GH), bf16),
            pltpu.VMEM((2, 4, ROWS, GH), f32),
            pltpu.VMEM((2, 4, ROWS, GH), f32),
            pltpu.VMEM((2, 4, ROWS, GH), f32),
            pltpu.VMEM((2, 4, ROWS, GH), f32),
            pltpu.VMEM((4, 4, ROWS, GH), f32),
            pltpu.VMEM((4, ROWS, GH), f32),
            pltpu.VMEM((4, GH), f32),
            pltpu.VMEM((4, 4, GH), f32),
            pltpu.VMEM((2, 1, LANES), f32),
            pltpu.VMEM((2, N_DOM, 1, LANES), f32),
            pltpu.SemaphoreType.DMA,
            pltpu.SemaphoreType.DMA((2, 4)),
            pltpu.SemaphoreType.DMA((2, 4)),
            pltpu.SemaphoreType.DMA((2, 4)),
            pltpu.SemaphoreType.DMA((2, 4)),
            pltpu.SemaphoreType.DMA((4, 4)),
            pltpu.SemaphoreType.DMA((4, 4)),
            pltpu.SemaphoreType.DMA((4,)),
            pltpu.SemaphoreType.DMA((4,)),
            pltpu.SemaphoreType.DMA((2,)),
            pltpu.SemaphoreType.DMA((2,)),
        ],
        compiler_params=pltpu.CompilerParams(
            collective_id=0, has_side_effects=True, vmem_limit_bytes=65 * 1000 * 1000
        ),
    )(
        right_side, element_matrix, face_map, share_index.reshape(4, GH), share_count,
        face_mass.reshape(8, LANES), absorbing.reshape(8, LANES), impedance.reshape(8, LANES),
    )
    return lead + step * later, later - step * along


def solution(mesh):
    in_specs = (
        P(None, "dom"), P(None, None, "dom"), P(None, "dom"), P("dom", None, None),
        P("dom", None), P("dom"), P("dom"), P("dom"),
    )
    return jax.shard_map(
        shards, mesh=mesh, in_specs=in_specs,
        out_specs=(P(None, "dom"), P(None, "dom")), check_vma=False,
    )
```

```python
import functools

import jax
import jax.numpy as jnp
from jax import lax
from jax.experimental import pallas as pl
from jax.experimental.pallas import tpu as pltpu
from jax.sharding import PartitionSpec as P

TRACE = 18
ROWS = 24
SIDES = 4
DOFS = 72
E_DEV = 512
F_DEV = 1024
GH = 128
OFFSETS = (-2, -1, 1, 2)
N_DOM = 128
LANES = 128
WIDE = 256
MESH = pl.DeviceIdType.MESH


def lane_pick(blocks, index_row, first, base):
    low = jnp.broadcast_to(index_row & (LANES - 1), (8, LANES))
    high = jnp.broadcast_to(index_row >> 7, (8, LANES))
    masks = [high == first + at for at in range(len(blocks))]
    pieces = []
    for i in range(ROWS // 8):
        picked = jnp.zeros((8, LANES), jnp.float32) if base is None else base(i)
        for mask, block in zip(masks, blocks):
            moved = jnp.take_along_axis(block(i), low, axis=1, mode="promise_in_bounds")
            picked = jnp.where(mask, moved, picked)
        pieces.append(picked)
    return jnp.concatenate(pieces, axis=0)


def split_two(value):
    head = value.astype(jnp.bfloat16)
    tail = (value - head.astype(jnp.float32)).astype(jnp.bfloat16)
    return head.astype(jnp.float32), tail.astype(jnp.float32)


def spread_rows(value, index_row, groups):
    head, tail = split_two(value)
    high = jnp.broadcast_to(index_row >> 8, value.shape)
    pieces = []
    for group in groups:
        mask = high == group
        pieces.append(jnp.where(mask, head, 0.0))
        pieces.append(jnp.where(mask, tail, 0.0))
    return jnp.concatenate(pieces, axis=0).astype(jnp.bfloat16)


def as_column(row):
    return jnp.broadcast_to(row, (LANES, LANES)).T


def one_hot_low(index_row):
    column = as_column((index_row & (WIDE - 1)).astype(jnp.float32))
    lane = lax.broadcasted_iota(jnp.int32, (LANES, LANES), 1).astype(jnp.float32)
    halves = [jnp.where(column == lane + half * LANES, 1.0, 0.0) for half in range(2)]
    return jnp.concatenate(halves, axis=1).astype(jnp.bfloat16)


def stacked(blocks):
    pairs = [split_two(block) for block in blocks]
    return jnp.concatenate([jnp.concatenate(pair, axis=0) for pair in pairs], axis=1).astype(jnp.bfloat16)


def wide_dot(left, right):
    return jnp.dot(left, right, preferred_element_type=jnp.float32)


def kernel(
    right_hbm, matrix_hbm, map_hbm, share_hbm, count_hbm, mass_hbm, absorb_hbm, imped_hbm,
    lead_ref, later_ref, along_ref, step_ref,
    right_ref, map_ref, share_ref, count_ref, mass_ref, absorb_ref, imped_ref, load_sem, meet_sem,
    matrix, widened, field0, field1, image, diag, picked0, picked1, product, hot, hot_share, hot_back, match,
    out_buf, ghost_in, part_buf, back_in, near_in, ghost_sum, list_out, list_in, sum_buf, sum_in,
    matrix_sem, trade_send, trade_recv, list_send, list_recv, sum_send, sum_recv,
):
    me = lax.axis_index("dom")
    loads = [
        pltpu.make_async_copy(source, target, load_sem.at[at])
        for at, (source, target) in enumerate((
            (share_hbm, share_ref), (count_hbm, count_ref), (right_hbm, right_ref), (map_hbm, map_ref),
            (mass_hbm, mass_ref), (absorb_hbm, absorb_ref), (imped_hbm, imped_ref),
        ))
    ]
    rows18 = pl.ds(0, TRACE)

    def blocks_wait(ref, sem, count, options):
        for n in options:
            @pl.when(count == n)
            def _(n=n):
                some = ref.at[pl.ds(0, n), rows18]
                pltpu.make_async_copy(some, some, sem).wait()

    for load in loads:
        load.start()
    matrix_copy = pltpu.make_async_copy(matrix_hbm, matrix, matrix_sem)
    matrix_copy.start()

    core = lax.rem(me, 2)
    at_x = lax.rem(me // 2, 4)
    at_y = lax.rem(me // 8, 4)
    at_z = me // 32

    along_x = [lax.rem(at_x + d, 4) * 2 for d in range(4)]
    along_y = [lax.rem(at_y + d, 4) * 8 for d in range(4)]
    along_z = [lax.rem(at_z + d, 4) * 32 for d in range(4)]
    cores = (core, 1 - core)

    def device_at(dz, dy, dx, dc):
        return along_z[dz] + along_y[dy] + along_x[dx] + cores[dc]

    inside_to = [(me + o >= 0) & (me + o < N_DOM) for o in OFFSETS]
    inside_from = [(me - o >= 0) & (me - o < N_DOM) for o in OFFSETS]
    crosses = sorted(
        ((k, u) for k in range(4) for u in range(4) if k != u), key=lambda at: -abs(OFFSETS[at[1]] - OFFSETS[at[0]])
    )

    def cross_ok(k, u):
        user = me - OFFSETS[k] + OFFSETS[u]
        return inside_from[k] & (user >= 0) & (user < N_DOM)


    def tally(flags):
        return functools.reduce(lambda total, flag: total + flag.astype(jnp.int32), flags, jnp.int32(0))

    near_to, near_from = tally(inside_to), tally(inside_from)
    all_near = near_to + near_from + tally([cross_ok(k, u) for k, u in crosses])

    barrier = pltpu.get_barrier_semaphore()
    arrivals = jnp.int32(13)
    for k, o in enumerate(OFFSETS):
        @pl.when(inside_to[k])
        def _():
            pl.semaphore_signal(barrier, inc=1, device_id=(me + o,), device_id_type=MESH)
        arrivals = arrivals + inside_from[k].astype(jnp.int32)
    line_y = [device_at(0, d, 0, 0) for d in range(1, 4)]
    line_z = [device_at(d, 0, 0, 0) for d in range(1, 4)]
    pairs_x = [device_at(0, 0, d, c) for d in range(4) for c in range(2) if d or c]
    for other in pairs_x + line_y + line_z:
        pl.semaphore_signal(barrier, inc=1, device_id=(other,), device_id_type=MESH)

    def meet(at, others):
        for other in others:
            pl.semaphore_signal(meet_sem.at[at], inc=1, device_id=(other,), device_id_type=MESH)

    for load in loads:
        load.wait()
    field0[0:TRACE, :] = right_ref[...]
    field0[TRACE:ROWS, :] = jnp.zeros((ROWS - TRACE, F_DEV), jnp.float32)
    diag[...] = mass_ref[...] + absorb_ref[...].astype(jnp.float32) * imped_ref[...]
    blank = jnp.zeros((TRACE, GH), jnp.float32)
    for k in range(4):
        @pl.when(jnp.logical_not(inside_from[k]))
        def _():
            ghost_in[k, 0:TRACE] = blank
            near_in[4 + k, 0:TRACE] = blank
            list_in[k] = jnp.full((4, GH), -1.0, jnp.float32)
        @pl.when(jnp.logical_not(inside_to[k]))
        def _():
            near_in[k, 0:TRACE] = blank
            back_in[k, 0:TRACE] = blank
        for ref in (ghost_in, back_in):
            ref[k, TRACE:ROWS] = jnp.zeros((ROWS - TRACE, GH), jnp.float32)
    for k, u in crosses:
        @pl.when(jnp.logical_not(cross_ok(k, u)))
        def _():
            near_in[8 + 4 * k + u, 0:TRACE] = blank
    for at in range(24):
        near_in[at, TRACE:ROWS] = jnp.zeros((ROWS - TRACE, GH), jnp.float32)

    lane = lax.broadcasted_iota(jnp.int32, (ROWS, GH), 1)
    alive = [lane < count_ref[0, k] for k in range(4)]

    def own_blocks(ref):
        return [
            lambda i, b=b: ref[8 * i:8 * i + 8, b * LANES:(b + 1) * LANES] for b in range(F_DEV // LANES)
        ]

    def trade(turn, source, target, other):
        return pltpu.make_async_remote_copy(
            src_ref=source.at[rows18], dst_ref=target.at[rows18],
            send_sem=trade_send.at[turn], recv_sem=trade_recv.at[turn], device_id=(other,), device_id_type=MESH,
        )

    def out_copy(turn, k):
        return trade(turn, out_buf.at[turn, k], ghost_in.at[k] if turn == 0 else near_in.at[4 + k], me + OFFSETS[k])

    def list_copy(k):
        return pltpu.make_async_remote_copy(
            src_ref=list_out, dst_ref=list_in.at[k], send_sem=list_send, recv_sem=list_recv,
            device_id=(me + OFFSETS[k],), device_id_type=MESH,
        )

    def lists_wait(sem, count):
        for n in (2, 3, 4):
            @pl.when(count == n)
            def _(n=n):
                some = list_in.at[pl.ds(0, n)]
                pltpu.make_async_copy(some, some, sem).wait()

    def cross_copy(k, u):
        return trade(1, part_buf.at[0, k], near_in.at[8 + 4 * u + k], me - OFFSETS[k] + OFFSETS[u])

    def part_copy(turn, k):
        return trade(1 + turn, part_buf.at[turn, k], near_in.at[k] if turn == 0 else back_in.at[k], me - OFFSETS[k])

    trades = (
        (ghost_in, near_to, near_from, (2, 3, 4)),
        (near_in, all_near, all_near, (9, 13, 17, 19, 20)),
        (back_in, near_from, near_to, (2, 3, 4)),
    )

    def trade_wait_recv(turn):
        ref, _, count, options = trades[turn]
        blocks_wait(ref, trade_recv.at[turn], count, options)

    def trade_wait_send(turn):
        ref, count, _, options = trades[turn]
        blocks_wait(ref, trade_send.at[turn], count, options)

    def send_out(turn, ref):
        blocks = own_blocks(ref)
        for k in range(4):
            gone = lane_pick(blocks, share_ref[k:k + 1, :], 0, None)
            out_buf[turn, k] = jnp.where(alive[k], gone, 0.0)
        if turn == 0:
            pl.semaphore_wait(barrier, arrivals)
        for k in (0, 3, 1, 2):
            @pl.when(inside_to[k])
            def _():
                out_copy(turn, k).start()
                if turn == 0:
                    list_copy(k).start()

    def send_part(turn):
        for k in range(4):
            @pl.when(inside_from[k])
            def _():
                part_copy(turn, k).start()

    def send_cross():
        for k, u in crosses:
            @pl.when(cross_ok(k, u))
            def _():
                cross_copy(k, u).start()

    def pick_own(ref, picked):
        blocks = own_blocks(ref)
        for side in range(SIDES):
            for b in range(E_DEV // LANES):
                cols = slice(b * LANES, (b + 1) * LANES)
                picked[side, b] = lane_pick(blocks, map_ref[side:side + 1, cols], 0, None)

    def pick_ghost(ghosts, picked):
        blocks = [lambda i, k=k: ghosts[k, 8 * i:8 * i + 8] for k in range(4)]
        for side in range(SIDES):
            for b in range(E_DEV // LANES):
                cols = slice(b * LANES, (b + 1) * LANES)
                base = lambda i, side=side, b=b: picked[side, b, 8 * i:8 * i + 8]
                picked[side, b] = lane_pick(blocks, map_ref[side:side + 1, cols], F_DEV // LANES, base)

    def multiply(turn, picked):
        for b in range(E_DEV // LANES):
            cols = slice(b * LANES, (b + 1) * LANES)

            def one(side, total, b=b):
                for c in range(TRACE):
                    row = picked[side, b, c:c + 1, :]
                    total = total + widened[b, side * TRACE + c] * row
                return total

            total = lax.fori_loop(0, SIDES, one, jnp.zeros((DOFS, LANES), jnp.float32))
            for side in range(SIDES):
                product[turn, side, 0:TRACE, cols] = total[side * TRACE:(side + 1) * TRACE]

    def energy(step):
        total = jnp.zeros((ROWS, LANES), jnp.float32)
        for side in range(SIDES):
            for b in range(E_DEV // LANES):
                cols = slice(b * LANES, (b + 1) * LANES)
                image_part = product[0, side, :, cols]
                value = picked0[side, b]
                if step is not None:
                    image_part = image_part - step * product[1, side, :, cols]
                    product[1, side, :, cols] = image_part
                    value = value - step * picked1[side, b]
                total = total + value * image_part
        return jnp.sum(total, axis=0, keepdims=True)

    def face_sums(ref):
        square = jnp.zeros((8, LANES), jnp.float32)
        weighted = jnp.zeros((8, LANES), jnp.float32)
        for b in range(F_DEV // LANES):
            value = ref[:, b * LANES:(b + 1) * LANES]
            both = value * value
            both = both[0:8] + both[8:16] + both[16:24]
            square = square + both
            weighted = weighted + both * diag[b:b + 1, :]
        return jnp.sum(square, axis=0, keepdims=True), jnp.sum(weighted, axis=0, keepdims=True)

    def scatter(turn, groups):
        total = jnp.zeros((len(groups) * 2 * ROWS, WIDE), jnp.float32)
        for side in range(SIDES):
            left = spread_rows(product[turn, side], map_ref[side:side + 1, :], groups)
            total = total + wide_dot(left, hot[side * E_DEV:(side + 1) * E_DEV, :])
        for at in range(len(groups)):
            base = at * 2 * ROWS
            yield total[base:base + ROWS] + total[base + ROWS:base + 2 * ROWS]

    def scatter_ghost(turn):
        for at, both in enumerate(scatter(turn, (4, 5))):
            part_buf[turn, 2 * at] = both[:, 0:GH]
            part_buf[turn, 2 * at + 1] = both[:, GH:]

    def scatter_own(turn, ref):
        for at, both in enumerate(scatter(turn, (0, 1, 2, 3))):
            for half in range(2):
                b = 2 * at + half
                cols = slice(b * LANES, (b + 1) * LANES)
                image[turn, :, cols] = both[:, half * LANES:(half + 1) * LANES] + diag[b:b + 1, :] * ref[:, cols]

    def add_back(turn, back):
        total = jnp.zeros((4 * 2 * ROWS, WIDE), jnp.float32)
        for k in range(4):
            value = jnp.where(alive[k], back[k], 0.0)
            left = spread_rows(value, share_ref[k:k + 1, :], (0, 1, 2, 3))
            total = total + wide_dot(left, hot_share[k * GH:(k + 1) * GH, :])
        for group in range(4):
            base = group * 2 * ROWS
            both = total[base:base + ROWS] + total[base + ROWS:base + 2 * ROWS]
            cols = slice(group * WIDE, (group + 1) * WIDE)
            image[turn, :, cols] = image[turn, :, cols] + both

    others = sorted(
        ((dz, dy, dx, dc) for dz in range(4) for dy in range(4) for dx in range(4) for dc in range(2) if dz or dy or dx or dc),
        key=lambda at: -sum(min(d, 4 - d) for d in at[:3]),
    )

    def sum_start(turn, first, second):
        lane_at = lax.broadcasted_iota(jnp.int32, (1, LANES), 1)
        first = first + pltpu.roll(first, LANES // 2, 1)
        second = second + pltpu.roll(second, LANES // 2, 1)
        row = jnp.where(lane_at < LANES // 2, first, second)
        sum_buf[turn] = row
        sum_in[turn, me] = row
        for at in others:
            pltpu.make_async_remote_copy(
                src_ref=sum_buf.at[turn], dst_ref=sum_in.at[turn, me],
                send_sem=sum_send, recv_sem=sum_recv.at[turn],
                device_id=(device_at(*at),), device_id_type=MESH,
            ).start()

    def sum_finish(turn):
        pltpu.make_async_copy(
            sum_in.at[turn, pl.ds(0, N_DOM - 1)], sum_in.at[turn, pl.ds(1, N_DOM - 1)], sum_recv.at[turn]
        ).wait()
        total = jnp.sum(sum_in[turn], axis=0)
        lane_at = lax.broadcasted_iota(jnp.int32, (1, LANES), 1)
        first = jnp.sum(jnp.where(lane_at < LANES // 2, total, 0.0), axis=1, keepdims=True)
        second = jnp.sum(jnp.where(lane_at < LANES // 2, 0.0, total), axis=1, keepdims=True)
        return first, second

    def clear_tail(ref):
        for turn in range(2):
            for side in range(SIDES):
                ref[turn, side, TRACE:ROWS, :] = jnp.zeros((ROWS - TRACE, E_DEV), jnp.float32)

    def complete_ghosts():
        for k in range(4):
            left = stacked([part_buf[0, k] if u == k else near_in[8 + 4 * k + u] for u in range(4)])
            both = wide_dot(left, match[k])
            ghost_sum[k] = near_in[4 + k] + both[0:ROWS] + both[ROWS:2 * ROWS]

    def pick_back():
        both = wide_dot(stacked([near_in[k] for k in range(4)]), hot_back[...])
        for side in range(SIDES):
            for b in range(E_DEV // LANES):
                first = side * E_DEV + b * LANES
                part = both[0:ROWS, first:first + LANES] + both[ROWS:2 * ROWS, first:first + LANES]
                picked1[side, b] = picked1[side, b] + part

    lists = [jnp.where(alive[k][0:1], share_ref[k:k + 1, :].astype(jnp.float32), -1.0) for k in range(4)]
    for k in range(4):
        list_out[k:k + 1, :] = lists[k]
    send_out(0, field0)
    meet(0, line_y)
    clear_tail(product)
    for side in range(SIDES):
        for b in range(E_DEV // LANES):
            first = side * E_DEV + b * LANES
            hot[first:first + LANES, :] = one_hot_low(map_ref[side:side + 1, b * LANES:(b + 1) * LANES])
    for k in range(4):
        hot_share[k * GH:(k + 1) * GH, :] = one_hot_low(share_ref[k:k + 1, :])
    square, weighted = face_sums(field0)
    for u in range(4):
        column = as_column(lists[u])
        for side in range(SIDES):
            for b in range(E_DEV // LANES):
                cols = slice(b * LANES, (b + 1) * LANES)
                hit = column == map_ref[side:side + 1, cols].astype(jnp.float32)
                first = side * E_DEV + b * LANES
                hot_back[u * GH:(u + 1) * GH, first:first + LANES] = jnp.where(hit, 1.0, 0.0).astype(jnp.bfloat16)
    pl.semaphore_wait(meet_sem.at[0], 3)
    meet(1, line_z)
    matrix_copy.wait()

    def widen(row, carry):
        whole = matrix[row].astype(jnp.float32)
        for b in range(E_DEV // LANES):
            widened[b, row] = whole[:, b * LANES:(b + 1) * LANES]
        return carry

    pick_own(field0, picked0)
    lax.fori_loop(0, DOFS, widen, 0, unroll=2)
    pl.semaphore_wait(meet_sem.at[1], 3)
    trade_wait_recv(0)
    lists_wait(list_recv, near_from)

    pick_ghost(ghost_in, picked0)
    multiply(0, picked0)
    scatter_ghost(0)
    send_cross()
    send_part(0)
    scatter_own(0, field0)
    send_out(1, image.at[0])
    sum_start(0, square, weighted + energy(None))
    pick_own(image.at[0], picked1)
    for k in range(4):
        target = jnp.where(list_in[k, k:k + 1, :] < 0.0, -2.0, list_in[k, k:k + 1, :])
        for u in range(4):
            hit = as_column(list_in[k, u:u + 1, :]) == target
            match[k, u * GH:(u + 1) * GH, :] = jnp.where(hit, 1.0, 0.0).astype(jnp.bfloat16)
    trade_wait_recv(1)
    complete_ghosts()
    pick_back()
    add_back(0, near_in)
    pick_ghost(ghost_sum, picked1)
    multiply(1, picked1)
    norm0, curve0 = sum_finish(0)
    step0 = norm0 / curve0
    for b in range(F_DEV // LANES):
        cols = slice(b * LANES, (b + 1) * LANES)
        field1[:, cols] = field0[:, cols] - step0 * image[0, :, cols]
    square, weighted = face_sums(field1)
    sum_start(1, square, weighted + energy(step0))
    scatter_ghost(1)
    send_part(1)
    scatter_own(1, field1)
    trade_wait_recv(2)
    add_back(1, back_in)
    norm1, curve1 = sum_finish(1)
    ratio = norm1 / norm0
    step1 = norm1 / (curve1 - ratio * norm1 / step0)
    lead = step0 + step1 * ratio
    for b in range(F_DEV // LANES):
        cols = slice(b * LANES, (b + 1) * LANES)
        lead_ref[:, cols] = lead * field0[0:TRACE, cols]
        later_ref[:, cols] = field1[0:TRACE, cols]
        along_ref[:, cols] = image[1, 0:TRACE, cols] + ratio * image[0, 0:TRACE, cols]
    step_ref[...] = jnp.broadcast_to(step1, (TRACE, F_DEV))

    for turn in range(3):
        trade_wait_send(turn)
    lists_wait(list_send, near_to)
    pltpu.make_async_copy(
        sum_in.at[:, pl.ds(0, N_DOM - 1)], sum_in.at[:, pl.ds(1, N_DOM - 1)], sum_send
    ).wait()


def shards(right_side, element_matrix, face_map, share_index, share_count, face_mass, absorbing, impedance):
    hbm = pl.BlockSpec(memory_space=pltpu.HBM)
    f32, bf16, i32 = jnp.float32, jnp.bfloat16, jnp.int32
    out = pltpu.VMEM((TRACE, F_DEV), f32)
    vmem = pl.BlockSpec(memory_space=pltpu.VMEM)
    lead, later, along, step = pl.pallas_call(
        kernel,
        name="trace_cg",
        out_shape=(out, out, out, out),
        in_specs=[hbm] * 8,
        out_specs=(vmem, vmem, vmem, vmem),
        scratch_shapes=[
            pltpu.VMEM((TRACE, F_DEV), f32),
            pltpu.VMEM((SIDES, E_DEV), i32),
            pltpu.VMEM((4, GH), i32),
            pltpu.SMEM((1, 4), i32),
            pltpu.VMEM((8, LANES), f32),
            pltpu.VMEM((8, LANES), i32),
            pltpu.VMEM((8, LANES), f32),
            pltpu.SemaphoreType.DMA((7,)),
            pltpu.SemaphoreType.REGULAR((2,)),
            pltpu.VMEM((DOFS, DOFS, E_DEV), bf16),
            pltpu.VMEM((E_DEV // LANES, DOFS, DOFS, LANES), f32),
            pltpu.VMEM((ROWS, F_DEV), f32),
            pltpu.VMEM((ROWS, F_DEV), f32),
            pltpu.VMEM((2, ROWS, F_DEV), f32),
            pltpu.VMEM((8, LANES), f32),
            pltpu.VMEM((SIDES, 4, ROWS, LANES), f32),
            pltpu.VMEM((SIDES, 4, ROWS, LANES), f32),
            pltpu.VMEM((2, SIDES, ROWS, E_DEV), f32),
            pltpu.VMEM((SIDES * E_DEV, WIDE), bf16),
            pltpu.VMEM((4 * GH, WIDE), bf16),
            pltpu.VMEM((4 * GH, SIDES * E_DEV), bf16),
            pltpu.VMEM((4, 4 * GH, GH), bf16),
            pltpu.VMEM((2, 4, ROWS, GH), f32),
            pltpu.VMEM((4, ROWS, GH), f32),
            pltpu.VMEM((2, 4, ROWS, GH), f32),
            pltpu.VMEM((4, ROWS, GH), f32),
            pltpu.VMEM((24, ROWS, GH), f32),
            pltpu.VMEM((4, ROWS, GH), f32),
            pltpu.VMEM((4, GH), f32),
            pltpu.VMEM((4, 4, GH), f32),
            pltpu.VMEM((2, 1, LANES), f32),
            pltpu.VMEM((2, N_DOM, 1, LANES), f32),
            pltpu.SemaphoreType.DMA,
            pltpu.SemaphoreType.DMA((3,)),
            pltpu.SemaphoreType.DMA((3,)),
            pltpu.SemaphoreType.DMA,
            pltpu.SemaphoreType.DMA,
            pltpu.SemaphoreType.DMA,
            pltpu.SemaphoreType.DMA((2,)),
        ],
        compiler_params=pltpu.CompilerParams(
            collective_id=0, has_side_effects=True, vmem_limit_bytes=65 * 1000 * 1000
        ),
    )(
        right_side, element_matrix, face_map, share_index.reshape(4, GH), share_count,
        face_mass.reshape(8, LANES), absorbing.reshape(8, LANES), impedance.reshape(8, LANES),
    )
    return lead + step * later, later - step * along


def solution(mesh):
    in_specs = (
        P(None, "dom"), P(None, None, "dom"), P(None, "dom"), P("dom", None, None),
        P("dom", None), P("dom"), P("dom"), P("dom"),
    )
    return jax.shard_map(
        shards, mesh=mesh, in_specs=in_specs,
        out_specs=(P(None, "dom"), P(None, "dom")), check_vma=False,
    )
```

```python
import functools

import jax
import jax.numpy as jnp
from jax import lax
from jax.experimental import pallas as pl
from jax.experimental.pallas import tpu as pltpu
from jax.sharding import PartitionSpec as P

TRACE = 18
ROWS = 24
SIDES = 4
DOFS = 72
E_DEV = 512
F_DEV = 1024
GH = 128
OFFSETS = (-2, -1, 1, 2)
N_DOM = 128
LANES = 128
WIDE = 256
MESH = pl.DeviceIdType.MESH


def lane_pick(blocks, index_row, first, base):
    low = jnp.broadcast_to(index_row & (LANES - 1), (8, LANES))
    high = jnp.broadcast_to(index_row >> 7, (8, LANES))
    masks = [high == first + at for at in range(len(blocks))]
    pieces = []
    for i in range(ROWS // 8):
        picked = jnp.zeros((8, LANES), jnp.float32) if base is None else base(i)
        for mask, block in zip(masks, blocks):
            moved = jnp.take_along_axis(block(i), low, axis=1, mode="promise_in_bounds")
            picked = jnp.where(mask, moved, picked)
        pieces.append(picked)
    return jnp.concatenate(pieces, axis=0)


def split_two(value):
    head = value.astype(jnp.bfloat16)
    tail = (value - head.astype(jnp.float32)).astype(jnp.bfloat16)
    return head.astype(jnp.float32), tail.astype(jnp.float32)


def spread_rows(value, index_row, groups):
    head, tail = split_two(value)
    high = jnp.broadcast_to(index_row >> 8, value.shape)
    pieces = []
    for group in groups:
        mask = high == group
        pieces.append(jnp.where(mask, head, 0.0))
        pieces.append(jnp.where(mask, tail, 0.0))
    return jnp.concatenate(pieces, axis=0).astype(jnp.bfloat16)


def as_column(row):
    return jnp.broadcast_to(row, (LANES, LANES)).T


def one_hot_low(index_row):
    column = as_column((index_row & (WIDE - 1)).astype(jnp.float32))
    lane = lax.broadcasted_iota(jnp.int32, (LANES, LANES), 1).astype(jnp.float32)
    halves = [jnp.where(column == lane + half * LANES, 1.0, 0.0) for half in range(2)]
    return jnp.concatenate(halves, axis=1).astype(jnp.bfloat16)


def stacked(blocks):
    pairs = [split_two(block) for block in blocks]
    return jnp.concatenate([jnp.concatenate(pair, axis=0) for pair in pairs], axis=1).astype(jnp.bfloat16)


def wide_dot(left, right):
    return jnp.dot(left, right, preferred_element_type=jnp.float32)


def kernel(
    right_hbm, matrix_hbm, map_hbm, share_hbm, count_hbm, mass_hbm, absorb_hbm, imped_hbm,
    lead_ref, later_ref, along_ref, step_ref,
    right_ref, map_ref, share_ref, count_ref, mass_ref, absorb_ref, imped_ref, load_sem, meet_sem,
    matrix, widened, field0, field1, image, diag, picked0, picked1, product, hot, hot_share, hot_back, back_left, match,
    out_buf, ghost_in, part_buf, back_in, near_in, ghost_sum, list_out, list_in, sum_buf, sum_in,
    matrix_sem, trade_send, trade_recv, list_send, list_recv, sum_send, sum_recv,
):
    me = lax.axis_index("dom")
    loads = [
        pltpu.make_async_copy(source, target, load_sem.at[at])
        for at, (source, target) in enumerate((
            (share_hbm, share_ref), (count_hbm, count_ref), (right_hbm, right_ref), (map_hbm, map_ref),
            (mass_hbm, mass_ref), (absorb_hbm, absorb_ref), (imped_hbm, imped_ref),
        ))
    ]
    rows18 = pl.ds(0, TRACE)

    def blocks_wait(ref, sem, count, options):
        for n in options:
            @pl.when(count == n)
            def _(n=n):
                some = ref.at[pl.ds(0, n), rows18]
                pltpu.make_async_copy(some, some, sem).wait()

    core = lax.rem(me, 2)
    at_x = lax.rem(me // 2, 4)
    at_y = lax.rem(me // 8, 4)
    at_z = me // 32

    along_x = [lax.rem(at_x + d, 4) * 2 for d in range(4)]
    along_y = [lax.rem(at_y + d, 4) * 8 for d in range(4)]
    along_z = [lax.rem(at_z + d, 4) * 32 for d in range(4)]
    cores = (core, 1 - core)

    def device_at(dz, dy, dx, dc):
        return along_z[dz] + along_y[dy] + along_x[dx] + cores[dc]

    inside_to = [(me + o >= 0) & (me + o < N_DOM) for o in OFFSETS]
    inside_from = [(me - o >= 0) & (me - o < N_DOM) for o in OFFSETS]
    crosses = sorted(
        ((k, u) for k in range(4) for u in range(4) if k != u), key=lambda at: -abs(OFFSETS[at[1]] - OFFSETS[at[0]])
    )

    def cross_ok(k, u):
        user = me - OFFSETS[k] + OFFSETS[u]
        return inside_from[k] & (user >= 0) & (user < N_DOM)


    def tally(flags):
        return functools.reduce(lambda total, flag: total + flag.astype(jnp.int32), flags, jnp.int32(0))

    near_to, near_from = tally(inside_to), tally(inside_from)
    all_near = near_to + near_from + tally([cross_ok(k, u) for k, u in crosses])

    barrier = pltpu.get_barrier_semaphore()
    arrivals = jnp.int32(13)
    for k, o in enumerate(OFFSETS):
        @pl.when(inside_to[k])
        def _():
            pl.semaphore_signal(barrier, inc=1, device_id=(me + o,), device_id_type=MESH)
        arrivals = arrivals + inside_from[k].astype(jnp.int32)
    line_y = [device_at(0, d, 0, 0) for d in range(1, 4)]
    line_z = [device_at(d, 0, 0, 0) for d in range(1, 4)]
    pairs_x = [device_at(0, 0, d, c) for d in range(4) for c in range(2) if d or c]
    for other in pairs_x + line_y + line_z:
        pl.semaphore_signal(barrier, inc=1, device_id=(other,), device_id_type=MESH)

    for load in loads:
        load.start()
    matrix_copy = pltpu.make_async_copy(matrix_hbm, matrix, matrix_sem)
    matrix_copy.start()


    def meet(at, others):
        for other in others:
            pl.semaphore_signal(meet_sem.at[at], inc=1, device_id=(other,), device_id_type=MESH)

    for load in loads:
        load.wait()
    field0[0:TRACE, :] = right_ref[...]
    field0[TRACE:ROWS, :] = jnp.zeros((ROWS - TRACE, F_DEV), jnp.float32)
    diag[...] = mass_ref[...] + absorb_ref[...].astype(jnp.float32) * imped_ref[...]
    blank = jnp.zeros((TRACE, GH), jnp.float32)
    for k in range(4):
        @pl.when(jnp.logical_not(inside_from[k]))
        def _():
            ghost_in[k, 0:TRACE] = blank
            near_in[4 + k, 0:TRACE] = blank
            list_in[k] = jnp.full((4, GH), -1.0, jnp.float32)
        @pl.when(jnp.logical_not(inside_to[k]))
        def _():
            near_in[k, 0:TRACE] = blank
            back_in[k, 0:TRACE] = blank
        for ref in (ghost_in, back_in):
            ref[k, TRACE:ROWS] = jnp.zeros((ROWS - TRACE, GH), jnp.float32)
    for k, u in crosses:
        @pl.when(jnp.logical_not(cross_ok(k, u)))
        def _():
            near_in[8 + 4 * k + u, 0:TRACE] = blank
    for at in range(24):
        near_in[at, TRACE:ROWS] = jnp.zeros((ROWS - TRACE, GH), jnp.float32)

    lane = lax.broadcasted_iota(jnp.int32, (ROWS, GH), 1)
    alive = [lane < count_ref[0, k] for k in range(4)]

    def own_blocks(ref):
        return [
            lambda i, b=b: ref[8 * i:8 * i + 8, b * LANES:(b + 1) * LANES] for b in range(F_DEV // LANES)
        ]

    def trade(turn, source, target, other):
        return pltpu.make_async_remote_copy(
            src_ref=source.at[rows18], dst_ref=target.at[rows18],
            send_sem=trade_send.at[turn], recv_sem=trade_recv.at[turn], device_id=(other,), device_id_type=MESH,
        )

    def out_copy(turn, k):
        return trade(turn, out_buf.at[turn, k], ghost_in.at[k] if turn == 0 else near_in.at[4 + k], me + OFFSETS[k])

    def list_copy(k):
        return pltpu.make_async_remote_copy(
            src_ref=list_out, dst_ref=list_in.at[k], send_sem=list_send, recv_sem=list_recv,
            device_id=(me + OFFSETS[k],), device_id_type=MESH,
        )

    def lists_wait(sem, count):
        for n in (2, 3, 4):
            @pl.when(count == n)
            def _(n=n):
                some = list_in.at[pl.ds(0, n)]
                pltpu.make_async_copy(some, some, sem).wait()

    def cross_copy(k, u):
        return trade(1, part_buf.at[0, k], near_in.at[8 + 4 * u + k], me - OFFSETS[k] + OFFSETS[u])

    def part_copy(turn, k):
        return trade(1 + turn, part_buf.at[turn, k], near_in.at[k] if turn == 0 else back_in.at[k], me - OFFSETS[k])

    trades = (
        (ghost_in, near_to, near_from, (2, 3, 4)),
        (near_in, all_near, all_near, (9, 13, 17, 19, 20)),
        (back_in, near_from, near_to, (2, 3, 4)),
    )

    def trade_wait_recv(turn):
        ref, _, count, options = trades[turn]
        blocks_wait(ref, trade_recv.at[turn], count, options)

    def trade_wait_send(turn):
        ref, count, _, options = trades[turn]
        blocks_wait(ref, trade_send.at[turn], count, options)

    def send_out(turn, ref):
        blocks = own_blocks(ref)
        for k in range(4):
            gone = lane_pick(blocks, share_ref[k:k + 1, :], 0, None)
            out_buf[turn, k] = jnp.where(alive[k], gone, 0.0)
        if turn == 0:
            pl.semaphore_wait(barrier, arrivals)
        for k in (0, 3, 1, 2):
            @pl.when(inside_to[k])
            def _():
                out_copy(turn, k).start()
                if turn == 0:
                    list_copy(k).start()

    def send_part(turn):
        for k in range(4):
            @pl.when(inside_from[k])
            def _():
                part_copy(turn, k).start()

    def send_cross():
        for k, u in crosses:
            @pl.when(cross_ok(k, u))
            def _():
                cross_copy(k, u).start()

    def pick_own(ref, picked):
        blocks = own_blocks(ref)
        for side in range(SIDES):
            for b in range(E_DEV // LANES):
                cols = slice(b * LANES, (b + 1) * LANES)
                picked[side, b] = lane_pick(blocks, map_ref[side:side + 1, cols], 0, None)

    def pick_ghost(ghosts, picked, b):
        blocks = [lambda i, k=k: ghosts[k, 8 * i:8 * i + 8] for k in range(4)]
        first = b * LANES if isinstance(b, int) else pl.multiple_of(b * LANES, LANES)
        cols = pl.ds(first, LANES)
        for side in range(SIDES):
            base = lambda i, side=side: picked[side, b, 8 * i:8 * i + 8]
            picked[side, b] = lane_pick(blocks, map_ref[side:side + 1, cols], F_DEV // LANES, base)

    def multiply(turn, picked, b):
        def one(side, total):
            for c in range(TRACE):
                row = picked[side, b, c:c + 1, :]
                total = total + widened[b, side * TRACE + c] * row
            return total

        total = jnp.zeros((DOFS, LANES), jnp.float32)
        for side in range(SIDES):
            total = one(side, total)
        for side in range(SIDES):
            product[turn, side, b, 0:TRACE, :] = total[side * TRACE:(side + 1) * TRACE]

    def scatter_block(turn, groups, b):
        lefts = [
            spread_rows(product[turn, side, b], map_ref[side:side + 1, b * LANES:(b + 1) * LANES], groups)
            for side in range(SIDES)
        ]
        return wide_dot(jnp.concatenate(lefts, axis=1), hot[b])

    def energy(step):
        total = jnp.zeros((ROWS, LANES), jnp.float32)
        for side in range(SIDES):
            for b in range(E_DEV // LANES):
                image_part = product[0, side, b]
                value = picked0[side, b]
                if step is not None:
                    image_part = image_part - step * product[1, side, b]
                    product[1, side, b] = image_part
                    value = value - step * picked1[side, b]
                total = total + value * image_part
        return jnp.sum(total, axis=0, keepdims=True)

    def face_sums(ref):
        square = jnp.zeros((8, LANES), jnp.float32)
        weighted = jnp.zeros((8, LANES), jnp.float32)
        for b in range(F_DEV // LANES):
            value = ref[:, b * LANES:(b + 1) * LANES]
            both = value * value
            both = both[0:8] + both[8:16] + both[16:24]
            square = square + both
            weighted = weighted + both * diag[b:b + 1, :]
        return jnp.sum(square, axis=0, keepdims=True), jnp.sum(weighted, axis=0, keepdims=True)

    def scatter(turn, groups, total):
        if total is None:
            parts = [scatter_block(turn, groups, b) for b in range(E_DEV // LANES)]
            total = (parts[0] + parts[1]) + (parts[2] + parts[3])
        for at in range(len(groups)):
            base = at * 2 * ROWS
            yield total[base:base + ROWS] + total[base + ROWS:base + 2 * ROWS]

    def scatter_ghost(turn, total=None):
        for at, both in enumerate(scatter(turn, (4, 5), total)):
            part_buf[turn, 2 * at] = both[:, 0:GH]
            part_buf[turn, 2 * at + 1] = both[:, GH:]

    def scatter_own(turn, ref):
        for at, both in enumerate(scatter(turn, (0, 1, 2, 3), None)):
            for half in range(2):
                b = 2 * at + half
                cols = slice(b * LANES, (b + 1) * LANES)
                image[turn, :, cols] = both[:, half * LANES:(half + 1) * LANES] + diag[b:b + 1, :] * ref[:, cols]

    def add_back(turn, back):
        total = jnp.zeros((4 * 2 * ROWS, WIDE), jnp.float32)
        for k in range(4):
            value = jnp.where(alive[k], back[k], 0.0)
            left = spread_rows(value, share_ref[k:k + 1, :], (0, 1, 2, 3))
            total = total + wide_dot(left, hot_share[k * GH:(k + 1) * GH, :])
        for group in range(4):
            base = group * 2 * ROWS
            both = total[base:base + ROWS] + total[base + ROWS:base + 2 * ROWS]
            cols = slice(group * WIDE, (group + 1) * WIDE)
            image[turn, :, cols] = image[turn, :, cols] + both

    others = sorted(
        ((dz, dy, dx, dc) for dz in range(4) for dy in range(4) for dx in range(4) for dc in range(2) if dz or dy or dx or dc),
        key=lambda at: -sum(min(d, 4 - d) for d in at[:3]),
    )

    def sum_start(turn, first, second):
        lane_at = lax.broadcasted_iota(jnp.int32, (1, LANES), 1)
        first = first + pltpu.roll(first, LANES // 2, 1)
        second = second + pltpu.roll(second, LANES // 2, 1)
        row = jnp.where(lane_at < LANES // 2, first, second)
        sum_buf[turn] = row
        sum_in[turn, pl.ds(me, 1), :] = row
        for at in others:
            pltpu.make_async_remote_copy(
                src_ref=sum_buf.at[turn], dst_ref=sum_in.at[turn, pl.ds(me, 1), :],
                send_sem=sum_send, recv_sem=sum_recv.at[turn],
                device_id=(device_at(*at),), device_id_type=MESH,
            ).start()

    def sum_finish(turn):
        pltpu.make_async_copy(
            sum_in.at[turn, pl.ds(0, N_DOM - 1)], sum_in.at[turn, pl.ds(1, N_DOM - 1)], sum_recv.at[turn]
        ).wait()
        total = jnp.sum(sum_in[turn], axis=0, keepdims=True)
        lane_at = lax.broadcasted_iota(jnp.int32, (1, LANES), 1)
        first = jnp.sum(jnp.where(lane_at < LANES // 2, total, 0.0), axis=1, keepdims=True)
        second = jnp.sum(jnp.where(lane_at < LANES // 2, 0.0, total), axis=1, keepdims=True)
        return first, second

    def clear_tail(ref):
        for turn in range(2):
            for side in range(SIDES):
                for b in range(E_DEV // LANES):
                    ref[turn, side, b, TRACE:ROWS, :] = jnp.zeros((ROWS - TRACE, LANES), jnp.float32)

    def complete_ghosts():
        for k in range(4):
            left = stacked([part_buf[0, k] if u == k else near_in[8 + 4 * k + u] for u in range(4)])
            both = wide_dot(left, match[k])
            ghost_sum[k] = near_in[4 + k] + both[0:ROWS] + both[ROWS:2 * ROWS]

    def pick_back(b):
        both = wide_dot(back_left[...], hot_back[b])
        for side in range(SIDES):
            cols = slice(side * LANES, (side + 1) * LANES)
            picked1[side, b] = picked1[side, b] + both[0:ROWS, cols] + both[ROWS:2 * ROWS, cols]

    lists = [jnp.where(alive[k][0:1], share_ref[k:k + 1, :].astype(jnp.float32), -1.0) for k in range(4)]
    for k in range(4):
        list_out[k:k + 1, :] = lists[k]
    send_out(0, field0)
    meet(0, line_y)
    clear_tail(product)
    for side in range(SIDES):
        for b in range(E_DEV // LANES):
            first = side * LANES
            hot[b, first:first + LANES, :] = one_hot_low(map_ref[side:side + 1, b * LANES:(b + 1) * LANES])
    for k in range(4):
        hot_share[k * GH:(k + 1) * GH, :] = one_hot_low(share_ref[k:k + 1, :])
    square, weighted = face_sums(field0)
    for u in range(4):
        column = as_column(lists[u])
        for side in range(SIDES):
            for b in range(E_DEV // LANES):
                cols = slice(b * LANES, (b + 1) * LANES)
                hit = column == map_ref[side:side + 1, cols].astype(jnp.float32)
                first = side * LANES
                hot_back[b, u * GH:(u + 1) * GH, first:first + LANES] = jnp.where(hit, 1.0, 0.0).astype(jnp.bfloat16)
    pl.semaphore_wait(meet_sem.at[0], 3)
    meet(1, line_z)
    matrix_copy.wait()

    def widen(row, carry):
        whole = matrix[row].astype(jnp.float32)
        for b in range(E_DEV // LANES):
            widened[b, row] = whole[:, b * LANES:(b + 1) * LANES]
        return carry

    pick_own(field0, picked0)
    lax.fori_loop(0, DOFS, widen, 0, unroll=2)
    pl.semaphore_wait(meet_sem.at[1], 3)
    trade_wait_recv(0)
    lists_wait(list_recv, near_from)

    total = None
    for b in range(E_DEV // LANES):
        pick_ghost(ghost_in, picked0, b)
        multiply(0, picked0, b)
        part = scatter_block(0, (4, 5), b)
        total = part if total is None else total + part
    scatter_ghost(0, total)
    send_cross()
    send_part(0)
    scatter_own(0, field0)
    send_out(1, image.at[0])
    sum_start(0, square, weighted + energy(None))
    pick_own(image.at[0], picked1)
    for k in range(4):
        target = jnp.where(list_in[k, k:k + 1, :] < 0.0, -2.0, list_in[k, k:k + 1, :])
        for u in range(4):
            hit = as_column(list_in[k, u:u + 1, :]) == target
            match[k, u * GH:(u + 1) * GH, :] = jnp.where(hit, 1.0, 0.0).astype(jnp.bfloat16)
    trade_wait_recv(1)
    complete_ghosts()
    back_left[...] = stacked([near_in[k] for k in range(4)])
    pick_back(0)
    pick_ghost(ghost_sum, picked1, 0)
    add_back(0, near_in)
    last = E_DEV // LANES - 1

    def middle(b, carry):
        multiply(1, picked1, b)
        pick_back(b + 1)
        pick_ghost(ghost_sum, picked1, b + 1)
        return carry

    lax.fori_loop(0, last, middle, 0)
    norm0, curve0 = sum_finish(0)
    step0 = norm0 / curve0
    multiply(1, picked1, last)
    for b in range(F_DEV // LANES):
        cols = slice(b * LANES, (b + 1) * LANES)
        field1[:, cols] = field0[:, cols] - step0 * image[0, :, cols]
    square, weighted = face_sums(field1)
    sum_start(1, square, weighted + energy(step0))
    scatter_ghost(1)
    send_part(1)
    scatter_own(1, field1)
    trade_wait_recv(2)
    add_back(1, back_in)
    norm1, curve1 = sum_finish(1)
    ratio = norm1 / norm0
    step1 = norm1 / (curve1 - ratio * norm1 / step0)
    lead = step0 + step1 * ratio
    for b in range(F_DEV // LANES):
        cols = slice(b * LANES, (b + 1) * LANES)
        lead_ref[:, cols] = lead * field0[0:TRACE, cols]
        later_ref[:, cols] = field1[0:TRACE, cols]
        along_ref[:, cols] = image[1, 0:TRACE, cols] + ratio * image[0, 0:TRACE, cols]
    step_ref[...] = jnp.broadcast_to(step1, (TRACE, F_DEV))

    for turn in range(3):
        trade_wait_send(turn)
    lists_wait(list_send, near_to)
    pltpu.make_async_copy(
        sum_in.at[:, pl.ds(0, N_DOM - 1)], sum_in.at[:, pl.ds(1, N_DOM - 1)], sum_send
    ).wait()


def shards(right_side, element_matrix, face_map, share_index, share_count, face_mass, absorbing, impedance):
    hbm = pl.BlockSpec(memory_space=pltpu.HBM)
    f32, bf16, i32 = jnp.float32, jnp.bfloat16, jnp.int32
    out = pltpu.VMEM((TRACE, F_DEV), f32)
    vmem = pl.BlockSpec(memory_space=pltpu.VMEM)
    lead, later, along, step = pl.pallas_call(
        kernel,
        name="trace_cg",
        out_shape=(out, out, out, out),
        in_specs=[hbm] * 8,
        out_specs=(vmem, vmem, vmem, vmem),
        scratch_shapes=[
            pltpu.VMEM((TRACE, F_DEV), f32),
            pltpu.VMEM((SIDES, E_DEV), i32),
            pltpu.VMEM((4, GH), i32),
            pltpu.SMEM((1, 4), i32),
            pltpu.VMEM((8, LANES), f32),
            pltpu.VMEM((8, LANES), i32),
            pltpu.VMEM((8, LANES), f32),
            pltpu.SemaphoreType.DMA((7,)),
            pltpu.SemaphoreType.REGULAR((2,)),
            pltpu.VMEM((DOFS, DOFS, E_DEV), bf16),
            pltpu.VMEM((E_DEV // LANES, DOFS, DOFS, LANES), f32),
            pltpu.VMEM((ROWS, F_DEV), f32),
            pltpu.VMEM((ROWS, F_DEV), f32),
            pltpu.VMEM((2, ROWS, F_DEV), f32),
            pltpu.VMEM((8, LANES), f32),
            pltpu.VMEM((SIDES, 4, ROWS, LANES), f32),
            pltpu.VMEM((SIDES, 4, ROWS, LANES), f32),
            pltpu.VMEM((2, SIDES, E_DEV // LANES, ROWS, LANES), f32),
            pltpu.VMEM((E_DEV // LANES, SIDES * LANES, WIDE), bf16),
            pltpu.VMEM((4 * GH, WIDE), bf16),
            pltpu.VMEM((E_DEV // LANES, 4 * GH, SIDES * LANES), bf16),
            pltpu.VMEM((2 * ROWS, 4 * GH), bf16),
            pltpu.VMEM((4, 4 * GH, GH), bf16),
            pltpu.VMEM((2, 4, ROWS, GH), f32),
            pltpu.VMEM((4, ROWS, GH), f32),
            pltpu.VMEM((2, 4, ROWS, GH), f32),
            pltpu.VMEM((4, ROWS, GH), f32),
            pltpu.VMEM((24, ROWS, GH), f32),
            pltpu.VMEM((4, ROWS, GH), f32),
            pltpu.VMEM((4, GH), f32),
            pltpu.VMEM((4, 4, GH), f32),
            pltpu.VMEM((2, 1, LANES), f32),
            pltpu.VMEM((2, N_DOM, LANES), f32),
            pltpu.SemaphoreType.DMA,
            pltpu.SemaphoreType.DMA((3,)),
            pltpu.SemaphoreType.DMA((3,)),
            pltpu.SemaphoreType.DMA,
            pltpu.SemaphoreType.DMA,
            pltpu.SemaphoreType.DMA,
            pltpu.SemaphoreType.DMA((2,)),
        ],
        compiler_params=pltpu.CompilerParams(
            collective_id=0, has_side_effects=True, vmem_limit_bytes=65 * 1000 * 1000
        ),
    )(
        right_side, element_matrix, face_map, share_index.reshape(4, GH), share_count,
        face_mass.reshape(8, LANES), absorbing.reshape(8, LANES), impedance.reshape(8, LANES),
    )
    return lead + step * later, later - step * along


def solution(mesh):
    in_specs = (
        P(None, "dom"), P(None, None, "dom"), P(None, "dom"), P("dom", None, None),
        P("dom", None), P("dom"), P("dom"), P("dom"),
    )
    return jax.shard_map(
        shards, mesh=mesh, in_specs=in_specs,
        out_specs=(P(None, "dom"), P(None, "dom")), check_vma=False,
    )
```

```python
import functools

import jax
import jax.numpy as jnp
from jax import lax
from jax.experimental import pallas as pl
from jax.experimental.pallas import tpu as pltpu
from jax.sharding import PartitionSpec as P

TRACE = 18
ROWS = 24
SIDES = 4
DOFS = 72
E_DEV = 512
F_DEV = 1024
GH = 128
OFFSETS = (-2, -1, 1, 2)
N_DOM = 128
LANES = 128
WIDE = 256
MESH = pl.DeviceIdType.MESH


def lane_pick(blocks, index_row, first, base):
    low = jnp.broadcast_to(index_row & (LANES - 1), (8, LANES))
    high = jnp.broadcast_to(index_row >> 7, (8, LANES))
    masks = [high == first + at for at in range(len(blocks))]
    pieces = []
    for i in range(ROWS // 8):
        picked = jnp.zeros((8, LANES), jnp.float32) if base is None else base(i)
        for mask, block in zip(masks, blocks):
            moved = jnp.take_along_axis(block(i), low, axis=1, mode="promise_in_bounds")
            picked = jnp.where(mask, moved, picked)
        pieces.append(picked)
    return jnp.concatenate(pieces, axis=0)


def split_two(value):
    head = value.astype(jnp.bfloat16)
    tail = (value - head.astype(jnp.float32)).astype(jnp.bfloat16)
    return head.astype(jnp.float32), tail.astype(jnp.float32)


def spread_rows(value, index_row, groups):
    head, tail = split_two(value)
    high = jnp.broadcast_to(index_row >> 8, value.shape)
    pieces = []
    for group in groups:
        mask = high == group
        pieces.append(jnp.where(mask, head, 0.0))
        pieces.append(jnp.where(mask, tail, 0.0))
    return jnp.concatenate(pieces, axis=0).astype(jnp.bfloat16)


def as_column(row):
    return jnp.broadcast_to(row, (LANES, LANES)).T


def one_hot_low(index_row):
    column = as_column((index_row & (WIDE - 1)).astype(jnp.float32))
    lane = lax.broadcasted_iota(jnp.int32, (LANES, LANES), 1).astype(jnp.float32)
    halves = [jnp.where(column == lane + half * LANES, 1.0, 0.0) for half in range(2)]
    return jnp.concatenate(halves, axis=1).astype(jnp.bfloat16)


def stacked(blocks):
    pairs = [split_two(block) for block in blocks]
    return jnp.concatenate([jnp.concatenate(pair, axis=0) for pair in pairs], axis=1).astype(jnp.bfloat16)


def wide_dot(left, right):
    return jnp.dot(left, right, preferred_element_type=jnp.float32)


def kernel(
    right_hbm, matrix_hbm, map_hbm, share_hbm, count_hbm, mass_hbm, absorb_hbm, imped_hbm,
    lead_ref, later_ref, along_ref, step_ref,
    right_ref, map_ref, share_ref, count_ref, mass_ref, absorb_ref, imped_ref, load_sem, meet_sem,
    matrix, widened, field0, field1, image, diag, picked0, picked1, product, hot, hot_share, hot_back, back_left, match,
    out_buf, ghost_in, part_buf, back_in, near_in, ghost_sum, sum_buf, sum_in,
    matrix_sem, trade_send, trade_recv, sum_send, sum_recv,
):
    me = lax.axis_index("dom")
    rows18, rows22 = pl.ds(0, TRACE), pl.ds(0, TRACE + 4)

    def blocks_wait(ref, rows, sem, count, options):
        for n in options:
            @pl.when(count == n)
            def _(n=n):
                some = ref.at[pl.ds(0, n), rows]
                pltpu.make_async_copy(some, some, sem).wait()

    core = lax.rem(me, 2)
    at_x = lax.rem(me // 2, 4)
    at_y = lax.rem(me // 8, 4)
    at_z = me // 32

    along_x = [lax.rem(at_x + d, 4) * 2 for d in range(4)]
    along_y = [lax.rem(at_y + d, 4) * 8 for d in range(4)]
    along_z = [lax.rem(at_z + d, 4) * 32 for d in range(4)]
    cores = (core, 1 - core)

    def device_at(dz, dy, dx, dc):
        return along_z[dz] + along_y[dy] + along_x[dx] + cores[dc]

    inside_to = [(me + o >= 0) & (me + o < N_DOM) for o in OFFSETS]
    inside_from = [(me - o >= 0) & (me - o < N_DOM) for o in OFFSETS]
    crosses = sorted(
        ((k, u) for k in range(4) for u in range(4) if k != u), key=lambda at: -abs(OFFSETS[at[1]] - OFFSETS[at[0]])
    )

    def cross_ok(k, u):
        user = me - OFFSETS[k] + OFFSETS[u]
        return inside_from[k] & (user >= 0) & (user < N_DOM)


    def tally(flags):
        return functools.reduce(lambda total, flag: total + flag.astype(jnp.int32), flags, jnp.int32(0))

    barrier = pltpu.get_barrier_semaphore()
    for k, o in sorted(enumerate(OFFSETS), key=lambda at: -abs(at[1])):
        @pl.when(inside_to[k])
        def _():
            pl.semaphore_signal(barrier, inc=1, device_id=(me + o,), device_id_type=MESH)
    loads = [
        pltpu.make_async_copy(source, target, load_sem.at[at])
        for at, (source, target) in enumerate((
            (share_hbm, share_ref), (count_hbm, count_ref), (right_hbm, right_ref), (map_hbm, map_ref),
            (mass_hbm, mass_ref), (absorb_hbm, absorb_ref), (imped_hbm, imped_ref),
        ))
    ]
    for load in loads[:4]:
        load.start()
    for load in loads[4:]:
        load.start()
    matrix_copy = pltpu.make_async_copy(matrix_hbm, matrix, matrix_sem)
    matrix_copy.start()

    line_y = [device_at(0, d, 0, 0) for d in range(1, 4)]
    line_z = [device_at(d, 0, 0, 0) for d in range(1, 4)]
    pairs_x = [device_at(0, 0, d, c) for d in range(4) for c in range(2) if d or c]
    for other in pairs_x + line_y + line_z:
        pl.semaphore_signal(barrier, inc=1, device_id=(other,), device_id_type=MESH)

    near_to, near_from = tally(inside_to), tally(inside_from)
    all_near = near_to + near_from + tally([cross_ok(k, u) for k, u in crosses])

    arrivals = 13 + near_from

    def meet(at, others):
        for other in others:
            pl.semaphore_signal(meet_sem.at[at], inc=1, device_id=(other,), device_id_type=MESH)

    for load in loads[:3]:
        load.wait()
    field0[0:TRACE, :] = right_ref[...]
    field0[TRACE:ROWS, :] = jnp.zeros((ROWS - TRACE, F_DEV), jnp.float32)
    lane = lax.broadcasted_iota(jnp.int32, (ROWS, GH), 1)
    alive = [lane < count_ref[0, k] for k in range(4)]

    def own_blocks(ref):
        return [
            lambda i, b=b: ref[8 * i:8 * i + 8, b * LANES:(b + 1) * LANES] for b in range(F_DEV // LANES)
        ]

    def trade(turn, source, target, other):
        rows = rows22 if turn == 0 else rows18
        return pltpu.make_async_remote_copy(
            src_ref=source.at[rows], dst_ref=target.at[rows],
            send_sem=trade_send.at[turn], recv_sem=trade_recv.at[turn], device_id=(other,), device_id_type=MESH,
        )

    def out_copy(turn, k):
        return trade(turn, out_buf.at[turn, k], ghost_in.at[k] if turn == 0 else near_in.at[4 + k], me + OFFSETS[k])

    def cross_copy(k, u):
        return trade(1, part_buf.at[0, k], near_in.at[8 + 4 * u + k], me - OFFSETS[k] + OFFSETS[u])

    def part_copy(turn, k):
        return trade(1 + turn, part_buf.at[turn, k], near_in.at[k] if turn == 0 else back_in.at[k], me - OFFSETS[k])

    trades = (
        (ghost_in, near_to, near_from, (2, 3, 4)),
        (near_in, all_near, all_near, (9, 13, 17, 19, 20)),
        (back_in, near_from, near_to, (2, 3, 4)),
    )

    def trade_wait_recv(turn):
        ref, _, count, options = trades[turn]
        blocks_wait(ref, rows18 if turn else rows22, trade_recv.at[turn], count, options)

    def trade_wait_send(turn):
        ref, count, _, options = trades[turn]
        blocks_wait(ref, rows18 if turn else rows22, trade_send.at[turn], count, options)

    def send_out(turn, ref):
        blocks = own_blocks(ref)
        for k in range(4):
            gone = lane_pick(blocks, share_ref[k:k + 1, :], 0, None)
            out_buf[turn, k, 0:TRACE] = jnp.where(alive[k], gone, 0.0)[0:TRACE]
        if turn == 0:
            pl.semaphore_wait(barrier, arrivals)
        for k in (0, 3, 1, 2):
            @pl.when(inside_to[k])
            def _():
                out_copy(turn, k).start()

    def send_part(turn):
        for k in range(4):
            @pl.when(inside_from[k])
            def _():
                part_copy(turn, k).start()

    def send_cross():
        for k, u in crosses:
            @pl.when(cross_ok(k, u))
            def _():
                cross_copy(k, u).start()

    def pick_own(ref, picked):
        blocks = own_blocks(ref)
        for side in range(SIDES):
            for b in range(E_DEV // LANES):
                cols = slice(b * LANES, (b + 1) * LANES)
                picked[side, b] = lane_pick(blocks, map_ref[side:side + 1, cols], 0, None)

    def pick_ghost(ghosts, picked, b):
        blocks = [lambda i, k=k: ghosts[k, 8 * i:8 * i + 8] for k in range(4)]
        first = b * LANES if isinstance(b, int) else pl.multiple_of(b * LANES, LANES)
        cols = pl.ds(first, LANES)
        for side in range(SIDES):
            base = lambda i, side=side: picked[side, b, 8 * i:8 * i + 8]
            picked[side, b] = lane_pick(blocks, map_ref[side:side + 1, cols], F_DEV // LANES, base)

    def multiply(turn, picked, b):
        def one(side, total):
            for c in range(TRACE):
                row = picked[side, b, c:c + 1, :]
                total = total + widened[b, side * TRACE + c] * row
            return total

        total = jnp.zeros((DOFS, LANES), jnp.float32)
        for side in range(SIDES):
            total = one(side, total)
        for side in range(SIDES):
            product[turn, side, b, 0:TRACE, :] = total[side * TRACE:(side + 1) * TRACE]

    def scatter_block(turn, groups, b):
        lefts = [
            spread_rows(product[turn, side, b], map_ref[side:side + 1, b * LANES:(b + 1) * LANES], groups)
            for side in range(SIDES)
        ]
        return wide_dot(jnp.concatenate(lefts, axis=1), hot[b])

    def energy(step):
        total = jnp.zeros((ROWS, LANES), jnp.float32)
        for side in range(SIDES):
            for b in range(E_DEV // LANES):
                image_part = product[0, side, b] - step * product[1, side, b]
                product[1, side, b] = image_part
                total = total + (picked0[side, b] - step * picked1[side, b]) * image_part
        return jnp.sum(total, axis=0, keepdims=True)

    def scatter_block(turn, groups, b):
        lefts = [
            spread_rows(product[turn, side, b], map_ref[side:side + 1, b * LANES:(b + 1) * LANES], groups)
            for side in range(SIDES)
        ]
        return wide_dot(jnp.concatenate(lefts, axis=1), hot[b])

    def energy(step):
        total = jnp.zeros((ROWS, LANES), jnp.float32)
        for side in range(SIDES):
            for b in range(E_DEV // LANES):
                image_part = product[0, side, b]
                value = picked0[side, b]
                if step is not None:
                    image_part = image_part - step * product[1, side, b]
                    product[1, side, b] = image_part
                    value = value - step * picked1[side, b]
                total = total + value * image_part
        return jnp.sum(total, axis=0, keepdims=True)

    def face_sums(ref):
        square = jnp.zeros((8, LANES), jnp.float32)
        weighted = jnp.zeros((8, LANES), jnp.float32)
        for b in range(F_DEV // LANES):
            value = ref[:, b * LANES:(b + 1) * LANES]
            both = value * value
            both = both[0:8] + both[8:16] + both[16:24]
            square = square + both
            weighted = weighted + both * diag[b:b + 1, :]
        return jnp.sum(square, axis=0, keepdims=True), jnp.sum(weighted, axis=0, keepdims=True)

    def scatter(turn, groups, total):
        if total is None:
            parts = [scatter_block(turn, groups, b) for b in range(E_DEV // LANES)]
            total = (parts[0] + parts[1]) + (parts[2] + parts[3])
        for at in range(len(groups)):
            base = at * 2 * ROWS
            yield total[base:base + ROWS] + total[base + ROWS:base + 2 * ROWS]

    def scatter_ghost(turn, total=None):
        for at, both in enumerate(scatter(turn, (4, 5), total)):
            part_buf[turn, 2 * at] = both[:, 0:GH]
            part_buf[turn, 2 * at + 1] = both[:, GH:]

    def scatter_own(turn, ref):
        for at, both in enumerate(scatter(turn, (0, 1, 2, 3), None)):
            for half in range(2):
                b = 2 * at + half
                cols = slice(b * LANES, (b + 1) * LANES)
                image[turn, :, cols] = both[:, half * LANES:(half + 1) * LANES] + diag[b:b + 1, :] * ref[:, cols]

    def add_back(turn, back):
        total = jnp.zeros((4 * 2 * ROWS, WIDE), jnp.float32)
        for k in range(4):
            value = jnp.where(alive[k], back[k], 0.0)
            left = spread_rows(value, share_ref[k:k + 1, :], (0, 1, 2, 3))
            total = total + wide_dot(left, hot_share[k * GH:(k + 1) * GH, :])
        for group in range(4):
            base = group * 2 * ROWS
            both = total[base:base + ROWS] + total[base + ROWS:base + 2 * ROWS]
            cols = slice(group * WIDE, (group + 1) * WIDE)
            image[turn, :, cols] = image[turn, :, cols] + both

    others = sorted(
        ((dz, dy, dx, dc) for dz in range(4) for dy in range(4) for dx in range(4) for dc in range(2) if dz or dy or dx or dc),
        key=lambda at: -sum(min(d, 4 - d) for d in at[:3]),
    )

    def sum_start(turn, first, second):
        lane_at = lax.broadcasted_iota(jnp.int32, (1, LANES), 1)
        first = first + pltpu.roll(first, LANES // 2, 1)
        second = second + pltpu.roll(second, LANES // 2, 1)
        row = jnp.where(lane_at < LANES // 2, first, second)
        sum_buf[turn] = row
        sum_in[turn, pl.ds(me, 1), :] = row
        for at in others:
            pltpu.make_async_remote_copy(
                src_ref=sum_buf.at[turn], dst_ref=sum_in.at[turn, pl.ds(me, 1), :],
                send_sem=sum_send, recv_sem=sum_recv.at[turn],
                device_id=(device_at(*at),), device_id_type=MESH,
            ).start()

    def sum_finish(turn):
        pltpu.make_async_copy(
            sum_in.at[turn, pl.ds(0, N_DOM - 1)], sum_in.at[turn, pl.ds(1, N_DOM - 1)], sum_recv.at[turn]
        ).wait()
        total = jnp.sum(sum_in[turn], axis=0, keepdims=True)
        lane_at = lax.broadcasted_iota(jnp.int32, (1, LANES), 1)
        first = jnp.sum(jnp.where(lane_at < LANES // 2, total, 0.0), axis=1, keepdims=True)
        second = jnp.sum(jnp.where(lane_at < LANES // 2, 0.0, total), axis=1, keepdims=True)
        return first, second

    def clear_tail(ref):
        for turn in range(2):
            for side in range(SIDES):
                for b in range(E_DEV // LANES):
                    ref[turn, side, b, TRACE:ROWS, :] = jnp.zeros((ROWS - TRACE, LANES), jnp.float32)

    def complete_ghosts():
        for k in range(4):
            left = stacked([part_buf[0, k] if u == k else near_in[8 + 4 * k + u] for u in range(4)])
            both = wide_dot(left, match[k])
            ghost_sum[k] = near_in[4 + k] + both[0:ROWS] + both[ROWS:2 * ROWS]

    def pick_back(b):
        both = wide_dot(back_left[...], hot_back[b])
        for side in range(SIDES):
            cols = slice(side * LANES, (side + 1) * LANES)
            picked1[side, b] = picked1[side, b] + both[0:ROWS, cols] + both[ROWS:2 * ROWS, cols]

    lists = [jnp.where(alive[k][0:1], share_ref[k:k + 1, :].astype(jnp.float32), -1.0) for k in range(4)]
    for k in range(4):
        out_buf[0, k, TRACE:TRACE + 4] = jnp.concatenate(lists, axis=0)
    send_out(0, field0)
    for load in loads[3:]:
        load.wait()
    diag[...] = mass_ref[...] + absorb_ref[...].astype(jnp.float32) * imped_ref[...]
    blank = jnp.zeros((TRACE, GH), jnp.float32)
    for k in range(4):
        @pl.when(jnp.logical_not(inside_from[k]))
        def _():
            ghost_in[k, 0:TRACE] = blank
            near_in[4 + k, 0:TRACE] = blank
            ghost_in[k, TRACE:TRACE + 4] = jnp.full((4, GH), -1.0, jnp.float32)
        @pl.when(jnp.logical_not(inside_to[k]))
        def _():
            near_in[k, 0:TRACE] = blank
            back_in[k, 0:TRACE] = blank
        ghost_in[k, TRACE + 4:ROWS] = jnp.zeros((ROWS - TRACE - 4, GH), jnp.float32)
        back_in[k, TRACE:ROWS] = jnp.zeros((ROWS - TRACE, GH), jnp.float32)
    for k, u in crosses:
        @pl.when(jnp.logical_not(cross_ok(k, u)))
        def _():
            near_in[8 + 4 * k + u, 0:TRACE] = blank
    for at in range(24):
        near_in[at, TRACE:ROWS] = jnp.zeros((ROWS - TRACE, GH), jnp.float32)

    meet(0, line_y)
    clear_tail(product)
    for side in range(SIDES):
        for b in range(E_DEV // LANES):
            first = side * LANES
            hot[b, first:first + LANES, :] = one_hot_low(map_ref[side:side + 1, b * LANES:(b + 1) * LANES])
    for k in range(4):
        hot_share[k * GH:(k + 1) * GH, :] = one_hot_low(share_ref[k:k + 1, :])
    square, weighted = face_sums(field0)
    for u in range(4):
        column = as_column(lists[u])
        for side in range(SIDES):
            for b in range(E_DEV // LANES):
                cols = slice(b * LANES, (b + 1) * LANES)
                hit = column == map_ref[side:side + 1, cols].astype(jnp.float32)
                first = side * LANES
                hot_back[b, u * GH:(u + 1) * GH, first:first + LANES] = jnp.where(hit, 1.0, 0.0).astype(jnp.bfloat16)
    pl.semaphore_wait(meet_sem.at[0], 3)
    meet(1, line_z)
    matrix_copy.wait()

    def widen(row, carry):
        whole = matrix[row].astype(jnp.float32)
        for b in range(E_DEV // LANES):
            widened[b, row] = whole[:, b * LANES:(b + 1) * LANES]
        return carry

    pick_own(field0, picked0)
    lax.fori_loop(0, DOFS, widen, 0, unroll=2)
    pl.semaphore_wait(meet_sem.at[1], 3)
    trade_wait_recv(0)

    total, force = None, None
    for b in range(E_DEV // LANES):
        pick_ghost(ghost_in, picked0, b)
        multiply(0, picked0, b)
        part = scatter_block(0, (4, 5), b)
        total = part if total is None else total + part
        for side in range(SIDES):
            both = picked0[side, b] * product[0, side, b]
            force = both if force is None else force + both
    scatter_ghost(0, total)
    send_cross()
    send_part(0)
    scatter_own(0, field0)
    send_out(1, image.at[0])
    sum_start(0, square, weighted + jnp.sum(force, axis=0, keepdims=True))
    pick_own(image.at[0], picked1)
    for k in range(4):
        mine = ghost_in[k, TRACE + k:TRACE + k + 1, :]
        target = jnp.where(mine < 0.0, -2.0, mine)
        for u in range(4):
            hit = as_column(ghost_in[k, TRACE + u:TRACE + u + 1, :]) == target
            match[k, u * GH:(u + 1) * GH, :] = jnp.where(hit, 1.0, 0.0).astype(jnp.bfloat16)
    trade_wait_recv(1)
    complete_ghosts()
    back_left[...] = stacked([near_in[k] for k in range(4)])
    pick_back(0)
    pick_ghost(ghost_sum, picked1, 0)
    add_back(0, near_in)
    last = E_DEV // LANES - 1

    def middle(b, carry):
        multiply(1, picked1, b)
        pick_back(b + 1)
        pick_ghost(ghost_sum, picked1, b + 1)
        return carry

    lax.fori_loop(0, last, middle, 0)
    norm0, curve0 = sum_finish(0)
    step0 = norm0 / curve0
    multiply(1, picked1, last)
    for b in range(F_DEV // LANES):
        cols = slice(b * LANES, (b + 1) * LANES)
        field1[:, cols] = field0[:, cols] - step0 * image[0, :, cols]
    square, weighted = face_sums(field1)
    sum_start(1, square, weighted + energy(step0))
    scatter_ghost(1)
    send_part(1)
    scatter_own(1, field1)
    trade_wait_recv(2)
    add_back(1, back_in)
    norm1, curve1 = sum_finish(1)
    ratio = norm1 / norm0
    step1 = norm1 / (curve1 - ratio * norm1 / step0)
    lead = step0 + step1 * ratio
    for b in range(F_DEV // LANES):
        cols = slice(b * LANES, (b + 1) * LANES)
        lead_ref[:, cols] = lead * field0[0:TRACE, cols]
        later_ref[:, cols] = field1[0:TRACE, cols]
        along_ref[:, cols] = image[1, 0:TRACE, cols] + ratio * image[0, 0:TRACE, cols]
    step_ref[...] = jnp.broadcast_to(step1, (TRACE, F_DEV))

    for turn in range(3):
        trade_wait_send(turn)
    pltpu.make_async_copy(
        sum_in.at[:, pl.ds(0, N_DOM - 1)], sum_in.at[:, pl.ds(1, N_DOM - 1)], sum_send
    ).wait()


def shards(right_side, element_matrix, face_map, share_index, share_count, face_mass, absorbing, impedance):
    hbm = pl.BlockSpec(memory_space=pltpu.HBM)
    f32, bf16, i32 = jnp.float32, jnp.bfloat16, jnp.int32
    out = pltpu.VMEM((TRACE, F_DEV), f32)
    vmem = pl.BlockSpec(memory_space=pltpu.VMEM)
    lead, later, along, step = pl.pallas_call(
        kernel,
        name="trace_cg",
        out_shape=(out, out, out, out),
        in_specs=[hbm] * 8,
        out_specs=(vmem, vmem, vmem, vmem),
        scratch_shapes=[
            pltpu.VMEM((TRACE, F_DEV), f32),
            pltpu.VMEM((SIDES, E_DEV), i32),
            pltpu.VMEM((4, GH), i32),
            pltpu.SMEM((1, 4), i32),
            pltpu.VMEM((8, LANES), f32),
            pltpu.VMEM((8, LANES), i32),
            pltpu.VMEM((8, LANES), f32),
            pltpu.SemaphoreType.DMA((7,)),
            pltpu.SemaphoreType.REGULAR((2,)),
            pltpu.VMEM((DOFS, DOFS, E_DEV), bf16),
            pltpu.VMEM((E_DEV // LANES, DOFS, DOFS, LANES), f32),
            pltpu.VMEM((ROWS, F_DEV), f32),
            pltpu.VMEM((ROWS, F_DEV), f32),
            pltpu.VMEM((2, ROWS, F_DEV), f32),
            pltpu.VMEM((8, LANES), f32),
            pltpu.VMEM((SIDES, 4, ROWS, LANES), f32),
            pltpu.VMEM((SIDES, 4, ROWS, LANES), f32),
            pltpu.VMEM((2, SIDES, E_DEV // LANES, ROWS, LANES), f32),
            pltpu.VMEM((E_DEV // LANES, SIDES * LANES, WIDE), bf16),
            pltpu.VMEM((4 * GH, WIDE), bf16),
            pltpu.VMEM((E_DEV // LANES, 4 * GH, SIDES * LANES), bf16),
            pltpu.VMEM((2 * ROWS, 4 * GH), bf16),
            pltpu.VMEM((4, 4 * GH, GH), bf16),
            pltpu.VMEM((2, 4, ROWS, GH), f32),
            pltpu.VMEM((4, ROWS, GH), f32),
            pltpu.VMEM((2, 4, ROWS, GH), f32),
            pltpu.VMEM((4, ROWS, GH), f32),
            pltpu.VMEM((24, ROWS, GH), f32),
            pltpu.VMEM((4, ROWS, GH), f32),
            pltpu.VMEM((2, 1, LANES), f32),
            pltpu.VMEM((2, N_DOM, LANES), f32),
            pltpu.SemaphoreType.DMA,
            pltpu.SemaphoreType.DMA((3,)),
            pltpu.SemaphoreType.DMA((3,)),
            pltpu.SemaphoreType.DMA,
            pltpu.SemaphoreType.DMA((2,)),
        ],
        compiler_params=pltpu.CompilerParams(
            collective_id=0, has_side_effects=True, vmem_limit_bytes=65 * 1000 * 1000
        ),
    )(
        right_side, element_matrix, face_map, share_index.reshape(4, GH), share_count,
        face_mass.reshape(8, LANES), absorbing.reshape(8, LANES), impedance.reshape(8, LANES),
    )
    return lead + step * later, later - step * along


def solution(mesh):
    in_specs = (
        P(None, "dom"), P(None, None, "dom"), P(None, "dom"), P("dom", None, None),
        P("dom", None), P("dom"), P("dom"), P("dom"),
    )
    return jax.shard_map(
        shards, mesh=mesh, in_specs=in_specs,
        out_specs=(P(None, "dom"), P(None, "dom")), check_vma=False,
    )
```

```python
import functools

import jax
import jax.numpy as jnp
from jax import lax
from jax.experimental import pallas as pl
from jax.experimental.pallas import tpu as pltpu
from jax.sharding import PartitionSpec as P

TRACE = 18
ROWS = 24
SIDES = 4
DOFS = 72
E_DEV = 512
F_DEV = 1024
GH = 128
OFFSETS = (-2, -1, 1, 2)
N_DOM = 128
LANES = 128
WIDE = 256
MESH = pl.DeviceIdType.MESH


def lane_pick(blocks, index_row, first, base):
    low = jnp.broadcast_to(index_row & (LANES - 1), (8, LANES))
    high = jnp.broadcast_to(index_row >> 7, (8, LANES))
    masks = [high == first + at for at in range(len(blocks))]
    pieces = []
    for i in range(ROWS // 8):
        picked = jnp.zeros((8, LANES), jnp.float32) if base is None else base(i)
        for mask, block in zip(masks, blocks):
            moved = jnp.take_along_axis(block(i), low, axis=1, mode="promise_in_bounds")
            picked = jnp.where(mask, moved, picked)
        pieces.append(picked)
    return jnp.concatenate(pieces, axis=0)


def split_two(value):
    head = value.astype(jnp.bfloat16)
    tail = (value - head.astype(jnp.float32)).astype(jnp.bfloat16)
    return head.astype(jnp.float32), tail.astype(jnp.float32)


def spread_rows(value, index_row, groups):
    head, tail = split_two(value)
    high = jnp.broadcast_to(index_row >> 8, value.shape)
    pieces = []
    for group in groups:
        mask = high == group
        pieces.append(jnp.where(mask, head, 0.0))
        pieces.append(jnp.where(mask, tail, 0.0))
    return jnp.concatenate(pieces, axis=0).astype(jnp.bfloat16)


def as_column(row):
    return jnp.broadcast_to(row, (LANES, LANES)).T


def one_hot_low(index_row):
    column = as_column((index_row & (WIDE - 1)).astype(jnp.float32))
    lane = lax.broadcasted_iota(jnp.int32, (LANES, LANES), 1).astype(jnp.float32)
    halves = [jnp.where(column == lane + half * LANES, 1.0, 0.0) for half in range(2)]
    return jnp.concatenate(halves, axis=1).astype(jnp.bfloat16)


def stacked(blocks):
    pairs = [split_two(block) for block in blocks]
    return jnp.concatenate([jnp.concatenate(pair, axis=0) for pair in pairs], axis=1).astype(jnp.bfloat16)


def wide_dot(left, right):
    return jnp.dot(left, right, preferred_element_type=jnp.float32)


def kernel(
    right_hbm, matrix_hbm, map_hbm, share_hbm, count_hbm, mass_hbm, absorb_hbm, imped_hbm,
    lead_ref, later_ref, along_ref, step_ref,
    right_ref, map_ref, share_ref, count_ref, mass_ref, absorb_ref, imped_ref, load_sem, meet_sem,
    matrix, widened, field0, field1, image, diag, picked0, picked1, product, hot, hot_share, hot_back, back_left, match,
    out_buf, ghost_in, part_buf, back_in, near_in, ghost_sum, sum_buf, sum_in,
    matrix_sem, trade_send, trade_recv, sum_send, sum_recv,
):
    me = lax.axis_index("dom")
    rows18, rows22 = pl.ds(0, TRACE), pl.ds(0, TRACE + 4)

    def blocks_wait(ref, rows, sem, count, options):
        for n in options:
            @pl.when(count == n)
            def _(n=n):
                some = ref.at[pl.ds(0, n), rows]
                pltpu.make_async_copy(some, some, sem).wait()

    core = lax.rem(me, 2)
    at_x = lax.rem(me // 2, 4)
    at_y = lax.rem(me // 8, 4)
    at_z = me // 32

    along_x = [lax.rem(at_x + d, 4) * 2 for d in range(4)]
    along_y = [lax.rem(at_y + d, 4) * 8 for d in range(4)]
    along_z = [lax.rem(at_z + d, 4) * 32 for d in range(4)]
    cores = (core, 1 - core)

    def device_at(dz, dy, dx, dc):
        return along_z[dz] + along_y[dy] + along_x[dx] + cores[dc]

    inside_to = [(me + o >= 0) & (me + o < N_DOM) for o in OFFSETS]
    inside_from = [(me - o >= 0) & (me - o < N_DOM) for o in OFFSETS]
    crosses = sorted(
        ((k, u) for k in range(4) for u in range(4) if k != u), key=lambda at: -abs(OFFSETS[at[1]] - OFFSETS[at[0]])
    )

    def cross_ok(k, u):
        user = me - OFFSETS[k] + OFFSETS[u]
        return inside_from[k] & (user >= 0) & (user < N_DOM)


    def tally(flags):
        return functools.reduce(lambda total, flag: total + flag.astype(jnp.int32), flags, jnp.int32(0))

    barrier = pltpu.get_barrier_semaphore()
    for k, o in sorted(enumerate(OFFSETS), key=lambda at: -abs(at[1])):
        @pl.when(inside_to[k])
        def _():
            pl.semaphore_signal(barrier, inc=1, device_id=(me + o,), device_id_type=MESH)
    loads = [
        pltpu.make_async_copy(source, target, load_sem.at[min(at, 4)])
        for at, (source, target) in enumerate((
            (share_hbm, share_ref), (count_hbm, count_ref), (right_hbm, right_ref), (map_hbm, map_ref),
            (mass_hbm, mass_ref), (absorb_hbm, absorb_ref), (imped_hbm, imped_ref),
        ))
    ]
    for load in loads[:4]:
        load.start()
    for load in loads[4:]:
        load.start()
    matrix_copy = pltpu.make_async_copy(matrix_hbm, matrix, matrix_sem)
    matrix_copy.start()

    line_y = [device_at(0, d, 0, 0) for d in range(1, 4)]
    line_z = [device_at(d, 0, 0, 0) for d in range(1, 4)]
    pairs_x = [device_at(0, 0, d, c) for d in range(4) for c in range(2) if d or c]
    for other in pairs_x + line_y + line_z:
        pl.semaphore_signal(barrier, inc=1, device_id=(other,), device_id_type=MESH)

    near_to, near_from = tally(inside_to), tally(inside_from)
    all_near = near_to + near_from + tally([cross_ok(k, u) for k, u in crosses])

    arrivals = 13 + near_from

    def meet(at, others):
        for other in others:
            pl.semaphore_signal(meet_sem.at[at], inc=1, device_id=(other,), device_id_type=MESH)

    for load in loads[:3]:
        load.wait()
    field0[0:TRACE, :] = right_ref[...]
    field0[TRACE:ROWS, :] = jnp.zeros((ROWS - TRACE, F_DEV), jnp.float32)
    lane = lax.broadcasted_iota(jnp.int32, (ROWS, GH), 1)
    alive = [lane < count_ref[0, k] for k in range(4)]

    def own_blocks(ref):
        return [
            lambda i, b=b: ref[8 * i:8 * i + 8, b * LANES:(b + 1) * LANES] for b in range(F_DEV // LANES)
        ]

    def trade(turn, source, target, other):
        rows = rows22 if turn == 0 else rows18
        return pltpu.make_async_remote_copy(
            src_ref=source.at[rows], dst_ref=target.at[rows],
            send_sem=trade_send.at[turn], recv_sem=trade_recv.at[turn], device_id=(other,), device_id_type=MESH,
        )

    def out_copy(turn, k):
        return trade(turn, out_buf.at[turn, k], ghost_in.at[k] if turn == 0 else near_in.at[4 + k], me + OFFSETS[k])

    def cross_copy(k, u):
        return trade(1, part_buf.at[0, k], near_in.at[8 + 4 * u + k], me - OFFSETS[k] + OFFSETS[u])

    def part_copy(turn, k):
        return trade(1 + turn, part_buf.at[turn, k], near_in.at[k] if turn == 0 else back_in.at[k], me - OFFSETS[k])

    trades = (
        (ghost_in, near_to, near_from, (2, 3, 4)),
        (near_in, all_near, all_near, (9, 13, 17, 19, 20)),
        (back_in, near_from, near_to, (2, 3, 4)),
    )

    def trade_wait_recv(turn):
        ref, _, count, options = trades[turn]
        blocks_wait(ref, rows18 if turn else rows22, trade_recv.at[turn], count, options)

    def trade_wait_send(turn):
        ref, count, _, options = trades[turn]
        blocks_wait(ref, rows18 if turn else rows22, trade_send.at[turn], count, options)

    def send_out(turn, ref):
        blocks = own_blocks(ref)
        for k in range(4):
            gone = lane_pick(blocks, share_ref[k:k + 1, :], 0, None)
            out_buf[turn, k, 0:TRACE] = jnp.where(alive[k], gone, 0.0)[0:TRACE]
        if turn == 0:
            pl.semaphore_wait(barrier, arrivals)
        for k in (0, 3, 1, 2):
            @pl.when(inside_to[k])
            def _():
                out_copy(turn, k).start()

    def send_part(turn):
        for k in range(4):
            @pl.when(inside_from[k])
            def _():
                part_copy(turn, k).start()

    def send_cross():
        for k, u in crosses:
            @pl.when(cross_ok(k, u))
            def _():
                cross_copy(k, u).start()

    def pick_own(ref, picked):
        blocks = own_blocks(ref)
        for side in range(SIDES):
            for b in range(E_DEV // LANES):
                cols = slice(b * LANES, (b + 1) * LANES)
                picked[side, b] = lane_pick(blocks, map_ref[side:side + 1, cols], 0, None)

    def pick_ghost(ghosts, picked, b):
        blocks = [lambda i, k=k: ghosts[k, 8 * i:8 * i + 8] for k in range(4)]
        first = b * LANES if isinstance(b, int) else pl.multiple_of(b * LANES, LANES)
        cols = pl.ds(first, LANES)
        for side in range(SIDES):
            base = lambda i, side=side: picked[side, b, 8 * i:8 * i + 8]
            picked[side, b] = lane_pick(blocks, map_ref[side:side + 1, cols], F_DEV // LANES, base)

    def multiply(turn, picked, b):
        def one(side, total):
            for c in range(TRACE):
                row = picked[side, b, c:c + 1, :]
                total = total + widened[b, side * TRACE + c] * row
            return total

        total = jnp.zeros((DOFS, LANES), jnp.float32)
        for side in range(SIDES):
            total = one(side, total)
        for side in range(SIDES):
            product[turn, side, b, 0:TRACE, :] = total[side * TRACE:(side + 1) * TRACE]

    def scatter_block(turn, groups, b):
        lefts = [
            spread_rows(product[turn, side, b], map_ref[side:side + 1, b * LANES:(b + 1) * LANES], groups)
            for side in range(SIDES)
        ]
        return wide_dot(jnp.concatenate(lefts, axis=1), hot[b])

    def energy(step):
        total = jnp.zeros((ROWS, LANES), jnp.float32)
        for side in range(SIDES):
            for b in range(E_DEV // LANES):
                image_part = product[0, side, b] - step * product[1, side, b]
                product[1, side, b] = image_part
                total = total + (picked0[side, b] - step * picked1[side, b]) * image_part
        return jnp.sum(total, axis=0, keepdims=True)

    def scatter_block(turn, groups, b):
        lefts = [
            spread_rows(product[turn, side, b], map_ref[side:side + 1, b * LANES:(b + 1) * LANES], groups)
            for side in range(SIDES)
        ]
        return wide_dot(jnp.concatenate(lefts, axis=1), hot[b])

    def energy(step):
        total = jnp.zeros((ROWS, LANES), jnp.float32)
        for side in range(SIDES):
            for b in range(E_DEV // LANES):
                image_part = product[0, side, b]
                value = picked0[side, b]
                if step is not None:
                    image_part = image_part - step * product[1, side, b]
                    product[1, side, b] = image_part
                    value = value - step * picked1[side, b]
                total = total + value * image_part
        return jnp.sum(total, axis=0, keepdims=True)

    def face_sums(ref):
        square = jnp.zeros((8, LANES), jnp.float32)
        weighted = jnp.zeros((8, LANES), jnp.float32)
        for b in range(F_DEV // LANES):
            value = ref[:, b * LANES:(b + 1) * LANES]
            both = value * value
            both = both[0:8] + both[8:16] + both[16:24]
            square = square + both
            weighted = weighted + both * diag[b:b + 1, :]
        return jnp.sum(square, axis=0, keepdims=True), jnp.sum(weighted, axis=0, keepdims=True)

    def scatter(turn, groups, total):
        if total is None:
            parts = [scatter_block(turn, groups, b) for b in range(E_DEV // LANES)]
            total = (parts[0] + parts[1]) + (parts[2] + parts[3])
        for at in range(len(groups)):
            base = at * 2 * ROWS
            yield total[base:base + ROWS] + total[base + ROWS:base + 2 * ROWS]

    def scatter_ghost(turn, total=None):
        for at, both in enumerate(scatter(turn, (4, 5), total)):
            part_buf[turn, 2 * at] = both[:, 0:GH]
            part_buf[turn, 2 * at + 1] = both[:, GH:]

    def scatter_own(turn, ref):
        for at, both in enumerate(scatter(turn, (0, 1, 2, 3), None)):
            for half in range(2):
                b = 2 * at + half
                cols = slice(b * LANES, (b + 1) * LANES)
                image[turn, :, cols] = both[:, half * LANES:(half + 1) * LANES] + diag[b:b + 1, :] * ref[:, cols]

    def add_back(turn, back):
        total = jnp.zeros((4 * 2 * ROWS, WIDE), jnp.float32)
        for k in range(4):
            value = jnp.where(alive[k], back[k], 0.0)
            left = spread_rows(value, share_ref[k:k + 1, :], (0, 1, 2, 3))
            total = total + wide_dot(left, hot_share[k * GH:(k + 1) * GH, :])
        for group in range(4):
            base = group * 2 * ROWS
            both = total[base:base + ROWS] + total[base + ROWS:base + 2 * ROWS]
            cols = slice(group * WIDE, (group + 1) * WIDE)
            image[turn, :, cols] = image[turn, :, cols] + both

    others = sorted(
        ((dz, dy, dx, dc) for dz in range(4) for dy in range(4) for dx in range(4) for dc in range(2) if dz or dy or dx or dc),
        key=lambda at: -sum(min(d, 4 - d) for d in at[:3]),
    )

    def sum_start(turn, first, second):
        lane_at = lax.broadcasted_iota(jnp.int32, (1, LANES), 1)
        first = first + pltpu.roll(first, LANES // 2, 1)
        second = second + pltpu.roll(second, LANES // 2, 1)
        row = jnp.where(lane_at < LANES // 2, first, second)
        sum_buf[turn] = row
        sum_in[turn, pl.ds(me, 1), :] = row
        for at in others:
            pltpu.make_async_remote_copy(
                src_ref=sum_buf.at[turn], dst_ref=sum_in.at[turn, pl.ds(me, 1), :],
                send_sem=sum_send, recv_sem=sum_recv.at[turn],
                device_id=(device_at(*at),), device_id_type=MESH,
            ).start()

    def sum_finish(turn):
        pltpu.make_async_copy(
            sum_in.at[turn, pl.ds(0, N_DOM - 1)], sum_in.at[turn, pl.ds(1, N_DOM - 1)], sum_recv.at[turn]
        ).wait()
        total = jnp.sum(sum_in[turn], axis=0, keepdims=True)
        lane_at = lax.broadcasted_iota(jnp.int32, (1, LANES), 1)
        first = jnp.sum(jnp.where(lane_at < LANES // 2, total, 0.0), axis=1, keepdims=True)
        second = jnp.sum(jnp.where(lane_at < LANES // 2, 0.0, total), axis=1, keepdims=True)
        return first, second

    def clear_tail(ref):
        for turn in range(2):
            for side in range(SIDES):
                for b in range(E_DEV // LANES):
                    ref[turn, side, b, TRACE:ROWS, :] = jnp.zeros((ROWS - TRACE, LANES), jnp.float32)

    def complete_ghosts():
        for k in range(4):
            left = stacked([part_buf[0, k] if u == k else near_in[8 + 4 * k + u] for u in range(4)])
            both = wide_dot(left, match[k])
            ghost_sum[k] = near_in[4 + k] + both[0:ROWS] + both[ROWS:2 * ROWS]

    def pick_back(b):
        both = wide_dot(back_left[...], hot_back[b])
        for side in range(SIDES):
            cols = slice(side * LANES, (side + 1) * LANES)
            picked1[side, b] = picked1[side, b] + both[0:ROWS, cols] + both[ROWS:2 * ROWS, cols]

    lists = [jnp.where(alive[k][0:1], share_ref[k:k + 1, :].astype(jnp.float32), -1.0) for k in range(4)]
    for k in range(4):
        out_buf[0, k, TRACE:TRACE + 4] = jnp.concatenate(lists, axis=0)
    send_out(0, field0)
    loads[3].wait()
    pltpu.make_async_copy(near_in.at[0], near_in.at[0], load_sem.at[4]).wait()
    diag[...] = mass_ref[...] + absorb_ref[...].astype(jnp.float32) * imped_ref[...]
    blank = jnp.zeros((TRACE, GH), jnp.float32)
    for k in range(4):
        @pl.when(jnp.logical_not(inside_from[k]))
        def _():
            ghost_in[k, 0:TRACE] = blank
            near_in[4 + k, 0:TRACE] = blank
            ghost_in[k, TRACE:TRACE + 4] = jnp.full((4, GH), -1.0, jnp.float32)
        @pl.when(jnp.logical_not(inside_to[k]))
        def _():
            near_in[k, 0:TRACE] = blank
            back_in[k, 0:TRACE] = blank
        ghost_in[k, TRACE + 4:ROWS] = jnp.zeros((ROWS - TRACE - 4, GH), jnp.float32)
        back_in[k, TRACE:ROWS] = jnp.zeros((ROWS - TRACE, GH), jnp.float32)
    for k, u in crosses:
        @pl.when(jnp.logical_not(cross_ok(k, u)))
        def _():
            near_in[8 + 4 * k + u, 0:TRACE] = blank
    for at in range(24):
        near_in[at, TRACE:ROWS] = jnp.zeros((ROWS - TRACE, GH), jnp.float32)

    meet(0, line_y)
    clear_tail(product)
    for side in range(SIDES):
        for b in range(E_DEV // LANES):
            first = side * LANES
            hot[b, first:first + LANES, :] = one_hot_low(map_ref[side:side + 1, b * LANES:(b + 1) * LANES])
    for k in range(4):
        hot_share[k * GH:(k + 1) * GH, :] = one_hot_low(share_ref[k:k + 1, :])
    square, weighted = face_sums(field0)
    for u in range(4):
        column = as_column(lists[u])
        for side in range(SIDES):
            for b in range(E_DEV // LANES):
                cols = slice(b * LANES, (b + 1) * LANES)
                hit = column == map_ref[side:side + 1, cols].astype(jnp.float32)
                first = side * LANES
                hot_back[b, u * GH:(u + 1) * GH, first:first + LANES] = jnp.where(hit, 1.0, 0.0).astype(jnp.bfloat16)
    pl.semaphore_wait(meet_sem.at[0], 3)
    meet(1, line_z)
    matrix_copy.wait()

    def widen(row, carry):
        whole = matrix[row].astype(jnp.float32)
        for b in range(E_DEV // LANES):
            widened[b, row] = whole[:, b * LANES:(b + 1) * LANES]
        return carry

    pick_own(field0, picked0)
    lax.fori_loop(0, DOFS, widen, 0, unroll=2)
    pl.semaphore_wait(meet_sem.at[1], 3)
    trade_wait_recv(0)

    total, force = None, None
    for b in range(E_DEV // LANES):
        pick_ghost(ghost_in, picked0, b)
        multiply(0, picked0, b)
        part = scatter_block(0, (4, 5), b)
        total = part if total is None else total + part
        for side in range(SIDES):
            both = picked0[side, b] * product[0, side, b]
            force = both if force is None else force + both
    scatter_ghost(0, total)
    send_cross()
    send_part(0)
    scatter_own(0, field0)
    send_out(1, image.at[0])
    sum_start(0, square, weighted + jnp.sum(force, axis=0, keepdims=True))
    pick_own(image.at[0], picked1)
    for k in range(4):
        mine = ghost_in[k, TRACE + k:TRACE + k + 1, :]
        target = jnp.where(mine < 0.0, -2.0, mine)
        for u in range(4):
            hit = as_column(ghost_in[k, TRACE + u:TRACE + u + 1, :]) == target
            match[k, u * GH:(u + 1) * GH, :] = jnp.where(hit, 1.0, 0.0).astype(jnp.bfloat16)
    trade_wait_recv(1)
    complete_ghosts()
    back_left[...] = stacked([near_in[k] for k in range(4)])
    pick_back(0)
    pick_ghost(ghost_sum, picked1, 0)
    add_back(0, near_in)
    last = E_DEV // LANES - 1

    def middle(b, carry):
        multiply(1, picked1, b)
        pick_back(b + 1)
        pick_ghost(ghost_sum, picked1, b + 1)
        return carry

    lax.fori_loop(0, last, middle, 0)
    norm0, curve0 = sum_finish(0)
    step0 = norm0 / curve0
    multiply(1, picked1, last)
    for b in range(F_DEV // LANES):
        cols = slice(b * LANES, (b + 1) * LANES)
        field1[:, cols] = field0[:, cols] - step0 * image[0, :, cols]
    square, weighted = face_sums(field1)
    sum_start(1, square, weighted + energy(step0))
    scatter_ghost(1)
    send_part(1)
    scatter_own(1, field1)
    trade_wait_recv(2)
    add_back(1, back_in)
    for b in range(F_DEV // LANES):
        cols = slice(b * LANES, (b + 1) * LANES)
        later_ref[:, cols] = field1[0:TRACE, cols]
    norm1, curve1 = sum_finish(1)
    ratio = norm1 / norm0
    step1 = norm1 / (curve1 - ratio * norm1 / step0)
    lead = step0 + step1 * ratio
    for b in range(F_DEV // LANES):
        cols = slice(b * LANES, (b + 1) * LANES)
        lead_ref[:, cols] = lead * field0[0:TRACE, cols]
        along_ref[:, cols] = image[1, 0:TRACE, cols] + ratio * image[0, 0:TRACE, cols]
    step_ref[...] = jnp.broadcast_to(step1, (TRACE, F_DEV))

    for turn in range(3):
        trade_wait_send(turn)
    pltpu.make_async_copy(
        sum_in.at[:, pl.ds(0, N_DOM - 1)], sum_in.at[:, pl.ds(1, N_DOM - 1)], sum_send
    ).wait()


def shards(right_side, element_matrix, face_map, share_index, share_count, face_mass, absorbing, impedance):
    hbm = pl.BlockSpec(memory_space=pltpu.HBM)
    f32, bf16, i32 = jnp.float32, jnp.bfloat16, jnp.int32
    out = pltpu.VMEM((TRACE, F_DEV), f32)
    vmem = pl.BlockSpec(memory_space=pltpu.VMEM)
    lead, later, along, step = pl.pallas_call(
        kernel,
        name="trace_cg",
        out_shape=(out, out, out, out),
        in_specs=[hbm] * 8,
        out_specs=(vmem, vmem, vmem, vmem),
        scratch_shapes=[
            pltpu.VMEM((TRACE, F_DEV), f32),
            pltpu.VMEM((SIDES, E_DEV), i32),
            pltpu.VMEM((4, GH), i32),
            pltpu.SMEM((1, 4), i32),
            pltpu.VMEM((8, LANES), f32),
            pltpu.VMEM((8, LANES), i32),
            pltpu.VMEM((8, LANES), f32),
            pltpu.SemaphoreType.DMA((5,)),
            pltpu.SemaphoreType.REGULAR((2,)),
            pltpu.VMEM((DOFS, DOFS, E_DEV), bf16),
            pltpu.VMEM((E_DEV // LANES, DOFS, DOFS, LANES), f32),
            pltpu.VMEM((ROWS, F_DEV), f32),
            pltpu.VMEM((ROWS, F_DEV), f32),
            pltpu.VMEM((2, ROWS, F_DEV), f32),
            pltpu.VMEM((8, LANES), f32),
            pltpu.VMEM((SIDES, 4, ROWS, LANES), f32),
            pltpu.VMEM((SIDES, 4, ROWS, LANES), f32),
            pltpu.VMEM((2, SIDES, E_DEV // LANES, ROWS, LANES), f32),
            pltpu.VMEM((E_DEV // LANES, SIDES * LANES, WIDE), bf16),
            pltpu.VMEM((4 * GH, WIDE), bf16),
            pltpu.VMEM((E_DEV // LANES, 4 * GH, SIDES * LANES), bf16),
            pltpu.VMEM((2 * ROWS, 4 * GH), bf16),
            pltpu.VMEM((4, 4 * GH, GH), bf16),
            pltpu.VMEM((2, 4, ROWS, GH), f32),
            pltpu.VMEM((4, ROWS, GH), f32),
            pltpu.VMEM((2, 4, ROWS, GH), f32),
            pltpu.VMEM((4, ROWS, GH), f32),
            pltpu.VMEM((24, ROWS, GH), f32),
            pltpu.VMEM((4, ROWS, GH), f32),
            pltpu.VMEM((2, 1, LANES), f32),
            pltpu.VMEM((2, N_DOM, LANES), f32),
            pltpu.SemaphoreType.DMA,
            pltpu.SemaphoreType.DMA((3,)),
            pltpu.SemaphoreType.DMA((3,)),
            pltpu.SemaphoreType.DMA,
            pltpu.SemaphoreType.DMA((2,)),
        ],
        compiler_params=pltpu.CompilerParams(
            collective_id=0, has_side_effects=True, vmem_limit_bytes=65 * 1000 * 1000
        ),
    )(
        right_side, element_matrix, face_map, share_index.reshape(4, GH), share_count,
        face_mass.reshape(8, LANES), absorbing.reshape(8, LANES), impedance.reshape(8, LANES),
    )
    return lead + step * later, later - step * along


def solution(mesh):
    in_specs = (
        P(None, "dom"), P(None, None, "dom"), P(None, "dom"), P("dom", None, None),
        P("dom", None), P("dom"), P("dom"), P("dom"),
    )
    return jax.shard_map(
        shards, mesh=mesh, in_specs=in_specs,
        out_specs=(P(None, "dom"), P(None, "dom")), check_vma=False,
    )
```

```python
import functools

import jax
import jax.numpy as jnp
from jax import lax
from jax.experimental import pallas as pl
from jax.experimental.pallas import tpu as pltpu
from jax.sharding import PartitionSpec as P

TRACE = 18
ROWS = 24
SIDES = 4
DOFS = 72
E_DEV = 512
F_DEV = 1024
GH = 128
OFFSETS = (-2, -1, 1, 2)
N_DOM = 128
LANES = 128
WIDE = 256
MESH = pl.DeviceIdType.MESH


def lane_pick(blocks, index_row, first, base):
    low = jnp.broadcast_to(index_row & (LANES - 1), (8, LANES))
    high = jnp.broadcast_to(index_row >> 7, (8, LANES))
    masks = [high == first + at for at in range(len(blocks))]
    pieces = []
    for i in range(ROWS // 8):
        picked = jnp.zeros((8, LANES), jnp.float32) if base is None else base(i)
        for mask, block in zip(masks, blocks):
            moved = jnp.take_along_axis(block(i), low, axis=1, mode="promise_in_bounds")
            picked = jnp.where(mask, moved, picked)
        pieces.append(picked)
    return jnp.concatenate(pieces, axis=0)


def split_two(value):
    head = value.astype(jnp.bfloat16)
    tail = (value - head.astype(jnp.float32)).astype(jnp.bfloat16)
    return head.astype(jnp.float32), tail.astype(jnp.float32)


def spread_rows(value, index_row, groups):
    head, tail = split_two(value)
    high = jnp.broadcast_to(index_row >> 8, value.shape)
    pieces = []
    for group in groups:
        mask = high == group
        pieces.append(jnp.where(mask, head, 0.0))
        pieces.append(jnp.where(mask, tail, 0.0))
    return jnp.concatenate(pieces, axis=0).astype(jnp.bfloat16)


def as_column(row):
    return jnp.broadcast_to(row, (LANES, LANES)).T


def one_hot_low(index_row):
    column = as_column((index_row & (WIDE - 1)).astype(jnp.float32))
    lane = lax.broadcasted_iota(jnp.int32, (LANES, LANES), 1).astype(jnp.float32)
    halves = [jnp.where(column == lane + half * LANES, 1.0, 0.0) for half in range(2)]
    return jnp.concatenate(halves, axis=1).astype(jnp.bfloat16)


def stacked(blocks):
    pairs = [split_two(block) for block in blocks]
    return jnp.concatenate([jnp.concatenate(pair, axis=0) for pair in pairs], axis=1).astype(jnp.bfloat16)


def wide_dot(left, right):
    return jnp.dot(left, right, preferred_element_type=jnp.float32)


def kernel(
    right_hbm, matrix_hbm, map_hbm, share_hbm, count_hbm, mass_hbm, absorb_hbm, imped_hbm,
    lead_ref, later_ref, along_ref, step_ref,
    right_ref, map_ref, share_ref, count_ref, mass_ref, absorb_ref, imped_ref, load_sem, meet_sem,
    matrix, widened, field0, field1, image, diag, picked0, picked1, product, hot, hot_share, hot_back, back_left, match,
    out_buf, ghost_in, part_buf, back_in, near_in, ghost_sum, sum_buf, sum_in,
    matrix_sem, trade_send, trade_recv, sum_send, sum_recv,
):
    me = lax.axis_index("dom")
    rows18, rows22 = pl.ds(0, TRACE), pl.ds(0, TRACE + 4)

    def blocks_wait(ref, rows, sem, count, options):
        for n in options:
            @pl.when(count == n)
            def _(n=n):
                some = ref.at[pl.ds(0, n), rows]
                pltpu.make_async_copy(some, some, sem).wait()

    core = lax.rem(me, 2)
    at_x = lax.rem(me // 2, 4)
    at_y = lax.rem(me // 8, 4)
    at_z = me // 32

    along_x = [lax.rem(at_x + d, 4) * 2 for d in range(4)]
    along_y = [lax.rem(at_y + d, 4) * 8 for d in range(4)]
    along_z = [lax.rem(at_z + d, 4) * 32 for d in range(4)]
    cores = (core, 1 - core)

    def device_at(dz, dy, dx, dc):
        return along_z[dz] + along_y[dy] + along_x[dx] + cores[dc]

    inside_to = [(me + o >= 0) & (me + o < N_DOM) for o in OFFSETS]
    inside_from = [(me - o >= 0) & (me - o < N_DOM) for o in OFFSETS]
    crosses = sorted(
        ((k, u) for k in range(4) for u in range(4) if k != u), key=lambda at: -abs(OFFSETS[at[1]] - OFFSETS[at[0]])
    )

    def cross_ok(k, u):
        user = me - OFFSETS[k] + OFFSETS[u]
        return inside_from[k] & (user >= 0) & (user < N_DOM)


    def tally(flags):
        return functools.reduce(lambda total, flag: total + flag.astype(jnp.int32), flags, jnp.int32(0))

    barrier = pltpu.get_barrier_semaphore()
    for k, o in sorted(enumerate(OFFSETS), key=lambda at: -abs(at[1])):
        @pl.when(inside_to[k])
        def _():
            pl.semaphore_signal(barrier, inc=1, device_id=(me + o,), device_id_type=MESH)
    loads = [
        pltpu.make_async_copy(source, target, load_sem.at[min(at, 4)])
        for at, (source, target) in enumerate((
            (share_hbm, share_ref), (count_hbm, count_ref), (right_hbm, right_ref), (map_hbm, map_ref),
            (mass_hbm, mass_ref), (absorb_hbm, absorb_ref), (imped_hbm, imped_ref),
        ))
    ]
    for load in loads[:4]:
        load.start()
    for load in loads[4:]:
        load.start()
    matrix_copy = pltpu.make_async_copy(matrix_hbm, matrix, matrix_sem)
    matrix_copy.start()

    line_y = [device_at(0, d, 0, 0) for d in range(1, 4)]
    line_z = [device_at(d, 0, 0, 0) for d in range(1, 4)]
    pairs_x = [device_at(0, 0, d, c) for d in range(4) for c in range(2) if d or c]
    for other in pairs_x + line_y + line_z:
        pl.semaphore_signal(barrier, inc=1, device_id=(other,), device_id_type=MESH)

    near_to, near_from = tally(inside_to), tally(inside_from)
    all_near = near_to + near_from + tally([cross_ok(k, u) for k, u in crosses])

    arrivals = 13 + near_from

    def meet(at, others):
        for other in others:
            pl.semaphore_signal(meet_sem.at[at], inc=1, device_id=(other,), device_id_type=MESH)

    for load in loads[:3]:
        load.wait()
    field0[0:TRACE, :] = right_ref[...]
    field0[TRACE:ROWS, :] = jnp.zeros((ROWS - TRACE, F_DEV), jnp.float32)
    lane = lax.broadcasted_iota(jnp.int32, (ROWS, GH), 1)
    alive = [lane < count_ref[0, k] for k in range(4)]

    def own_blocks(ref):
        return [
            lambda i, b=b: ref[8 * i:8 * i + 8, b * LANES:(b + 1) * LANES] for b in range(F_DEV // LANES)
        ]

    def trade(turn, source, target, other):
        rows = rows22 if turn == 0 else rows18
        return pltpu.make_async_remote_copy(
            src_ref=source.at[rows], dst_ref=target.at[rows],
            send_sem=trade_send.at[turn], recv_sem=trade_recv.at[turn], device_id=(other,), device_id_type=MESH,
        )

    def out_copy(turn, k):
        return trade(turn, out_buf.at[turn, k], ghost_in.at[k] if turn == 0 else near_in.at[4 + k], me + OFFSETS[k])

    def cross_copy(k, u):
        return trade(1, part_buf.at[0, k], near_in.at[8 + 4 * u + k], me - OFFSETS[k] + OFFSETS[u])

    def part_copy(turn, k):
        return trade(1 + turn, part_buf.at[turn, k], near_in.at[k] if turn == 0 else back_in.at[k], me - OFFSETS[k])

    trades = (
        (ghost_in, near_to, near_from, (2, 3, 4)),
        (near_in, all_near, all_near, (9, 13, 17, 19, 20)),
        (back_in, near_from, near_to, (2, 3, 4)),
    )

    def trade_wait_recv(turn):
        ref, _, count, options = trades[turn]
        blocks_wait(ref, rows18 if turn else rows22, trade_recv.at[turn], count, options)

    def trade_wait_send(turn):
        ref, count, _, options = trades[turn]
        blocks_wait(ref, rows18 if turn else rows22, trade_send.at[turn], count, options)

    def send_out(turn, ref):
        blocks = own_blocks(ref)
        for k in range(4):
            gone = lane_pick(blocks, share_ref[k:k + 1, :], 0, None)
            out_buf[turn, k, 0:TRACE] = jnp.where(alive[k], gone, 0.0)[0:TRACE]
        if turn == 0:
            pl.semaphore_wait(barrier, arrivals)
        for k in (0, 3, 1, 2):
            @pl.when(inside_to[k])
            def _():
                out_copy(turn, k).start()

    def send_part(turn):
        for k in (0, 3, 1, 2):
            @pl.when(inside_from[k])
            def _():
                part_copy(turn, k).start()

    def send_cross():
        for k, u in crosses:
            @pl.when(cross_ok(k, u))
            def _():
                cross_copy(k, u).start()

    def pick_own(ref, picked):
        blocks = own_blocks(ref)
        for side in range(SIDES):
            for b in range(E_DEV // LANES):
                cols = slice(b * LANES, (b + 1) * LANES)
                picked[side, b] = lane_pick(blocks, map_ref[side:side + 1, cols], 0, None)

    def pick_ghost(ghosts, picked, b):
        blocks = [lambda i, k=k: ghosts[k, 8 * i:8 * i + 8] for k in range(4)]
        first = b * LANES if isinstance(b, int) else pl.multiple_of(b * LANES, LANES)
        cols = pl.ds(first, LANES)
        for side in range(SIDES):
            base = lambda i, side=side: picked[side, b, 8 * i:8 * i + 8]
            picked[side, b] = lane_pick(blocks, map_ref[side:side + 1, cols], F_DEV // LANES, base)

    def multiply(turn, picked, b):
        def one(side, total):
            for c in range(TRACE):
                row = picked[side, b, c:c + 1, :]
                total = total + widened[b, side * TRACE + c] * row
            return total

        total = jnp.zeros((DOFS, LANES), jnp.float32)
        for side in range(SIDES):
            total = one(side, total)
        for side in range(SIDES):
            product[turn, side, b, 0:TRACE, :] = total[side * TRACE:(side + 1) * TRACE]

    def scatter_block(turn, groups, b):
        lefts = [
            spread_rows(product[turn, side, b], map_ref[side:side + 1, b * LANES:(b + 1) * LANES], groups)
            for side in range(SIDES)
        ]
        return wide_dot(jnp.concatenate(lefts, axis=1), hot[b])

    def energy(step):
        total = jnp.zeros((ROWS, LANES), jnp.float32)
        for side in range(SIDES):
            for b in range(E_DEV // LANES):
                image_part = product[0, side, b] - step * product[1, side, b]
                product[1, side, b] = image_part
                total = total + (picked0[side, b] - step * picked1[side, b]) * image_part
        return jnp.sum(total, axis=0, keepdims=True)

    def scatter_block(turn, groups, b):
        lefts = [
            spread_rows(product[turn, side, b], map_ref[side:side + 1, b * LANES:(b + 1) * LANES], groups)
            for side in range(SIDES)
        ]
        return wide_dot(jnp.concatenate(lefts, axis=1), hot[b])

    def energy(step):
        total = jnp.zeros((ROWS, LANES), jnp.float32)
        for side in range(SIDES):
            for b in range(E_DEV // LANES):
                image_part = product[0, side, b]
                value = picked0[side, b]
                if step is not None:
                    image_part = image_part - step * product[1, side, b]
                    product[1, side, b] = image_part
                    value = value - step * picked1[side, b]
                total = total + value * image_part
        return jnp.sum(total, axis=0, keepdims=True)

    def face_sums(ref):
        square = jnp.zeros((8, LANES), jnp.float32)
        weighted = jnp.zeros((8, LANES), jnp.float32)
        for b in range(F_DEV // LANES):
            value = ref[:, b * LANES:(b + 1) * LANES]
            both = value * value
            both = both[0:8] + both[8:16] + both[16:24]
            square = square + both
            weighted = weighted + both * diag[b:b + 1, :]
        return jnp.sum(square, axis=0, keepdims=True), jnp.sum(weighted, axis=0, keepdims=True)

    def scatter(turn, groups, total):
        if total is None:
            parts = [scatter_block(turn, groups, b) for b in range(E_DEV // LANES)]
            total = (parts[0] + parts[1]) + (parts[2] + parts[3])
        for at in range(len(groups)):
            base = at * 2 * ROWS
            yield total[base:base + ROWS] + total[base + ROWS:base + 2 * ROWS]

    def scatter_ghost(turn, total=None):
        for at, both in enumerate(scatter(turn, (4, 5), total)):
            part_buf[turn, 2 * at] = both[:, 0:GH]
            part_buf[turn, 2 * at + 1] = both[:, GH:]

    def scatter_own(turn, ref):
        for at, both in enumerate(scatter(turn, (0, 1, 2, 3), None)):
            for half in range(2):
                b = 2 * at + half
                cols = slice(b * LANES, (b + 1) * LANES)
                image[turn, :, cols] = both[:, half * LANES:(half + 1) * LANES] + diag[b:b + 1, :] * ref[:, cols]

    def add_back(turn, back):
        total = jnp.zeros((4 * 2 * ROWS, WIDE), jnp.float32)
        for k in range(4):
            value = jnp.where(alive[k], back[k], 0.0)
            left = spread_rows(value, share_ref[k:k + 1, :], (0, 1, 2, 3))
            total = total + wide_dot(left, hot_share[k * GH:(k + 1) * GH, :])
        for group in range(4):
            base = group * 2 * ROWS
            both = total[base:base + ROWS] + total[base + ROWS:base + 2 * ROWS]
            cols = slice(group * WIDE, (group + 1) * WIDE)
            image[turn, :, cols] = image[turn, :, cols] + both

    others = sorted(
        ((dz, dy, dx, dc) for dz in range(4) for dy in range(4) for dx in range(4) for dc in range(2) if dz or dy or dx or dc),
        key=lambda at: -sum(min(d, 4 - d) for d in at[:3]),
    )

    def sum_start(turn, first, second):
        lane_at = lax.broadcasted_iota(jnp.int32, (1, LANES), 1)
        first = first + pltpu.roll(first, LANES // 2, 1)
        second = second + pltpu.roll(second, LANES // 2, 1)
        row = jnp.where(lane_at < LANES // 2, first, second)
        sum_buf[turn] = row
        sum_in[turn, pl.ds(me, 1), :] = row
        for at in others:
            pltpu.make_async_remote_copy(
                src_ref=sum_buf.at[turn], dst_ref=sum_in.at[turn, pl.ds(me, 1), :],
                send_sem=sum_send, recv_sem=sum_recv.at[turn],
                device_id=(device_at(*at),), device_id_type=MESH,
            ).start()

    def sum_finish(turn):
        pltpu.make_async_copy(
            sum_in.at[turn, pl.ds(0, N_DOM - 1)], sum_in.at[turn, pl.ds(1, N_DOM - 1)], sum_recv.at[turn]
        ).wait()
        total = jnp.sum(sum_in[turn], axis=0, keepdims=True)
        lane_at = lax.broadcasted_iota(jnp.int32, (1, LANES), 1)
        first = jnp.sum(jnp.where(lane_at < LANES // 2, total, 0.0), axis=1, keepdims=True)
        second = jnp.sum(jnp.where(lane_at < LANES // 2, 0.0, total), axis=1, keepdims=True)
        return first, second

    def clear_tail(ref):
        for turn in range(2):
            for side in range(SIDES):
                for b in range(E_DEV // LANES):
                    ref[turn, side, b, TRACE:ROWS, :] = jnp.zeros((ROWS - TRACE, LANES), jnp.float32)

    def complete_ghosts():
        for k in range(4):
            left = stacked([part_buf[0, k] if u == k else near_in[8 + 4 * k + u] for u in range(4)])
            both = wide_dot(left, match[k])
            ghost_sum[k] = near_in[4 + k] + both[0:ROWS] + both[ROWS:2 * ROWS]

    def pick_back(b):
        both = wide_dot(back_left[...], hot_back[b])
        for side in range(SIDES):
            cols = slice(side * LANES, (side + 1) * LANES)
            picked1[side, b] = picked1[side, b] + both[0:ROWS, cols] + both[ROWS:2 * ROWS, cols]

    lists = [jnp.where(alive[k][0:1], share_ref[k:k + 1, :].astype(jnp.float32), -1.0) for k in range(4)]
    for k in range(4):
        out_buf[0, k, TRACE:TRACE + 4] = jnp.concatenate(lists, axis=0)
    send_out(0, field0)
    loads[3].wait()
    pltpu.make_async_copy(near_in.at[0], near_in.at[0], load_sem.at[4]).wait()
    diag[...] = mass_ref[...] + absorb_ref[...].astype(jnp.float32) * imped_ref[...]
    blank = jnp.zeros((TRACE, GH), jnp.float32)
    for k in range(4):
        @pl.when(jnp.logical_not(inside_from[k]))
        def _():
            ghost_in[k, 0:TRACE] = blank
            near_in[4 + k, 0:TRACE] = blank
            ghost_in[k, TRACE:TRACE + 4] = jnp.full((4, GH), -1.0, jnp.float32)
        @pl.when(jnp.logical_not(inside_to[k]))
        def _():
            near_in[k, 0:TRACE] = blank
            back_in[k, 0:TRACE] = blank
        ghost_in[k, TRACE + 4:ROWS] = jnp.zeros((ROWS - TRACE - 4, GH), jnp.float32)
        back_in[k, TRACE:ROWS] = jnp.zeros((ROWS - TRACE, GH), jnp.float32)
    for k, u in crosses:
        @pl.when(jnp.logical_not(cross_ok(k, u)))
        def _():
            near_in[8 + 4 * k + u, 0:TRACE] = blank
    for at in range(24):
        near_in[at, TRACE:ROWS] = jnp.zeros((ROWS - TRACE, GH), jnp.float32)

    meet(0, line_y)
    clear_tail(product)
    for side in range(SIDES):
        for b in range(E_DEV // LANES):
            first = side * LANES
            hot[b, first:first + LANES, :] = one_hot_low(map_ref[side:side + 1, b * LANES:(b + 1) * LANES])
    for k in range(4):
        hot_share[k * GH:(k + 1) * GH, :] = one_hot_low(share_ref[k:k + 1, :])
    square, weighted = face_sums(field0)
    for u in range(4):
        column = as_column(lists[u])
        for side in range(SIDES):
            for b in range(E_DEV // LANES):
                cols = slice(b * LANES, (b + 1) * LANES)
                hit = column == map_ref[side:side + 1, cols].astype(jnp.float32)
                first = side * LANES
                hot_back[b, u * GH:(u + 1) * GH, first:first + LANES] = jnp.where(hit, 1.0, 0.0).astype(jnp.bfloat16)
    pl.semaphore_wait(meet_sem.at[0], 3)
    meet(1, line_z)
    matrix_copy.wait()

    def widen(row, carry):
        whole = matrix[row].astype(jnp.float32)
        for b in range(E_DEV // LANES):
            widened[b, row] = whole[:, b * LANES:(b + 1) * LANES]
        return carry

    pick_own(field0, picked0)
    lax.fori_loop(0, DOFS, widen, 0, unroll=2)
    pl.semaphore_wait(meet_sem.at[1], 3)
    trade_wait_recv(0)

    total, force = None, None
    for b in range(E_DEV // LANES):
        pick_ghost(ghost_in, picked0, b)
        multiply(0, picked0, b)
        part = scatter_block(0, (4, 5), b)
        total = part if total is None else total + part
        for side in range(SIDES):
            both = picked0[side, b] * product[0, side, b]
            force = both if force is None else force + both
    scatter_ghost(0, total)
    send_part(0)
    send_cross()
    scatter_own(0, field0)
    send_out(1, image.at[0])
    sum_start(0, square, weighted + jnp.sum(force, axis=0, keepdims=True))
    pick_own(image.at[0], picked1)
    for k in range(4):
        mine = ghost_in[k, TRACE + k:TRACE + k + 1, :]
        target = jnp.where(mine < 0.0, -2.0, mine)
        for u in range(4):
            hit = as_column(ghost_in[k, TRACE + u:TRACE + u + 1, :]) == target
            match[k, u * GH:(u + 1) * GH, :] = jnp.where(hit, 1.0, 0.0).astype(jnp.bfloat16)
    trade_wait_recv(1)
    complete_ghosts()
    back_left[...] = stacked([near_in[k] for k in range(4)])
    pick_back(0)
    pick_ghost(ghost_sum, picked1, 0)
    add_back(0, near_in)
    last = E_DEV // LANES - 1

    def middle(b, carry):
        multiply(1, picked1, b)
        pick_back(b + 1)
        pick_ghost(ghost_sum, picked1, b + 1)
        return carry

    lax.fori_loop(0, last, middle, 0)
    norm0, curve0 = sum_finish(0)
    step0 = norm0 / curve0
    multiply(1, picked1, last)
    for b in range(F_DEV // LANES):
        cols = slice(b * LANES, (b + 1) * LANES)
        field1[:, cols] = field0[:, cols] - step0 * image[0, :, cols]
    square, weighted = face_sums(field1)
    sum_start(1, square, weighted + energy(step0))
    scatter_ghost(1)
    send_part(1)
    scatter_own(1, field1)
    trade_wait_recv(2)
    add_back(1, back_in)
    for b in range(F_DEV // LANES):
        cols = slice(b * LANES, (b + 1) * LANES)
        later_ref[:, cols] = field1[0:TRACE, cols]
    norm1, curve1 = sum_finish(1)
    ratio = norm1 / norm0
    step1 = norm1 / (curve1 - ratio * norm1 / step0)
    lead = step0 + step1 * ratio
    for b in range(F_DEV // LANES):
        cols = slice(b * LANES, (b + 1) * LANES)
        lead_ref[:, cols] = lead * field0[0:TRACE, cols]
        along_ref[:, cols] = image[1, 0:TRACE, cols] + ratio * image[0, 0:TRACE, cols]
    step_ref[...] = jnp.broadcast_to(step1, (TRACE, F_DEV))

    for turn in range(3):
        trade_wait_send(turn)
    pltpu.make_async_copy(
        sum_in.at[:, pl.ds(0, N_DOM - 1)], sum_in.at[:, pl.ds(1, N_DOM - 1)], sum_send
    ).wait()


def shards(right_side, element_matrix, face_map, share_index, share_count, face_mass, absorbing, impedance):
    hbm = pl.BlockSpec(memory_space=pltpu.HBM)
    f32, bf16, i32 = jnp.float32, jnp.bfloat16, jnp.int32
    out = pltpu.VMEM((TRACE, F_DEV), f32)
    vmem = pl.BlockSpec(memory_space=pltpu.VMEM)
    lead, later, along, step = pl.pallas_call(
        kernel,
        name="trace_cg",
        out_shape=(out, out, out, out),
        in_specs=[hbm] * 8,
        out_specs=(vmem, vmem, vmem, vmem),
        scratch_shapes=[
            pltpu.VMEM((TRACE, F_DEV), f32),
            pltpu.VMEM((SIDES, E_DEV), i32),
            pltpu.VMEM((4, GH), i32),
            pltpu.SMEM((1, 4), i32),
            pltpu.VMEM((8, LANES), f32),
            pltpu.VMEM((8, LANES), i32),
            pltpu.VMEM((8, LANES), f32),
            pltpu.SemaphoreType.DMA((5,)),
            pltpu.SemaphoreType.REGULAR((2,)),
            pltpu.VMEM((DOFS, DOFS, E_DEV), bf16),
            pltpu.VMEM((E_DEV // LANES, DOFS, DOFS, LANES), f32),
            pltpu.VMEM((ROWS, F_DEV), f32),
            pltpu.VMEM((ROWS, F_DEV), f32),
            pltpu.VMEM((2, ROWS, F_DEV), f32),
            pltpu.VMEM((8, LANES), f32),
            pltpu.VMEM((SIDES, 4, ROWS, LANES), f32),
            pltpu.VMEM((SIDES, 4, ROWS, LANES), f32),
            pltpu.VMEM((2, SIDES, E_DEV // LANES, ROWS, LANES), f32),
            pltpu.VMEM((E_DEV // LANES, SIDES * LANES, WIDE), bf16),
            pltpu.VMEM((4 * GH, WIDE), bf16),
            pltpu.VMEM((E_DEV // LANES, 4 * GH, SIDES * LANES), bf16),
            pltpu.VMEM((2 * ROWS, 4 * GH), bf16),
            pltpu.VMEM((4, 4 * GH, GH), bf16),
            pltpu.VMEM((2, 4, ROWS, GH), f32),
            pltpu.VMEM((4, ROWS, GH), f32),
            pltpu.VMEM((2, 4, ROWS, GH), f32),
            pltpu.VMEM((4, ROWS, GH), f32),
            pltpu.VMEM((24, ROWS, GH), f32),
            pltpu.VMEM((4, ROWS, GH), f32),
            pltpu.VMEM((2, 1, LANES), f32),
            pltpu.VMEM((2, N_DOM, LANES), f32),
            pltpu.SemaphoreType.DMA,
            pltpu.SemaphoreType.DMA((3,)),
            pltpu.SemaphoreType.DMA((3,)),
            pltpu.SemaphoreType.DMA,
            pltpu.SemaphoreType.DMA((2,)),
        ],
        compiler_params=pltpu.CompilerParams(
            collective_id=0, has_side_effects=True, vmem_limit_bytes=65 * 1000 * 1000
        ),
    )(
        right_side, element_matrix, face_map, share_index.reshape(4, GH), share_count,
        face_mass.reshape(8, LANES), absorbing.reshape(8, LANES), impedance.reshape(8, LANES),
    )
    return lead + step * later, later - step * along


def solution(mesh):
    in_specs = (
        P(None, "dom"), P(None, None, "dom"), P(None, "dom"), P("dom", None, None),
        P("dom", None), P("dom"), P("dom"), P("dom"),
    )
    return jax.shard_map(
        shards, mesh=mesh, in_specs=in_specs,
        out_specs=(P(None, "dom"), P(None, "dom")), check_vma=False,
    )
```
